32 devices in a mesh: dp: 4 (over y, z), sp: 8 (over x, core).
Axes of the slice: x: 4, y: 2, z: 2, core: 2. Of those that a mesh axis runs over, the one named last changes fastest.
The devices are a block of a 4x4x8 slice.
Arguments:
- prompt: bfloat16 [32, 2048, 2048], P('dp', 'sp'), parts along dimension 0
- w_q: bfloat16 [2048, 2048], replicated
- w_k: bfloat16 [2048, 2048], replicated
- w_v: bfloat16 [2048, 2048], replicated
- w_o: bfloat16 [2048, 2048], replicated
- q_norm_w: float32 [2048], replicated
- k_norm_w: float32 [2048], replicated
- post_norm_w: float32 [2048], replicated
- new_token: bfloat16 [32, 2048], P('dp'), parts along dimension 0
Outputs:
- output 1: bfloat16 [32, 2048, 2048], P('dp', 'sp'), parts along dimension 0
- output 2: bfloat16 [32, 2049, 16, 128], P('dp', None, 'sp'), parts along dimension 0
- output 3: bfloat16 [32, 2049, 16, 128], P('dp', None, 'sp'), parts along dimension 0
- output 4: bfloat16 [32, 2048], P('dp'), parts along dimension 0
There are 4 independent parts. The reference program is written for one: setup_inputs(seed, part) draws one part's arguments, and reference() takes and returns one part's arrays. A program takes and returns all parts, laid end to end along the dimension named above; an argument that names none is the same for every part.
All inputs are finite; a program needn't handle non-finite values.
Results may differ from the reference program's by a relative error of at most 0.00731166.
Values are sent between devices in bfloat16 or wider.
A program may use at most 768 MiB of HBM per device.

```python
import jax
import jax.numpy as jnp
from jax import lax

BATCH_ROWS = 8
TOKENS_DEV = 256
GROUP_SIZE = 8
MODEL_WIDTH = 2048
NUM_HEADS = 16
HEAD_DIM = 128

SEQ_LEN = TOKENS_DEV * GROUP_SIZE
HEADS_LOCAL = NUM_HEADS // GROUP_SIZE
QUERY_ROWS = min(TOKENS_DEV, 128)
ROPE_THETA = 500000.0
NORM_EPS = 1e-6


def setup_inputs(seed: int = 0, part: int = 0) -> dict:
    base_key = jax.random.key(seed)
    part_key = jax.random.fold_in(base_key, part)
    w_keys = jax.random.split(base_key, 9)
    x_keys = jax.random.split(part_key, 2)
    fan_scale = MODEL_WIDTH ** -0.5
    q_heads = jnp.exp(jax.random.uniform(w_keys[0], (NUM_HEADS,), jnp.float32, -0.5, 0.5))
    k_heads = jnp.exp(jax.random.uniform(w_keys[1], (NUM_HEADS,), jnp.float32, -0.5, 0.5))
    q_cols = jnp.repeat(q_heads, HEAD_DIM) * fan_scale
    k_cols = jnp.repeat(k_heads, HEAD_DIM) * fan_scale
    w_shape = (MODEL_WIDTH, MODEL_WIDTH)
    w_q = (jax.random.normal(w_keys[2], w_shape, jnp.float32) * q_cols[None, :]).astype(jnp.bfloat16)
    w_k = (jax.random.normal(w_keys[3], w_shape, jnp.float32) * k_cols[None, :]).astype(jnp.bfloat16)
    w_v = (jax.random.normal(w_keys[4], w_shape, jnp.float32) * fan_scale).astype(jnp.bfloat16)
    w_o = (jax.random.normal(w_keys[5], w_shape, jnp.float32) * fan_scale).astype(jnp.bfloat16)
    q_norm_w = jax.random.uniform(w_keys[6], (MODEL_WIDTH,), jnp.float32, 0.5, 1.5)
    k_norm_w = jax.random.uniform(w_keys[7], (MODEL_WIDTH,), jnp.float32, 0.5, 1.5)
    post_norm_w = jax.random.uniform(w_keys[8], (MODEL_WIDTH,), jnp.float32, 0.5, 1.5)
    prompt = jax.random.normal(x_keys[0], (BATCH_ROWS, SEQ_LEN, MODEL_WIDTH), jnp.float32).astype(jnp.bfloat16)
    new_token = jax.random.normal(x_keys[1], (BATCH_ROWS, MODEL_WIDTH), jnp.float32).astype(jnp.bfloat16)
    return {"prompt": prompt, "w_q": w_q, "w_k": w_k, "w_v": w_v, "w_o": w_o, "q_norm_w": q_norm_w, "k_norm_w": k_norm_w, "post_norm_w": post_norm_w, "new_token": new_token}


def rms_norm(values, weight):
    return values * lax.rsqrt(jnp.mean(values * values, axis=-1, keepdims=True) + NORM_EPS) * weight


def rope_tables(positions):
    inv_freq = ROPE_THETA ** (-jnp.arange(0, HEAD_DIM, 2).astype(jnp.float32) / HEAD_DIM)
    angles = positions.astype(jnp.float32)[:, None] * inv_freq[None, :]
    angles = jnp.concatenate([angles, angles], axis=-1)
    return jnp.cos(angles), jnp.sin(angles)


def apply_rope(values, cos_t, sin_t):
    half_dim = HEAD_DIM // 2
    rotated = jnp.concatenate([-values[..., half_dim:], values[..., :half_dim]], axis=-1)
    return values * cos_t[:, None, :] + rotated * sin_t[:, None, :]


def project_heads(x_rows, w_mat, norm_w, cos_t, sin_t):
    normed = rms_norm(jnp.dot(x_rows, w_mat, preferred_element_type=jnp.float32), norm_w)
    return apply_rope(normed.reshape(x_rows.shape[0], NUM_HEADS, HEAD_DIM), cos_t, sin_t).astype(jnp.bfloat16)


def one_sequence(prompt_seq, new_row, w_q, w_k, w_v, w_o, q_norm_w, k_norm_w, post_norm_w):
    score_scale = HEAD_DIM ** -0.5
    cos_p, sin_p = rope_tables(jnp.arange(SEQ_LEN))
    q_seq = project_heads(prompt_seq, w_q, q_norm_w, cos_p, sin_p)
    k_seq = project_heads(prompt_seq, w_k, k_norm_w, cos_p, sin_p)
    v_seq = jnp.dot(prompt_seq, w_v, preferred_element_type=jnp.float32).astype(jnp.bfloat16).reshape(SEQ_LEN, NUM_HEADS, HEAD_DIM)
    k_wide = k_seq.astype(jnp.float32)
    v_wide = v_seq.astype(jnp.float32)
    key_pos = jnp.arange(SEQ_LEN)

    def query_block(block_idx):
        q_blk = lax.dynamic_slice_in_dim(q_seq, block_idx * QUERY_ROWS, QUERY_ROWS, axis=0).astype(jnp.float32)
        q_pos = block_idx * QUERY_ROWS + jnp.arange(QUERY_ROWS)
        scores = jnp.einsum("qhd,khd->hqk", q_blk, k_wide) * score_scale
        scores = jnp.where((q_pos[:, None] >= key_pos[None, :])[None], scores, -1e30)
        attn_p = jax.nn.softmax(scores, axis=-1).astype(jnp.bfloat16)
        return jnp.einsum("hqk,khd->qhd", attn_p.astype(jnp.float32), v_wide).astype(jnp.bfloat16)

    attn_out = lax.map(query_block, jnp.arange(SEQ_LEN // QUERY_ROWS)).reshape(SEQ_LEN, MODEL_WIDTH)
    proj_pre = jnp.dot(attn_out, w_o, preferred_element_type=jnp.float32)
    out_p = (prompt_seq.astype(jnp.float32) + rms_norm(proj_pre, post_norm_w)).astype(jnp.bfloat16)
    cos_d, sin_d = rope_tables(jnp.full((1,), SEQ_LEN))
    q_new = project_heads(new_row[None, :], w_q, q_norm_w, cos_d, sin_d)[0]
    k_new = project_heads(new_row[None, :], w_k, k_norm_w, cos_d, sin_d)[0]
    v_new = jnp.dot(new_row[None, :], w_v, preferred_element_type=jnp.float32).astype(jnp.bfloat16).reshape(NUM_HEADS, HEAD_DIM)
    k_cache = jnp.concatenate([k_seq, k_new[None]], axis=0)
    v_cache = jnp.concatenate([v_seq, v_new[None]], axis=0)
    scores_d = jnp.einsum("hd,khd->hk", q_new.astype(jnp.float32), k_cache.astype(jnp.float32)) * score_scale
    attn_d = jax.nn.softmax(scores_d, axis=-1).astype(jnp.bfloat16)
    o_new = jnp.einsum("hk,khd->hd", attn_d.astype(jnp.float32), v_cache.astype(jnp.float32)).astype(jnp.bfloat16)
    o_groups = o_new.reshape(GROUP_SIZE, HEADS_LOCAL * HEAD_DIM).astype(jnp.float32)
    w_groups = w_o.reshape(GROUP_SIZE, HEADS_LOCAL * HEAD_DIM, MODEL_WIDTH).astype(jnp.float32)
    part_proj = jnp.einsum("gc,gcn->gn", o_groups, w_groups).astype(jnp.bfloat16)
    proj_new = jnp.sum(part_proj.astype(jnp.float32), axis=0)
    out_d = (new_row.astype(jnp.float32) + rms_norm(proj_new, post_norm_w)).astype(jnp.bfloat16)
    return out_p, k_cache, v_cache, out_d


def reference(prompt, w_q, w_k, w_v, w_o, q_norm_w, k_norm_w, post_norm_w, new_token):
    out_p, k_cache, v_cache, out_d = lax.map(
        lambda seq_pair: one_sequence(seq_pair[0], seq_pair[1], w_q, w_k, w_v, w_o, q_norm_w, k_norm_w, post_norm_w),
        (prompt, new_token))
    return out_p, k_cache, v_cache, out_d
```

```python
import functools

import jax
import jax.numpy as jnp
from jax import lax
from jax.experimental import pallas as pl
from jax.experimental.pallas import tpu as pltpu
from jax.sharding import PartitionSpec as P

HEAD_DIM = 128
ROPE_THETA = 500000.0
NORM_EPS = 1e-6
CORES = 2
LOG2E = 1.4426950408889634
SLOTS = 3
COL_TILE = 512
VMEM_BYTES = 66_000_000


def rope_tables(positions):
    inv_freq = ROPE_THETA ** (-jnp.arange(0, HEAD_DIM, 2).astype(jnp.float32) / HEAD_DIM)
    angles = positions.astype(jnp.float32)[:, None] * inv_freq[None, :]
    cos_t, sin_t = jnp.cos(angles), jnp.sin(angles)
    return jnp.concatenate([cos_t, cos_t], axis=-1), jnp.concatenate([-sin_t, sin_t], axis=-1)


def rotate(values, cos_t, sin_t):
    return values * cos_t + pltpu.roll(values, HEAD_DIM // 2, 1) * sin_t


def exchange_kernel(group_n, x_hbm, wq_hbm, wk_hbm, wv_hbm, wo_hbm, gains_ref, post_ref, cos_ref, sin_ref, cosd_ref, sind_ref, new_ref,
                    qkv_ref, o_ref, rel_ref, relo_ref, knew_ref, vnew_ref, outd_ref,
                    w_vm, x_vm, raw_vm, ssq_vm, stage_vm, qkv_vm, ostage_vm, wo_vm, qnew_vm, deco_vm, decp_vm,
                    w_sem, x_sem, wo_sem, send_sem, recv_sem, rel_sem, fwd_sem, load_sem, osend_sem, orecv_sem, relo_sem, decs_sem, decr_sem):
    n_batch, tok, width = x_hbm.shape
    cols = width // group_n
    heads = cols // HEAD_DIM
    seq = tok * group_n
    half = tok // 2
    chips = group_n // CORES
    me = lax.axis_index("sp")
    chip, core = me // CORES, me % CORES
    right = (chip + 1) % chips
    left = (chip + chips - 1) % chips
    far = (chip + 2) % chips
    right_dev, left_dev = right * CORES + core, left * CORES + core
    partner = chip * CORES + (1 - core)
    w_hbm = (wq_hbm, wk_hbm, wv_hbm)
    scale2 = HEAD_DIM ** -0.5 * LOG2E

    def remote(src, dst, s_sem, r_sem, dev):
        return pltpu.make_async_remote_copy(src_ref=src, dst_ref=dst, send_sem=s_sem, recv_sem=r_sem,
                                            device_id={"sp": dev}, device_id_type=pl.DeviceIdType.MESH)

    def drain(ref, sem):
        pltpu.make_async_copy(ref, ref, sem).wait()

    def w_copy(j):
        return pltpu.make_async_copy(w_hbm[j], w_vm.at[j], w_sem.at[j])

    def x_copy(t):
        return pltpu.make_async_copy(x_hbm.at[t], x_vm.at[lax.rem(t, 2)], x_sem.at[lax.rem(t, 2)])

    x_copy(0).start()
    for j in range(3):
        w_copy(j).start()
    wo_copy = pltpu.make_async_copy(wo_hbm.at[pl.ds(me * cols, cols)], wo_vm, wo_sem)
    wo_copy.start()

    barrier = pltpu.get_barrier_semaphore()
    for step in range(1, group_n):
        pl.semaphore_signal(barrier, inc=1, device_id={"sp": lax.rem(me + step, group_n)}, device_id_type=pl.DeviceIdType.MESH)
    pl.semaphore_wait(barrier, group_n - 1)

    def send_tensor(t, slot, j):
        rows = pl.ds(me * tok, tok)
        far_devs = pl.ds(far * CORES, CORES)
        remote(stage_vm.at[slot, j, far_devs, pl.ds(0, half)], rel_ref.at[t, 0, :, j], send_sem.at[t], rel_sem.at[t], right_dev).start()
        remote(stage_vm.at[slot, j, far_devs, pl.ds(half, half)], rel_ref.at[t, 1, :, j], send_sem.at[t], rel_sem.at[t], left_dev).start()
        for side in (right, left):
            for c in range(CORES):
                dev = side * CORES + c
                remote(stage_vm.at[slot, j, dev], qkv_ref.at[j, t, rows], send_sem.at[t], recv_sem.at[t], dev).start()
        remote(stage_vm.at[slot, j, partner], qkv_ref.at[j, t, rows], send_sem.at[t], recv_sem.at[t], partner).start()
        pltpu.make_async_copy(stage_vm.at[slot, j, me], qkv_ref.at[j, t, rows], recv_sem.at[t]).start()

    def drain_sends(t):
        drain(stage_vm.at[lax.rem(t, SLOTS), :, pl.ds(0, group_n - 1)], send_sem.at[t])

    def project(t):
        slot = lax.rem(t, SLOTS)

        @pl.when(t >= SLOTS)
        def _():
            drain_sends(t - SLOTS)

        x_copy(t).wait()

        @pl.when(t + 1 < n_batch)
        def _():
            x_copy(t + 1).start()

        x_slot = lax.rem(t, 2)
        for j in range(3):
            @pl.when(t == 0)
            def _():
                w_copy(j).wait()

            ssq_vm[...] = jnp.zeros_like(ssq_vm)

            def col_tile(n, _):
                at = pl.ds(pl.multiple_of(n * COL_TILE, COL_TILE), COL_TILE)
                acc = jnp.dot(x_vm[x_slot], w_vm[j, :, at], preferred_element_type=jnp.float32)
                if j < 2:
                    raw_vm[:, at] = acc
                    sq = acc * acc
                    ssq_vm[...] += sum(sq[:, i * HEAD_DIM:(i + 1) * HEAD_DIM] for i in range(COL_TILE // HEAD_DIM))
                else:
                    for i in range(COL_TILE // cols):
                        stage_vm[slot, j, n * (COL_TILE // cols) + i] = acc[:, i * cols:(i + 1) * cols].astype(jnp.bfloat16)
                return 0

            lax.fori_loop(0, width // COL_TILE, col_tile, 0)
            if j < 2:
                inv = lax.rsqrt(jnp.sum(ssq_vm[...], axis=1, keepdims=True) / width + NORM_EPS)

                def group_tile(n, _):
                    for h in range(heads):
                        at = pl.ds(pl.multiple_of(n * cols + h * HEAD_DIM, HEAD_DIM), HEAD_DIM)
                        normed = raw_vm[:, at] * inv * gains_ref[j:j + 1, at]
                        stage_vm[slot, j, n, :, h * HEAD_DIM:(h + 1) * HEAD_DIM] = rotate(normed, cos_ref[...], sin_ref[...]).astype(jnp.bfloat16)
                    return 0

                lax.fori_loop(0, group_n, group_tile, 0)
            send_tensor(t, slot, j)

    def forward(b):
        drain(rel_ref.at[b], rel_sem.at[b])
        for way, came, to, first in ((0, left_dev, right, 0), (1, right_dev, left, half)):
            for c in range(CORES):
                remote(rel_ref.at[b, way, c], qkv_ref.at[:, b, pl.ds(came * tok + first, half)], fwd_sem.at[0], recv_sem.at[b], to * CORES + c).start()

    def forward_o(b):
        drain(relo_ref.at[b], relo_sem.at[b])
        for way, came, to, first in ((0, left_dev, right, 0), (1, right_dev, left, half)):
            for c in range(CORES):
                remote(relo_ref.at[b, way, c], o_ref.at[b, came, pl.ds(first, half)], fwd_sem.at[1], orecv_sem.at[b], to * CORES + c).start()

    def send_o(b, slot, dev):
        src = ostage_vm.at[slot, pl.ds(dev * tok, tok)]
        away = lax.rem(dev // CORES - chip + chips, chips)

        @pl.when(dev == me)
        def _():
            pltpu.make_async_copy(src, o_ref.at[b, me], osend_sem.at[b]).start()

        @pl.when(jnp.logical_and(dev != me, away != 2))
        def _():
            remote(src, o_ref.at[b, me], osend_sem.at[b], orecv_sem.at[b], dev).start()

        @pl.when(away == 2)
        def _():
            c = dev % CORES
            remote(ostage_vm.at[slot, pl.ds(dev * tok, half)], relo_ref.at[b, 0, c], osend_sem.at[b], relo_sem.at[b], right_dev).start()
            remote(ostage_vm.at[slot, pl.ds(dev * tok + half, half)], relo_ref.at[b, 1, c], osend_sem.at[b], relo_sem.at[b], left_dev).start()

    def new_row():
        def full(j):
            def col_tile(n, ssq):
                at = pl.ds(pl.multiple_of(n * COL_TILE, COL_TILE), COL_TILE)
                acc = jnp.dot(new_ref[...], w_vm[j, :, at], preferred_element_type=jnp.float32)
                return ssq + jnp.sum(acc * acc, axis=1, keepdims=True)

            ssq = lax.fori_loop(0, width // COL_TILE, col_tile, jnp.zeros((n_batch, 1), jnp.float32))
            return lax.rsqrt(ssq / width + NORM_EPS)

        own = pl.ds(pl.multiple_of(me * cols, cols), cols)
        for j, to in ((0, qnew_vm), (1, knew_ref)):
            inv = full(j)
            raw = jnp.dot(new_ref[...], w_vm[j, :, own], preferred_element_type=jnp.float32)
            normed = raw * inv * gains_ref[j:j + 1, own]
            for h in range(heads):
                at = slice(h * HEAD_DIM, (h + 1) * HEAD_DIM)
                to[:, at] = rotate(normed[:, at], cosd_ref[...], sind_ref[...]).astype(jnp.bfloat16)
        vnew_ref[...] = jnp.dot(new_ref[...], w_vm[2, :, own], preferred_element_type=jnp.float32).astype(jnp.bfloat16)
        deco_vm[...] = jnp.zeros_like(deco_vm)

    def attend(b):
        slot = lax.rem(b, 2)
        drain(qkv_ref.at[:, b], recv_sem.at[b])
        load = pltpu.make_async_copy(qkv_ref.at[:, b], qkv_vm, load_sem)
        load.start()

        @pl.when(b >= 2)
        def _():
            drain(ostage_vm.at[slot], osend_sem.at[b - 2])

        load.wait()
        keep = lax.broadcasted_iota(jnp.int32, (tok, tok), 0) >= lax.broadcasted_iota(jnp.int32, (tok, tok), 1)
        contract_last = (((1,), (1,)), ((), ()))
        for blk in range(group_n):
            rows = slice(blk * tok, (blk + 1) * tok)

            def one_head(h, _):
                at = pl.ds(pl.multiple_of(h * HEAD_DIM, HEAD_DIM), HEAD_DIM)
                q = qkv_vm[0, rows, at]
                diag = lax.dot_general(q, qkv_vm[1, rows, at], contract_last, preferred_element_type=jnp.float32)
                diag = jnp.where(keep, diag, -jnp.inf)
                top = jnp.max(diag, axis=1, keepdims=True)
                if blk:
                    past = lax.dot_general(q, qkv_vm[1, :blk * tok, at], contract_last, preferred_element_type=jnp.float32)
                    top = jnp.maximum(top, jnp.max(past, axis=1, keepdims=True))
                    past = jnp.exp2((past - top) * scale2)
                diag = jnp.exp2((diag - top) * scale2)
                total = jnp.sum(diag, axis=1, keepdims=True)
                if blk:
                    total = total + jnp.sum(past, axis=1, keepdims=True)
                inv = 1.0 / total
                out = jnp.dot((diag * inv).astype(jnp.bfloat16), qkv_vm[2, rows, at], preferred_element_type=jnp.float32)
                if blk:
                    out = out + jnp.dot((past * inv).astype(jnp.bfloat16), qkv_vm[2, :blk * tok, at], preferred_element_type=jnp.float32)
                ostage_vm[slot, rows, at] = out.astype(jnp.bfloat16)
                return 0

            lax.fori_loop(0, heads, one_head, 0)
            send_o(b, slot, blk)

        mine = lax.broadcasted_iota(jnp.int32, (n_batch, HEAD_DIM), 0) == b
        for h in range(heads):
            at = slice(h * HEAD_DIM, (h + 1) * HEAD_DIM)
            q = qnew_vm[:, at]
            past = lax.dot_general(q, qkv_vm[1, :, at], contract_last, preferred_element_type=jnp.float32)
            last = jnp.sum(q.astype(jnp.float32) * knew_ref[:, at].astype(jnp.float32), axis=1, keepdims=True)
            top = jnp.maximum(jnp.max(past, axis=1, keepdims=True), last)
            past, last = jnp.exp2((past - top) * scale2), jnp.exp2((last - top) * scale2)
            inv = 1.0 / (jnp.sum(past, axis=1, keepdims=True) + last)
            out = jnp.dot((past * inv).astype(jnp.bfloat16), qkv_vm[2, :, at], preferred_element_type=jnp.float32)
            out = out + (last * inv).astype(jnp.bfloat16).astype(jnp.float32) * vnew_ref[:, at].astype(jnp.float32)
            deco_vm[:, at] = jnp.where(mine, out, deco_vm[:, at])

    def send_part():
        wo_copy.wait()
        part = jnp.dot(deco_vm[...].astype(jnp.bfloat16), wo_vm[...], preferred_element_type=jnp.float32)
        decp_vm[me] = part.astype(jnp.bfloat16)
        for step in range(1, group_n):
            remote(decp_vm.at[me], decp_vm.at[me], decs_sem, decr_sem, lax.rem(me + step, group_n)).start()

    def step(t, _):
        @pl.when(t < n_batch)
        def _():
            project(t)

        @pl.when(t == 1)
        def _():
            new_row()

        @pl.when(jnp.logical_and(t >= 1, t <= n_batch))
        def _():
            forward(t - 1)

        @pl.when(t >= 3)
        def _():
            forward_o(t - 3)

        @pl.when(jnp.logical_and(t >= 2, t <= n_batch + 1))
        def _():
            attend(t - 2)

        return 0

    lax.fori_loop(0, n_batch + 2, step, 0)
    send_part()
    forward_o(n_batch - 1)

    drain(decp_vm.at[pl.ds(0, group_n - 1)], decs_sem)
    drain(decp_vm.at[pl.ds(0, group_n - 1)], decr_sem)
    proj = decp_vm[0].astype(jnp.float32)
    for g in range(1, group_n):
        proj = proj + decp_vm[g].astype(jnp.float32)
    inv = lax.rsqrt(jnp.sum(proj * proj, axis=1, keepdims=True) / width + NORM_EPS)
    outd_ref[...] = (new_ref[...].astype(jnp.float32) + proj * inv * post_ref[...]).astype(jnp.bfloat16)

    for t in range(n_batch - SLOTS, n_batch):
        drain_sends(t)
    for b in range(n_batch - 2, n_batch):
        drain(ostage_vm.at[b % 2], osend_sem.at[b])
    drain(rel_ref, fwd_sem.at[0])
    drain(relo_ref, fwd_sem.at[1])
    for b in range(n_batch):
        drain(o_ref.at[b, pl.ds(0, group_n - 1)], orecv_sem.at[b])


def output_kernel(o_ref, x_ref, wo_ref, post_ref, k_ref, v_ref, knew_ref, vnew_ref, out_ref, kc_ref, vc_ref, raw_vm):
    group_n, tok, cols = o_ref.shape[1:]
    width = group_n * cols
    heads = cols // HEAD_DIM
    o_all = jnp.concatenate([o_ref[0, g] for g in range(group_n)], axis=1)
    ssq = jnp.zeros((tok, 1), jnp.float32)
    for n in range(width // COL_TILE):
        at = slice(n * COL_TILE, (n + 1) * COL_TILE)
        acc = jnp.dot(o_all, wo_ref[:, at], preferred_element_type=jnp.float32)
        raw_vm[:, at] = acc
        ssq = ssq + jnp.sum(acc * acc, axis=1, keepdims=True)
    inv = lax.rsqrt(ssq / width + NORM_EPS)
    out_ref[0] = (x_ref[0].astype(jnp.float32) + raw_vm[...] * inv * post_ref[...]).astype(jnp.bfloat16)
    seq = k_ref.shape[2]
    for src, new, to in ((k_ref, knew_ref, kc_ref), (v_ref, vnew_ref, vc_ref)):
        to[0, :seq] = src[0, 0].reshape(seq, heads, HEAD_DIM)
        to[0, seq:] = new[0].reshape(1, heads, HEAD_DIM)


def solution(mesh):
    group_n = mesh.shape["sp"]

    def device_step(prompt_blk, w_q, w_k, w_v, w_o, q_norm_w, k_norm_w, post_norm_w, new_rows):
        n_batch, tok, width = prompt_blk.shape
        cols = width // group_n
        heads = cols // HEAD_DIM
        seq = tok * group_n
        half = tok // 2
        bf16, f32 = jnp.bfloat16, jnp.float32
        cos_p, sin_p = rope_tables(lax.axis_index("sp") * tok + jnp.arange(tok))
        cos_d, sin_d = rope_tables(jnp.full((1,), seq))
        gains = jnp.stack([q_norm_w, k_norm_w])
        post = post_norm_w[None]
        any_spec = pl.BlockSpec(memory_space=pl.ANY)
        vm_spec = pl.BlockSpec(memory_space=pltpu.VMEM)
        dma = pltpu.SemaphoreType.DMA
        qkv, o_all, _, _, k_new, v_new, out_d = pl.pallas_call(
            functools.partial(exchange_kernel, group_n),
            out_shape=(
                jax.ShapeDtypeStruct((3, n_batch, seq, cols), bf16),
                jax.ShapeDtypeStruct((n_batch, group_n, tok, cols), bf16),
                jax.ShapeDtypeStruct((n_batch, 2, CORES, 3, half, cols), bf16),
                jax.ShapeDtypeStruct((n_batch, 2, CORES, half, cols), bf16),
                jax.ShapeDtypeStruct((n_batch, cols), bf16),
                jax.ShapeDtypeStruct((n_batch, cols), bf16),
                jax.ShapeDtypeStruct((n_batch, width), bf16),
            ),
            in_specs=[any_spec] * 5 + [vm_spec] * 7,
            out_specs=(any_spec,) * 4 + (vm_spec,) * 3,
            scratch_shapes=[
                pltpu.VMEM((3, width, width), bf16),
                pltpu.VMEM((2, tok, width), bf16),
                pltpu.VMEM((tok, width), f32),
                pltpu.VMEM((tok, HEAD_DIM), f32),
                pltpu.VMEM((SLOTS, 3, group_n, tok, cols), bf16),
                pltpu.VMEM((3, seq, cols), bf16),
                pltpu.VMEM((2, seq, cols), bf16),
                pltpu.VMEM((cols, width), bf16),
                pltpu.VMEM((n_batch, cols), bf16),
                pltpu.VMEM((n_batch, cols), f32),
                pltpu.VMEM((group_n, n_batch, width), bf16),
                dma((3,)), dma((2,)), dma,
                dma((n_batch,)), dma((n_batch,)), dma((n_batch,)), dma((2,)), dma,
                dma((n_batch,)), dma((n_batch,)), dma((n_batch,)), dma, dma,
            ],
            compiler_params=pltpu.CompilerParams(collective_id=0, has_side_effects=True, vmem_limit_bytes=VMEM_BYTES),
        )(prompt_blk, w_q, w_k, w_v, w_o, gains, post, cos_p, sin_p, cos_d, sin_d, new_rows)

        row = lambda shape, at: pl.BlockSpec((1,) + shape, lambda b: (b,) + at)
        out_p, k_cache, v_cache = pl.pallas_call(
            output_kernel,
            grid=(n_batch,),
            out_shape=(
                jax.ShapeDtypeStruct((n_batch, tok, width), bf16),
                jax.ShapeDtypeStruct((n_batch, seq + 1, heads, HEAD_DIM), bf16),
                jax.ShapeDtypeStruct((n_batch, seq + 1, heads, HEAD_DIM), bf16),
            ),
            in_specs=[
                row((group_n, tok, cols), (0, 0, 0)),
                row((tok, width), (0, 0)),
                vm_spec,
                vm_spec,
                pl.BlockSpec((1, 1, seq, cols), lambda b: (1, b, 0, 0)),
                pl.BlockSpec((1, 1, seq, cols), lambda b: (2, b, 0, 0)),
                row((1, cols), (0, 0)),
                row((1, cols), (0, 0)),
            ],
            out_specs=(row((tok, width), (0, 0)), row((seq + 1, heads, HEAD_DIM), (0, 0, 0)), row((seq + 1, heads, HEAD_DIM), (0, 0, 0))),
            scratch_shapes=[pltpu.VMEM((tok, width), f32)],
            compiler_params=pltpu.CompilerParams(vmem_limit_bytes=VMEM_BYTES),
        )(o_all, prompt_blk, w_o, post, qkv, qkv, k_new[:, None], v_new[:, None])
        return out_p, k_cache, v_cache, out_d

    replicated = P()
    return jax.shard_map(
        device_step, mesh=mesh,
        in_specs=(P("dp", "sp", None), replicated, replicated, replicated, replicated, replicated, replicated, replicated, P("dp", None)),
        out_specs=(P("dp", "sp", None), P("dp", None, "sp", None), P("dp", None, "sp", None), P("dp", None)),
        check_vma=False)
```

```python
import functools

import jax
import jax.numpy as jnp
from jax import lax
from jax.experimental import pallas as pl
from jax.experimental.pallas import tpu as pltpu
from jax.sharding import PartitionSpec as P

HEAD_DIM = 128
ROPE_THETA = 500000.0
NORM_EPS = 1e-6
CORES = 2
LOG2E = 1.4426950408889634
SLOTS = 3
COL_TILE = 512
VMEM_BYTES = 66_000_000


def rope_tables(positions):
    inv_freq = ROPE_THETA ** (-jnp.arange(0, HEAD_DIM, 2).astype(jnp.float32) / HEAD_DIM)
    angles = positions.astype(jnp.float32)[:, None] * inv_freq[None, :]
    cos_t, sin_t = jnp.cos(angles), jnp.sin(angles)
    return jnp.concatenate([cos_t, cos_t], axis=-1), jnp.concatenate([-sin_t, sin_t], axis=-1)


def rotate(values, cos_t, sin_t):
    return values * cos_t + pltpu.roll(values, HEAD_DIM // 2, 1) * sin_t


def exchange_kernel(group_n, x_hbm, wq_hbm, wk_hbm, wv_hbm, wo_hbm, gains_ref, post_ref, cos_ref, sin_ref, cosd_ref, sind_ref, new_ref,
                    qkv_ref, o_ref, relkv_ref, relq_ref, relo_ref, kvp_ref, knew_ref, vnew_ref, outd_ref,
                    w_vm, x_vm, raw_vm, ssq_vm, stage_vm, qkv_vm, ostage_vm, kvp_vm, olocal_vm, wo_vm, qnew_vm, deco_vm, decp_vm,
                    w_sem, x_sem, wo_sem, send_sem, recvkv_sem, recvq_sem, relkv_sem, relq_sem, relo_sem, fwdkv_sem, fwdq_sem, fwdo_sem,
                    load_sem, osend_sem, orecv_sem, kvps_sem, kvpr_sem, kvpl_sem, olocal_sem, decs_sem, decr_sem):
    n_batch, tok, width = x_hbm.shape
    cols = width // group_n
    heads = cols // HEAD_DIM
    first_rows = CORES * tok
    chips = group_n // CORES
    me = lax.axis_index("sp")
    chip, core = me // CORES, me % CORES
    right = (chip + 1) % chips
    left = (chip + chips - 1) % chips
    far = (chip + 2) % chips
    right_dev, left_dev = right * CORES + core, left * CORES + core
    partner = chip * CORES + (1 - core)
    on_first = chip == 0
    w_hbm = (wq_hbm, wk_hbm, wv_hbm)
    scale2 = HEAD_DIM ** -0.5 * LOG2E
    contract_last = (((1,), (1,)), ((), ()))

    def remote(src, dst, s_sem, r_sem, dev):
        return pltpu.make_async_remote_copy(src_ref=src, dst_ref=dst, send_sem=s_sem, recv_sem=r_sem,
                                            device_id={"sp": dev}, device_id_type=pl.DeviceIdType.MESH)

    def drain(ref, sem):
        pltpu.make_async_copy(ref, ref, sem).wait()

    def with_split(source, use):
        mid, shift = tok // 2, tok // 8
        for n, holds in ((mid - shift, source == 1), (mid + shift, source == chips - 1), (mid, source % 2 == 0)):
            @pl.when(holds)
            def _():
                use(n)

    def w_copy(j):
        return pltpu.make_async_copy(w_hbm[j], w_vm.at[j], w_sem.at[j])

    def x_copy(t):
        return pltpu.make_async_copy(x_hbm.at[t], x_vm.at[lax.rem(t, 2)], x_sem.at[lax.rem(t, 2)])

    x_copy(0).start()
    for j in (2, 1, 0):
        w_copy(j).start()
    wo_copy = pltpu.make_async_copy(wo_hbm.at[pl.ds(me * cols, cols)], wo_vm, wo_sem)
    wo_copy.start()

    barrier = pltpu.get_barrier_semaphore()
    for step in range(1, group_n):
        pl.semaphore_signal(barrier, inc=1, device_id={"sp": lax.rem(me + step, group_n)}, device_id_type=pl.DeviceIdType.MESH)
    pl.semaphore_wait(barrier, group_n - 1)

    def send_tensor(t, slot, j):
        rows = pl.ds(me * tok, tok)
        far_devs = pl.ds(far * CORES, CORES)
        recv = recvkv_sem.at[t] if j else recvq_sem.at[t]

        def two_hops(n):
            for way, at, dev in ((0, pl.ds(0, n), right_dev), (1, pl.ds(n, tok - n), left_dev)):
                dst, sem = (relkv_ref.at[t, way, :, j - 1, at], relkv_sem.at[t, way]) if j else (relq_ref.at[t, way, :, at], relq_sem.at[t, way])
                remote(stage_vm.at[slot, j, far_devs, at], dst, send_sem.at[t], sem, dev).start()

        with_split(chip, two_hops)
        for side in (right, left):
            for c in range(CORES):
                dev = side * CORES + c
                remote(stage_vm.at[slot, j, dev], qkv_ref.at[j, t, rows], send_sem.at[t], recv, dev).start()
        remote(stage_vm.at[slot, j, partner], qkv_ref.at[j, t, rows], send_sem.at[t], recv, partner).start()
        pltpu.make_async_copy(stage_vm.at[slot, j, me], qkv_ref.at[j, t, rows], recv).start()

    def drain_sends(t):
        slot = lax.rem(t, SLOTS)

        @pl.when(on_first)
        def _():
            drain(stage_vm.at[slot, pl.ds(1, 2), pl.ds(0, group_n - 1)], send_sem.at[t])

        @pl.when(jnp.logical_not(on_first))
        def _():
            drain(stage_vm.at[slot, :, pl.ds(0, group_n - 1)], send_sem.at[t])

        @pl.when(me == 0)
        def _():
            drain(stage_vm.at[slot, pl.ds(1, 2)], kvps_sem.at[t])

    def project(t):
        slot = lax.rem(t, SLOTS)

        @pl.when(t >= SLOTS)
        def _():
            drain_sends(t - SLOTS)

        x_copy(t).wait()

        @pl.when(t + 1 < n_batch)
        def _():
            x_copy(t + 1).start()

        x_slot = lax.rem(t, 2)
        for j in (2, 1, 0):
            @pl.when(t == 0)
            def _():
                w_copy(j).wait()

            if j < 2:
                ssq_vm[...] = jnp.zeros_like(ssq_vm)

            def col_tile(n, _):
                at = pl.ds(pl.multiple_of(n * COL_TILE, COL_TILE), COL_TILE)
                acc = jnp.dot(x_vm[x_slot], w_vm[j, :, at], preferred_element_type=jnp.float32)
                if j < 2:
                    raw_vm[:, at] = acc
                    sq = acc * acc
                    ssq_vm[...] += sum(sq[:, i * HEAD_DIM:(i + 1) * HEAD_DIM] for i in range(COL_TILE // HEAD_DIM))
                else:
                    for i in range(COL_TILE // cols):
                        stage_vm[slot, j, n * (COL_TILE // cols) + i] = acc[:, i * cols:(i + 1) * cols].astype(jnp.bfloat16)
                return 0

            lax.fori_loop(0, width // COL_TILE, col_tile, 0)
            if j < 2:
                inv = lax.rsqrt(jnp.sum(ssq_vm[...], axis=1, keepdims=True) / width + NORM_EPS)

                def group_tile(n, _):
                    for h in range(heads):
                        at = pl.ds(pl.multiple_of(n * cols + h * HEAD_DIM, HEAD_DIM), HEAD_DIM)
                        normed = raw_vm[:, at] * inv * gains_ref[j:j + 1, at]
                        stage_vm[slot, j, n, :, h * HEAD_DIM:(h + 1) * HEAD_DIM] = rotate(normed, cos_ref[...], sin_ref[...]).astype(jnp.bfloat16)
                    return 0

                lax.fori_loop(0, group_n, group_tile, 0)
            if j:
                send_tensor(t, slot, j)
            else:
                @pl.when(jnp.logical_not(on_first))
                def _():
                    send_tensor(t, slot, j)

        @pl.when(me == 0)
        def _():
            remote(stage_vm.at[slot, pl.ds(1, 2)], kvp_ref.at[t], kvps_sem.at[t], kvpr_sem.at[t], partner).start()

    def relay_ways(use):
        with_split(left, lambda n: use(0, left, left_dev, right, 0, n))
        with_split(right, lambda n: use(1, right, right_dev, left, n, tok - n))

    def forward(b):
        def way_kv(way, source, source_dev, to, first, n):
            at, dst_rows = pl.ds(first, n), pl.ds(source_dev * tok + first, n)
            drain(relkv_ref.at[b, way, :, :, at], relkv_sem.at[b, way])
            for c in range(CORES):
                remote(relkv_ref.at[b, way, c, :, at], qkv_ref.at[pl.ds(1, 2), b, dst_rows], fwdkv_sem.at[way], recvkv_sem.at[b], to * CORES + c).start()

            @pl.when(source != 0)
            def _():
                drain(relq_ref.at[b, way, :, at], relq_sem.at[b, way])
                for c in range(CORES):
                    remote(relq_ref.at[b, way, c, at], qkv_ref.at[0, b, dst_rows], fwdq_sem.at[way], recvq_sem.at[b], to * CORES + c).start()

        relay_ways(way_kv)

    def forward_o(b):
        def way_o(way, source, source_dev, to, first, n):
            at = pl.ds(first, n)

            @pl.when(to != 0)
            def _():
                drain(relo_ref.at[b, way, :, at], relo_sem.at[b, way])
                for c in range(CORES):
                    remote(relo_ref.at[b, way, c, at], o_ref.at[b, source_dev, at], fwdo_sem.at[way], orecv_sem.at[b], to * CORES + c).start()

        relay_ways(way_o)

    def drain_forwards():
        def way_all(way, source, source_dev, to, first, n):
            at = pl.ds(first, n)
            drain(relkv_ref.at[:, way, :, :, at], fwdkv_sem.at[way])

            @pl.when(source != 0)
            def _():
                drain(relq_ref.at[:, way, :, at], fwdq_sem.at[way])

            @pl.when(to != 0)
            def _():
                drain(relo_ref.at[:, way, :, at], fwdo_sem.at[way])

        relay_ways(way_all)

    def send_o(b, slot, dev):
        src = ostage_vm.at[slot, pl.ds(dev * tok, tok)]
        c = dev % CORES
        away = lax.rem(dev // CORES - chip + chips, chips)

        @pl.when(dev == me)
        def _():
            pltpu.make_async_copy(src, o_ref.at[b, me], osend_sem.at[b]).start()

        @pl.when(jnp.logical_and(dev != me, away != 2))
        def _():
            remote(src, o_ref.at[b, me], osend_sem.at[b], orecv_sem.at[b], dev).start()

        @pl.when(away == 2)
        def _():
            def two_hops(n):
                remote(ostage_vm.at[slot, pl.ds(dev * tok, n)], relo_ref.at[b, 0, c, pl.ds(0, n)],
                       osend_sem.at[b], relo_sem.at[b, 0], right_dev).start()
                remote(ostage_vm.at[slot, pl.ds(dev * tok + n, tok - n)], relo_ref.at[b, 1, c, pl.ds(n, tok - n)],
                       osend_sem.at[b], relo_sem.at[b, 1], left_dev).start()

            with_split(chip, two_hops)

    def drain_o_sends(b):
        drain(ostage_vm.at[lax.rem(b, 2), pl.ds(first_rows, (group_n - CORES) * tok)], osend_sem.at[b])

    def new_row():
        def full(j):
            def col_tile(n, ssq):
                at = pl.ds(pl.multiple_of(n * COL_TILE, COL_TILE), COL_TILE)
                acc = jnp.dot(new_ref[...], w_vm[j, :, at], preferred_element_type=jnp.float32)
                return ssq + jnp.sum(acc * acc, axis=1, keepdims=True)

            ssq = lax.fori_loop(0, width // COL_TILE, col_tile, jnp.zeros((n_batch, 1), jnp.float32))
            return lax.rsqrt(ssq / width + NORM_EPS)

        own = pl.ds(pl.multiple_of(me * cols, cols), cols)
        for j, to in ((0, qnew_vm), (1, knew_ref)):
            inv = full(j)
            raw = jnp.dot(new_ref[...], w_vm[j, :, own], preferred_element_type=jnp.float32)
            normed = raw * inv * gains_ref[j:j + 1, own]
            for h in range(heads):
                at = slice(h * HEAD_DIM, (h + 1) * HEAD_DIM)
                to[:, at] = rotate(normed[:, at], cosd_ref[...], sind_ref[...]).astype(jnp.bfloat16)
        vnew_ref[...] = jnp.dot(new_ref[...], w_vm[2, :, own], preferred_element_type=jnp.float32).astype(jnp.bfloat16)
        deco_vm[...] = jnp.zeros_like(deco_vm)

    def block_attention(q, k_diag, v_diag, k_past, v_past):
        keep = lax.broadcasted_iota(jnp.int32, (tok, tok), 0) >= lax.broadcasted_iota(jnp.int32, (tok, tok), 1)
        diag = lax.dot_general(q, k_diag, contract_last, preferred_element_type=jnp.float32)
        diag = jnp.where(keep, diag, -jnp.inf)
        top = jnp.max(diag, axis=1, keepdims=True)
        if k_past is not None:
            past = lax.dot_general(q, k_past, contract_last, preferred_element_type=jnp.float32)
            top = jnp.maximum(top, jnp.max(past, axis=1, keepdims=True))
            past = jnp.exp2((past - top) * scale2)
        diag = jnp.exp2((diag - top) * scale2)
        total = jnp.sum(diag, axis=1, keepdims=True)
        if k_past is not None:
            total = total + jnp.sum(past, axis=1, keepdims=True)
        inv = 1.0 / total
        out = jnp.dot((diag * inv).astype(jnp.bfloat16), v_diag, preferred_element_type=jnp.float32)
        if k_past is not None:
            out = out + jnp.dot((past * inv).astype(jnp.bfloat16), v_past, preferred_element_type=jnp.float32)
        return out.astype(jnp.bfloat16)

    def attend_first(b):
        slot = lax.rem(b, SLOTS)

        @pl.when(b >= 1)
        def _():
            drain(olocal_vm, olocal_sem)

        for which in range(CORES):
            @pl.when(core == which)
            def _():
                if which:
                    drain(kvp_ref.at[b], kvpr_sem.at[b])
                    load = pltpu.make_async_copy(kvp_ref.at[b], kvp_vm, kvpl_sem)
                    load.start()
                    load.wait()

                def group(g, _):
                    for h in range(heads):
                        at = slice(h * HEAD_DIM, (h + 1) * HEAD_DIM)
                        past = (kvp_vm[0, g, :, at], kvp_vm[1, g, :, at]) if which else (None, None)
                        olocal_vm[g, :, at] = block_attention(stage_vm[slot, 0, g, :, at], stage_vm[slot, 1, g, :, at], stage_vm[slot, 2, g, :, at], *past)
                    return 0

                lax.fori_loop(0, group_n, group, 0)

        pltpu.make_async_copy(olocal_vm, o_ref.at[b], olocal_sem).start()

    def attend(b):
        slot = lax.rem(b, 2)
        q_rows = pl.ds(first_rows, (group_n - CORES) * tok)
        drain(qkv_ref.at[pl.ds(1, 2), b], recvkv_sem.at[b])
        drain(qkv_ref.at[0, b, q_rows], recvq_sem.at[b])
        load_kv = pltpu.make_async_copy(qkv_ref.at[pl.ds(1, 2), b], qkv_vm.at[pl.ds(1, 2)], load_sem.at[0])
        load_q = pltpu.make_async_copy(qkv_ref.at[0, b, q_rows], qkv_vm.at[0, q_rows], load_sem.at[1])
        load_kv.start()
        load_q.start()

        @pl.when(b >= 2)
        def _():
            drain_o_sends(b - 2)

        load_kv.wait()
        load_q.wait()
        for blk in range(CORES, group_n):
            rows = slice(blk * tok, (blk + 1) * tok)

            def one_head(h, _):
                at = pl.ds(pl.multiple_of(h * HEAD_DIM, HEAD_DIM), HEAD_DIM)
                ostage_vm[slot, rows, at] = block_attention(qkv_vm[0, rows, at], qkv_vm[1, rows, at], qkv_vm[2, rows, at],
                                                            qkv_vm[1, :blk * tok, at], qkv_vm[2, :blk * tok, at])
                return 0

            lax.fori_loop(0, heads, one_head, 0)
            send_o(b, slot, blk)

        mine = lax.broadcasted_iota(jnp.int32, (n_batch, HEAD_DIM), 0) == b
        for h in range(heads):
            at = slice(h * HEAD_DIM, (h + 1) * HEAD_DIM)
            q = qnew_vm[:, at]
            past = lax.dot_general(q, qkv_vm[1, :, at], contract_last, preferred_element_type=jnp.float32)
            last = jnp.sum(q.astype(jnp.float32) * knew_ref[:, at].astype(jnp.float32), axis=1, keepdims=True)
            top = jnp.maximum(jnp.max(past, axis=1, keepdims=True), last)
            past, last = jnp.exp2((past - top) * scale2), jnp.exp2((last - top) * scale2)
            inv = 1.0 / (jnp.sum(past, axis=1, keepdims=True) + last)
            out = jnp.dot((past * inv).astype(jnp.bfloat16), qkv_vm[2, :, at], preferred_element_type=jnp.float32)
            out = out + (last * inv).astype(jnp.bfloat16).astype(jnp.float32) * vnew_ref[:, at].astype(jnp.float32)
            deco_vm[:, at] = jnp.where(mine, out, deco_vm[:, at])

    def send_part():
        wo_copy.wait()
        part = jnp.dot(deco_vm[...].astype(jnp.bfloat16), wo_vm[...], preferred_element_type=jnp.float32)
        decp_vm[me] = part.astype(jnp.bfloat16)
        for step in range(1, group_n):
            remote(decp_vm.at[me], decp_vm.at[me], decs_sem, decr_sem, lax.rem(me + step, group_n)).start()

    def step(t, _):
        @pl.when(t < n_batch)
        def _():
            project(t)

        @pl.when(t == 1)
        def _():
            new_row()

        @pl.when(jnp.logical_and(t >= 1, t <= n_batch))
        def _():
            forward(t - 1)

        @pl.when(t >= 3)
        def _():
            forward_o(t - 3)

        @pl.when(jnp.logical_and(on_first, jnp.logical_and(t >= 1, t <= n_batch)))
        def _():
            attend_first(t - 1)

        @pl.when(jnp.logical_and(t >= 2, t <= n_batch + 1))
        def _():
            attend(t - 2)

        return 0

    lax.fori_loop(0, n_batch + 2, step, 0)
    send_part()
    forward_o(n_batch - 1)

    drain(decp_vm.at[pl.ds(0, group_n - 1)], decs_sem)
    drain(decp_vm.at[pl.ds(0, group_n - 1)], decr_sem)
    proj = decp_vm[0].astype(jnp.float32)
    for g in range(1, group_n):
        proj = proj + decp_vm[g].astype(jnp.float32)
    inv = lax.rsqrt(jnp.sum(proj * proj, axis=1, keepdims=True) / width + NORM_EPS)
    outd_ref[...] = (new_ref[...].astype(jnp.float32) + proj * inv * post_ref[...]).astype(jnp.bfloat16)

    for t in range(n_batch - SLOTS, n_batch):
        drain_sends(t)
    for b in range(n_batch - 2, n_batch):
        drain_o_sends(b)
    drain_forwards()

    @pl.when(on_first)
    def _():
        drain(olocal_vm, olocal_sem)

    @pl.when(jnp.logical_not(on_first))
    def _():
        for b in range(n_batch):
            drain(o_ref.at[b, pl.ds(0, group_n - 1)], orecv_sem.at[b])


def output_kernel(o_ref, x_ref, wo_ref, post_ref, k_ref, v_ref, knew_ref, vnew_ref, out_ref, kc_ref, vc_ref, raw_vm):
    n_seq, group_n, tok, cols = o_ref.shape
    width = group_n * cols
    heads = cols // HEAD_DIM
    o_all = jnp.concatenate([o_ref[:, g].reshape(n_seq * tok, cols) for g in range(group_n)], axis=1)
    ssq = jnp.zeros((n_seq * tok, 1), jnp.float32)
    for n in range(width // COL_TILE):
        at = slice(n * COL_TILE, (n + 1) * COL_TILE)
        acc = jnp.dot(o_all, wo_ref[:, at], preferred_element_type=jnp.float32)
        raw_vm[:, at] = acc
        ssq = ssq + jnp.sum(acc * acc, axis=1, keepdims=True)
    inv = lax.rsqrt(ssq / width + NORM_EPS)
    for i in range(n_seq):
        at = slice(i * tok, (i + 1) * tok)
        out_ref[i] = (x_ref[i].astype(jnp.float32) + raw_vm[at] * inv[at] * post_ref[...]).astype(jnp.bfloat16)
    seq = k_ref.shape[2]
    for src, new, to in ((k_ref, knew_ref, kc_ref), (v_ref, vnew_ref, vc_ref)):
        for i in range(n_seq):
            to[i, :seq] = src[0, i].reshape(seq, heads, HEAD_DIM)
            to[i, seq:] = new[i].reshape(1, heads, HEAD_DIM)


def solution(mesh):
    group_n = mesh.shape["sp"]

    def device_step(prompt_blk, w_q, w_k, w_v, w_o, q_norm_w, k_norm_w, post_norm_w, new_rows):
        n_batch, tok, width = prompt_blk.shape
        cols = width // group_n
        heads = cols // HEAD_DIM
        seq = tok * group_n
        bf16, f32 = jnp.bfloat16, jnp.float32
        cos_p, sin_p = rope_tables(lax.axis_index("sp") * tok + jnp.arange(tok))
        cos_d, sin_d = rope_tables(jnp.full((1,), seq))
        gains = jnp.stack([q_norm_w, k_norm_w])
        post = post_norm_w[None]
        any_spec = pl.BlockSpec(memory_space=pl.ANY)
        vm_spec = pl.BlockSpec(memory_space=pltpu.VMEM)
        dma = pltpu.SemaphoreType.DMA
        qkv, o_all, _, _, _, _, k_new, v_new, out_d = pl.pallas_call(
            functools.partial(exchange_kernel, group_n),
            out_shape=(
                jax.ShapeDtypeStruct((3, n_batch, seq, cols), bf16),
                jax.ShapeDtypeStruct((n_batch, group_n, tok, cols), bf16),
                jax.ShapeDtypeStruct((n_batch, 2, CORES, 2, tok, cols), bf16),
                jax.ShapeDtypeStruct((n_batch, 2, CORES, tok, cols), bf16),
                jax.ShapeDtypeStruct((n_batch, 2, CORES, tok, cols), bf16),
                jax.ShapeDtypeStruct((n_batch, 2, group_n, tok, cols), bf16),
                jax.ShapeDtypeStruct((n_batch, cols), bf16),
                jax.ShapeDtypeStruct((n_batch, cols), bf16),
                jax.ShapeDtypeStruct((n_batch, width), bf16),
            ),
            in_specs=[any_spec] * 5 + [vm_spec] * 7,
            out_specs=(any_spec,) * 6 + (vm_spec,) * 3,
            scratch_shapes=[
                pltpu.VMEM((3, width, width), bf16),
                pltpu.VMEM((2, tok, width), bf16),
                pltpu.VMEM((tok, width), f32),
                pltpu.VMEM((tok, HEAD_DIM), f32),
                pltpu.VMEM((SLOTS, 3, group_n, tok, cols), bf16),
                pltpu.VMEM((3, seq, cols), bf16),
                pltpu.VMEM((2, seq, cols), bf16),
                pltpu.VMEM((2, group_n, tok, cols), bf16),
                pltpu.VMEM((group_n, tok, cols), bf16),
                pltpu.VMEM((cols, width), bf16),
                pltpu.VMEM((n_batch, cols), bf16),
                pltpu.VMEM((n_batch, cols), f32),
                pltpu.VMEM((group_n, n_batch, width), bf16),
                dma((3,)), dma((2,)), dma,
                dma((n_batch,)), dma((n_batch,)), dma((n_batch,)), dma((n_batch, 2)), dma((n_batch, 2)), dma((n_batch, 2)), dma((2,)), dma((2,)), dma((2,)),
                dma((2,)), dma((n_batch,)), dma((n_batch,)), dma((n_batch,)), dma((n_batch,)), dma, dma, dma, dma,
            ],
            compiler_params=pltpu.CompilerParams(collective_id=0, has_side_effects=True, vmem_limit_bytes=VMEM_BYTES),
        )(prompt_blk, w_q, w_k, w_v, w_o, gains, post, cos_p, sin_p, cos_d, sin_d, new_rows)

        pair = 2 if n_batch % 2 == 0 else 1
        row = lambda shape, at: pl.BlockSpec((pair,) + shape, lambda b: (b,) + at)
        out_p, k_cache, v_cache = pl.pallas_call(
            output_kernel,
            grid=(n_batch // pair,),
            out_shape=(
                jax.ShapeDtypeStruct((n_batch, tok, width), bf16),
                jax.ShapeDtypeStruct((n_batch, seq + 1, heads, HEAD_DIM), bf16),
                jax.ShapeDtypeStruct((n_batch, seq + 1, heads, HEAD_DIM), bf16),
            ),
            in_specs=[
                row((group_n, tok, cols), (0, 0, 0)),
                row((tok, width), (0, 0)),
                vm_spec,
                vm_spec,
                pl.BlockSpec((1, pair, seq, cols), lambda b: (1, b, 0, 0)),
                pl.BlockSpec((1, pair, seq, cols), lambda b: (2, b, 0, 0)),
                row((1, cols), (0, 0)),
                row((1, cols), (0, 0)),
            ],
            out_specs=(row((tok, width), (0, 0)), row((seq + 1, heads, HEAD_DIM), (0, 0, 0)), row((seq + 1, heads, HEAD_DIM), (0, 0, 0))),
            scratch_shapes=[pltpu.VMEM((pair * tok, width), f32)],
            compiler_params=pltpu.CompilerParams(vmem_limit_bytes=VMEM_BYTES),
        )(o_all, prompt_blk, w_o, post, qkv, qkv, k_new[:, None], v_new[:, None])
        return out_p, k_cache, v_cache, out_d

    replicated = P()
    return jax.shard_map(
        device_step, mesh=mesh,
        in_specs=(P("dp", "sp", None), replicated, replicated, replicated, replicated, replicated, replicated, replicated, P("dp", None)),
        out_specs=(P("dp", "sp", None), P("dp", None, "sp", None), P("dp", None, "sp", None), P("dp", None)),
        check_vma=False)
```

```python
import functools

import jax
import jax.numpy as jnp
from jax import lax
from jax.experimental import pallas as pl
from jax.experimental.pallas import tpu as pltpu
from jax.sharding import PartitionSpec as P

HEAD_DIM = 128
ROPE_THETA = 500000.0
NORM_EPS = 1e-6
CORES = 2
LOG2E = 1.4426950408889634
SLOTS = 3
LATE = 2
COL_TILE = 512
VMEM_BYTES = 66_000_000


def rope_tables(positions):
    lane = jnp.arange(HEAD_DIM) % (HEAD_DIM // 2)
    inv_freq = ROPE_THETA ** (-(2 * lane).astype(jnp.float32) / HEAD_DIM)
    angles = positions.astype(jnp.float32)[:, None] * inv_freq[None, :]
    sign = jnp.where(jnp.arange(HEAD_DIM) < HEAD_DIM // 2, -1.0, 1.0)
    return jnp.cos(angles), jnp.sin(angles) * sign[None, :]


def rotate(values, cos_t, sin_t):
    return values * cos_t + pltpu.roll(values, HEAD_DIM // 2, 1) * sin_t


def exchange_kernel(group_n, x_hbm, wq_hbm, wk_hbm, wv_hbm, wo_hbm, qgain_ref, kgain_ref, post_ref, cos_ref, sin_ref, new_ref,
                    qkv_ref, o_ref, relkv_ref, relq_ref, relo_ref, kvp_ref, outp_ref, knew_ref, vnew_ref, outd_ref,
                    w_vm, x_vm, raw_vm, ssq_vm, stage_vm, qkv_vm, ostage_vm, kvp_vm, olocal_vm, wo_vm, oin_vm, xo_vm, outv_vm, qnew_vm, knew_vm, vnew_vm, deco_vm, decp_vm,
                    w_sem, x_sem, wo_sem, send_sem, recvkv_sem, recvq_sem, relkv_sem, relq_sem, relo_sem, fwdkv_sem, fwdq_sem, fwdo_sem,
                    load_sem, osend_sem, orecv_sem, kvps_sem, kvpr_sem, kvpl_sem, olocal_sem, oin_sem, xo_sem, outv_sem, decs_sem, decr_sem):
    n_batch, tok, width = x_hbm.shape
    cols = width // group_n
    heads = cols // HEAD_DIM
    first_rows = CORES * tok
    chips = group_n // CORES
    me = lax.axis_index("sp")
    chip, core = me // CORES, me % CORES
    right = (chip + 1) % chips
    left = (chip + chips - 1) % chips
    far = (chip + 2) % chips
    right_dev, left_dev = right * CORES + core, left * CORES + core
    partner = chip * CORES + (1 - core)
    on_first = chip == 0
    w_hbm = (wq_hbm, wk_hbm, wv_hbm)
    gains = (qgain_ref, kgain_ref)
    scale2 = HEAD_DIM ** -0.5 * LOG2E
    contract_last = (((1,), (1,)), ((), ()))

    def remote(src, dst, s_sem, r_sem, dev):
        return pltpu.make_async_remote_copy(src_ref=src, dst_ref=dst, send_sem=s_sem, recv_sem=r_sem,
                                            device_id={"sp": dev}, device_id_type=pl.DeviceIdType.MESH)

    def drain(ref, sem):
        pltpu.make_async_copy(ref, ref, sem).wait()

    def with_split(source, use):
        mid, shift = tok // 2, tok // 8
        for n, holds in ((mid - shift, source == 1), (mid + shift, source == chips - 1), (mid, source % 2 == 0)):
            @pl.when(holds)
            def _():
                use(n)

    def w_copy(j):
        return pltpu.make_async_copy(w_hbm[j], w_vm.at[j], w_sem.at[j])

    def x_copy(t):
        return pltpu.make_async_copy(x_hbm.at[t], x_vm.at[lax.rem(t, 2)], x_sem.at[lax.rem(t, 2)])

    x_copy(0).start()
    for j in (2, 1, 0):
        w_copy(j).start()
    wo_copy = pltpu.make_async_copy(wo_hbm, wo_vm, wo_sem)
    wo_copy.start()

    barrier = pltpu.get_barrier_semaphore()
    for step in range(1, group_n):
        pl.semaphore_signal(barrier, inc=1, device_id={"sp": lax.rem(me + step, group_n)}, device_id_type=pl.DeviceIdType.MESH)
    pl.semaphore_wait(barrier, group_n - 1)

    def send_tensor(t, slot, j):
        rows = pl.ds(me * tok, tok)
        far_devs = pl.ds(far * CORES, CORES)
        recv = recvkv_sem.at[t] if j else recvq_sem.at[t]

        def two_hops(n):
            for way, at, dev in ((0, pl.ds(0, n), right_dev), (1, pl.ds(n, tok - n), left_dev)):
                dst, sem = (relkv_ref.at[t, way, :, j - 1, at], relkv_sem.at[t, way]) if j else (relq_ref.at[t, way, :, at], relq_sem.at[t, way])
                remote(stage_vm.at[slot, j, far_devs, at], dst, send_sem.at[t], sem, dev).start()

        with_split(chip, two_hops)
        for side in (right, left):
            for c in range(CORES):
                dev = side * CORES + c
                remote(stage_vm.at[slot, j, dev], qkv_ref.at[j, t, rows], send_sem.at[t], recv, dev).start()
        remote(stage_vm.at[slot, j, partner], qkv_ref.at[j, t, rows], send_sem.at[t], recv, partner).start()
        pltpu.make_async_copy(stage_vm.at[slot, j, me], qkv_ref.at[j, t, rows], recv).start()

    def drain_sends(t):
        slot = lax.rem(t, SLOTS)

        @pl.when(on_first)
        def _():
            drain(stage_vm.at[slot, pl.ds(1, 2), pl.ds(0, group_n - 1)], send_sem.at[t])

        @pl.when(jnp.logical_not(on_first))
        def _():
            drain(stage_vm.at[slot, :, pl.ds(0, group_n - 1)], send_sem.at[t])

        @pl.when(me == 0)
        def _():
            drain(stage_vm.at[slot, pl.ds(1, 2)], kvps_sem.at[t])

    def project(t):
        slot = lax.rem(t, SLOTS)

        @pl.when(t >= SLOTS)
        def _():
            drain_sends(t - SLOTS)

        x_copy(t).wait()

        @pl.when(t + 1 < n_batch)
        def _():
            x_copy(t + 1).start()

        x_slot = lax.rem(t, 2)
        for j in (2, 1, 0):
            @pl.when(t == 0)
            def _():
                w_copy(j).wait()

            if j < 2:
                ssq_vm[...] = jnp.zeros_like(ssq_vm)

            def col_tile(n, _):
                at = pl.ds(pl.multiple_of(n * COL_TILE, COL_TILE), COL_TILE)
                acc = jnp.dot(x_vm[x_slot], w_vm[j, :, at], preferred_element_type=jnp.float32)
                if j < 2:
                    raw_vm[:, at] = acc
                    sq = acc * acc
                    ssq_vm[...] += sum(sq[:, i * HEAD_DIM:(i + 1) * HEAD_DIM] for i in range(COL_TILE // HEAD_DIM))
                else:
                    for i in range(COL_TILE // cols):
                        stage_vm[slot, j, n * (COL_TILE // cols) + i] = acc[:, i * cols:(i + 1) * cols].astype(jnp.bfloat16)
                return 0

            lax.fori_loop(0, width // COL_TILE, col_tile, 0)
            if j < 2:
                inv = lax.rsqrt(jnp.sum(ssq_vm[...], axis=1, keepdims=True) / width + NORM_EPS)

                def group_tile(n, _):
                    for h in range(heads):
                        at = pl.ds(pl.multiple_of(n * cols + h * HEAD_DIM, HEAD_DIM), HEAD_DIM)
                        normed = raw_vm[:, at] * inv * gains[j][:, at]
                        stage_vm[slot, j, n, :, h * HEAD_DIM:(h + 1) * HEAD_DIM] = rotate(normed, cos_ref[:tok], sin_ref[:tok]).astype(jnp.bfloat16)
                    return 0

                lax.fori_loop(0, group_n, group_tile, 0)
            if j:
                send_tensor(t, slot, j)
            else:
                @pl.when(jnp.logical_not(on_first))
                def _():
                    send_tensor(t, slot, j)

        @pl.when(me == 0)
        def _():
            remote(stage_vm.at[slot, pl.ds(1, 2)], kvp_ref.at[t], kvps_sem.at[t], kvpr_sem.at[t], partner).start()

    def relay_ways(use):
        with_split(left, lambda n: use(0, left, left_dev, right, 0, n))
        with_split(right, lambda n: use(1, right, right_dev, left, n, tok - n))

    def forward(b):
        def way_kv(way, source, source_dev, to, first, n):
            at, dst_rows = pl.ds(first, n), pl.ds(source_dev * tok + first, n)
            drain(relkv_ref.at[b, way, :, :, at], relkv_sem.at[b, way])
            for c in range(CORES):
                remote(relkv_ref.at[b, way, c, :, at], qkv_ref.at[pl.ds(1, 2), b, dst_rows], fwdkv_sem.at[way], recvkv_sem.at[b], to * CORES + c).start()

            @pl.when(source != 0)
            def _():
                drain(relq_ref.at[b, way, :, at], relq_sem.at[b, way])
                for c in range(CORES):
                    remote(relq_ref.at[b, way, c, at], qkv_ref.at[0, b, dst_rows], fwdq_sem.at[way], recvq_sem.at[b], to * CORES + c).start()

        relay_ways(way_kv)

    def forward_o(b):
        def way_o(way, source, source_dev, to, first, n):
            at = pl.ds(first, n)

            @pl.when(to != 0)
            def _():
                drain(relo_ref.at[b, way, :, at], relo_sem.at[b, way])
                for c in range(CORES):
                    remote(relo_ref.at[b, way, c, at], o_ref.at[b, source_dev, at], fwdo_sem.at[way], orecv_sem.at[b], to * CORES + c).start()

        relay_ways(way_o)

    def drain_forwards():
        def way_all(way, source, source_dev, to, first, n):
            at = pl.ds(first, n)
            drain(relkv_ref.at[:, way, :, :, at], fwdkv_sem.at[way])

            @pl.when(source != 0)
            def _():
                drain(relq_ref.at[:, way, :, at], fwdq_sem.at[way])

            @pl.when(to != 0)
            def _():
                drain(relo_ref.at[:, way, :, at], fwdo_sem.at[way])

        relay_ways(way_all)

    def send_o(b, slot, dev):
        src = ostage_vm.at[slot, pl.ds(dev * tok, tok)]
        c = dev % CORES
        away = lax.rem(dev // CORES - chip + chips, chips)

        @pl.when(dev == me)
        def _():
            pltpu.make_async_copy(src, o_ref.at[b, me], osend_sem.at[b]).start()

        @pl.when(jnp.logical_and(dev != me, away != 2))
        def _():
            remote(src, o_ref.at[b, me], osend_sem.at[b], orecv_sem.at[b], dev).start()

        @pl.when(away == 2)
        def _():
            def two_hops(n):
                remote(ostage_vm.at[slot, pl.ds(dev * tok, n)], relo_ref.at[b, 0, c, pl.ds(0, n)],
                       osend_sem.at[b], relo_sem.at[b, 0], right_dev).start()
                remote(ostage_vm.at[slot, pl.ds(dev * tok + n, tok - n)], relo_ref.at[b, 1, c, pl.ds(n, tok - n)],
                       osend_sem.at[b], relo_sem.at[b, 1], left_dev).start()

            with_split(chip, two_hops)

    def drain_o_sends(b):
        drain(ostage_vm.at[lax.rem(b, 2), pl.ds(first_rows, (group_n - CORES) * tok)], osend_sem.at[b])

    def new_row():
        def full(j):
            def col_tile(n, ssq):
                at = pl.ds(pl.multiple_of(n * COL_TILE, COL_TILE), COL_TILE)
                acc = jnp.dot(new_ref[...], w_vm[j, :, at], preferred_element_type=jnp.float32)
                return ssq + jnp.sum(acc * acc, axis=1, keepdims=True)

            ssq = lax.fori_loop(0, width // COL_TILE, col_tile, jnp.zeros((n_batch, 1), jnp.float32))
            return lax.rsqrt(ssq / width + NORM_EPS)

        own = pl.ds(pl.multiple_of(me * cols, cols), cols)
        for j, to in ((0, qnew_vm), (1, knew_vm)):
            inv = full(j)
            raw = jnp.dot(new_ref[...], w_vm[j, :, own], preferred_element_type=jnp.float32)
            normed = raw * inv * gains[j][:, own]
            for h in range(heads):
                at = slice(h * HEAD_DIM, (h + 1) * HEAD_DIM)
                to[:, at] = rotate(normed[:, at], cos_ref[tok:tok + 1], sin_ref[tok:tok + 1]).astype(jnp.bfloat16)
        vnew_vm[...] = jnp.dot(new_ref[...], w_vm[2, :, own], preferred_element_type=jnp.float32).astype(jnp.bfloat16)
        for b in range(n_batch):
            knew_ref[b] = knew_vm[b:b + 1]
            vnew_ref[b] = vnew_vm[b:b + 1]
        deco_vm[...] = jnp.zeros_like(deco_vm)

    def block_attention(q, k_diag, v_diag, k_past, v_past):
        keep = lax.broadcasted_iota(jnp.int32, (tok, tok), 0) >= lax.broadcasted_iota(jnp.int32, (tok, tok), 1)
        diag = lax.dot_general(q, k_diag, contract_last, preferred_element_type=jnp.float32)
        diag = jnp.where(keep, diag, -jnp.inf)
        top = jnp.max(diag, axis=1, keepdims=True)
        if k_past is not None:
            past = lax.dot_general(q, k_past, contract_last, preferred_element_type=jnp.float32)
            top = jnp.maximum(top, jnp.max(past, axis=1, keepdims=True))
            past = jnp.exp2((past - top) * scale2)
        diag = jnp.exp2((diag - top) * scale2)
        total = jnp.sum(diag, axis=1, keepdims=True)
        if k_past is not None:
            total = total + jnp.sum(past, axis=1, keepdims=True)
        inv = 1.0 / total
        out = jnp.dot((diag * inv).astype(jnp.bfloat16), v_diag, preferred_element_type=jnp.float32)
        if k_past is not None:
            out = out + jnp.dot((past * inv).astype(jnp.bfloat16), v_past, preferred_element_type=jnp.float32)
        return out.astype(jnp.bfloat16)

    def attend_first(b):
        slot = lax.rem(b, SLOTS)

        @pl.when(b >= 1)
        def _():
            drain(olocal_vm, olocal_sem)

        for which in range(CORES):
            @pl.when(core == which)
            def _():
                if which:
                    drain(kvp_ref.at[b], kvpr_sem.at[b])
                    load = pltpu.make_async_copy(kvp_ref.at[b], kvp_vm, kvpl_sem)
                    load.start()
                    load.wait()

                def group(g, _):
                    for h in range(heads):
                        at = slice(h * HEAD_DIM, (h + 1) * HEAD_DIM)
                        past = (kvp_vm[0, g, :, at], kvp_vm[1, g, :, at]) if which else (None, None)
                        olocal_vm[g, :, at] = block_attention(stage_vm[slot, 0, g, :, at], stage_vm[slot, 1, g, :, at], stage_vm[slot, 2, g, :, at], *past)
                    return 0

                lax.fori_loop(0, group_n, group, 0)

        pltpu.make_async_copy(olocal_vm, o_ref.at[b], olocal_sem).start()

    def attend(b):
        slot = lax.rem(b, 2)
        q_rows = pl.ds(first_rows, (group_n - CORES) * tok)
        drain(qkv_ref.at[pl.ds(1, 2), b], recvkv_sem.at[b])
        drain(qkv_ref.at[0, b, q_rows], recvq_sem.at[b])
        load_kv = pltpu.make_async_copy(qkv_ref.at[pl.ds(1, 2), b], qkv_vm.at[pl.ds(1, 2)], load_sem.at[0])
        load_q = pltpu.make_async_copy(qkv_ref.at[0, b, q_rows], qkv_vm.at[0, q_rows], load_sem.at[1])
        load_kv.start()
        load_q.start()

        @pl.when(b >= 2)
        def _():
            drain_o_sends(b - 2)

        load_kv.wait()
        load_q.wait()
        for blk in range(CORES, group_n):
            rows = slice(blk * tok, (blk + 1) * tok)

            def one_head(h, _):
                at = pl.ds(pl.multiple_of(h * HEAD_DIM, HEAD_DIM), HEAD_DIM)
                ostage_vm[slot, rows, at] = block_attention(qkv_vm[0, rows, at], qkv_vm[1, rows, at], qkv_vm[2, rows, at],
                                                            qkv_vm[1, :blk * tok, at], qkv_vm[2, :blk * tok, at])
                return 0

            lax.fori_loop(0, heads, one_head, 0)
            send_o(b, slot, blk)

        mine = lax.broadcasted_iota(jnp.int32, (n_batch, HEAD_DIM), 0) == b
        for h in range(heads):
            at = slice(h * HEAD_DIM, (h + 1) * HEAD_DIM)
            q = qnew_vm[:, at]
            past = lax.dot_general(q, qkv_vm[1, :, at], contract_last, preferred_element_type=jnp.float32)
            last = jnp.sum(q.astype(jnp.float32) * knew_vm[:, at].astype(jnp.float32), axis=1, keepdims=True)
            top = jnp.maximum(jnp.max(past, axis=1, keepdims=True), last)
            past, last = jnp.exp2((past - top) * scale2), jnp.exp2((last - top) * scale2)
            inv = 1.0 / (jnp.sum(past, axis=1, keepdims=True) + last)
            out = jnp.dot((past * inv).astype(jnp.bfloat16), qkv_vm[2, :, at], preferred_element_type=jnp.float32)
            out = out + (last * inv).astype(jnp.bfloat16).astype(jnp.float32) * vnew_vm[:, at].astype(jnp.float32)
            deco_vm[:, at] = jnp.where(mine, out, deco_vm[:, at])

    def output_rows(b):
        @pl.when(jnp.logical_not(on_first))
        def _():
            drain(o_ref.at[b, pl.ds(0, group_n - 1)], orecv_sem.at[b])

        for g in range(group_n):
            pltpu.make_async_copy(o_ref.at[b, g], oin_vm.at[:, pl.ds(g * cols, cols)], oin_sem).start()
        load_x = pltpu.make_async_copy(x_hbm.at[b], xo_vm, xo_sem)
        load_x.start()

        @pl.when(b >= 1)
        def _():
            drain(outv_vm, outv_sem)

        @pl.when(b == 0)
        def _():
            wo_copy.wait()

        ssq_vm[...] = jnp.zeros_like(ssq_vm)
        drain(oin_vm, oin_sem)

        def col_tile(n, _):
            at = pl.ds(pl.multiple_of(n * COL_TILE, COL_TILE), COL_TILE)
            acc = jnp.dot(oin_vm[...], wo_vm[:, at], preferred_element_type=jnp.float32)
            raw_vm[:, at] = acc
            sq = acc * acc
            ssq_vm[...] += sum(sq[:, i * HEAD_DIM:(i + 1) * HEAD_DIM] for i in range(COL_TILE // HEAD_DIM))
            return 0

        lax.fori_loop(0, width // COL_TILE, col_tile, 0)
        inv = lax.rsqrt(jnp.sum(ssq_vm[...], axis=1, keepdims=True) / width + NORM_EPS)
        load_x.wait()

        def out_tile(n, _):
            at = pl.ds(pl.multiple_of(n * cols, cols), cols)
            outv_vm[:, at] = (xo_vm[:, at].astype(jnp.float32) + raw_vm[:, at] * inv * post_ref[:, at]).astype(jnp.bfloat16)
            return 0

        lax.fori_loop(0, group_n, out_tile, 0)
        pltpu.make_async_copy(outv_vm, outp_ref.at[b], outv_sem).start()

    def send_part():
        own = pl.ds(pl.multiple_of(me * cols, cols), cols)
        part = jnp.dot(deco_vm[...].astype(jnp.bfloat16), wo_vm[own], preferred_element_type=jnp.float32)
        decp_vm[me] = part.astype(jnp.bfloat16)
        for step in range(1, group_n):
            remote(decp_vm.at[me], decp_vm.at[me], decs_sem, decr_sem, lax.rem(me + step, group_n)).start()

    def step(t, _):
        @pl.when(t < n_batch)
        def _():
            project(t)

        @pl.when(t == 1)
        def _():
            new_row()

        @pl.when(t >= 2)
        def _():
            forward_o(t - 2)

        @pl.when(jnp.logical_and(on_first, t >= 1))
        def _():
            attend_first(t - 1)

        @pl.when(t >= 1)
        def _():
            attend(t - 1)

        @pl.when(t < n_batch)
        def _():
            forward(t)

        @pl.when(jnp.logical_and(t >= 3, t < n_batch + 3 - LATE))
        def _():
            output_rows(t - 3)

        return 0

    lax.fori_loop(0, n_batch + 1, step, 0)
    send_part()
    forward_o(n_batch - 1)

    drain(decp_vm.at[pl.ds(0, group_n - 1)], decs_sem)
    drain(decp_vm.at[pl.ds(0, group_n - 1)], decr_sem)
    proj = decp_vm[0].astype(jnp.float32)
    for g in range(1, group_n):
        proj = proj + decp_vm[g].astype(jnp.float32)
    inv = lax.rsqrt(jnp.sum(proj * proj, axis=1, keepdims=True) / width + NORM_EPS)
    outd_ref[...] = (new_ref[...].astype(jnp.float32) + proj * inv * post_ref[...]).astype(jnp.bfloat16)

    for t in range(n_batch - SLOTS, n_batch):
        drain_sends(t)
    for b in range(n_batch - 2, n_batch):
        drain_o_sends(b)
    drain_forwards()

    @pl.when(on_first)
    def _():
        drain(olocal_vm, olocal_sem)

    @pl.when(jnp.logical_not(on_first))
    def _():
        for b in range(n_batch - LATE, n_batch):
            drain(o_ref.at[b, pl.ds(0, group_n - 1)], orecv_sem.at[b])

    drain(outv_vm, outv_sem)


def output_kernel(o_ref, x_ref, wo_hbm, post_ref, outp_ref, k_ref, v_ref, knew_ref, vnew_ref, out_ref, kc_ref, vc_ref, wo_vm, raw_vm, wo_sem):
    _, group_n, tok, cols = o_ref.shape
    width = group_n * cols
    heads = cols // HEAD_DIM
    b, n_batch = pl.program_id(0), pl.num_programs(0)
    wo_copy = pltpu.make_async_copy(wo_hbm, wo_vm, wo_sem)

    @pl.when(b == 0)
    def _():
        wo_copy.start()

    @pl.when(b < n_batch - LATE)
    def _():
        out_ref[...] = outp_ref[...]

    @pl.when(b == n_batch - LATE)
    def _():
        wo_copy.wait()

    @pl.when(b >= n_batch - LATE)
    def _():
        o_all = jnp.concatenate([o_ref[0, g] for g in range(group_n)], axis=1)
        ssq = jnp.zeros((tok, 1), jnp.float32)
        for n in range(width // COL_TILE):
            at = slice(n * COL_TILE, (n + 1) * COL_TILE)
            acc = jnp.dot(o_all, wo_vm[:, at], preferred_element_type=jnp.float32)
            raw_vm[:, at] = acc
            ssq = ssq + jnp.sum(acc * acc, axis=1, keepdims=True)
        inv = lax.rsqrt(ssq / width + NORM_EPS)
        out_ref[0] = (x_ref[0].astype(jnp.float32) + raw_vm[...] * inv * post_ref[...]).astype(jnp.bfloat16)

    seq = k_ref.shape[2]
    for src, new, to in ((k_ref, knew_ref, kc_ref), (v_ref, vnew_ref, vc_ref)):
        to[0, :seq] = src[0, 0].reshape(seq, heads, HEAD_DIM)
        to[0, seq:] = new[0].reshape(1, heads, HEAD_DIM)


def solution(mesh):
    group_n = mesh.shape["sp"]

    def device_step(prompt_blk, w_q, w_k, w_v, w_o, q_norm_w, k_norm_w, post_norm_w, new_rows):
        n_batch, tok, width = prompt_blk.shape
        cols = width // group_n
        heads = cols // HEAD_DIM
        seq = tok * group_n
        bf16, f32 = jnp.bfloat16, jnp.float32
        step = jnp.arange(tok + 8)
        cos_t, sin_t = rope_tables(jnp.where(step < tok, lax.axis_index("sp") * tok + step, seq))
        q_gain, k_gain, post = q_norm_w[None], k_norm_w[None], post_norm_w[None]
        any_spec = pl.BlockSpec(memory_space=pl.ANY)
        vm_spec = pl.BlockSpec(memory_space=pltpu.VMEM)
        dma = pltpu.SemaphoreType.DMA
        qkv, o_all, _, _, _, _, out_early, k_new, v_new, out_d = pl.pallas_call(
            functools.partial(exchange_kernel, group_n),
            out_shape=(
                jax.ShapeDtypeStruct((3, n_batch, seq, cols), bf16),
                jax.ShapeDtypeStruct((n_batch, group_n, tok, cols), bf16),
                jax.ShapeDtypeStruct((n_batch, 2, CORES, 2, tok, cols), bf16),
                jax.ShapeDtypeStruct((n_batch, 2, CORES, tok, cols), bf16),
                jax.ShapeDtypeStruct((n_batch, 2, CORES, tok, cols), bf16),
                jax.ShapeDtypeStruct((n_batch, 2, group_n, tok, cols), bf16),
                jax.ShapeDtypeStruct((n_batch - LATE, tok, width), bf16),
                jax.ShapeDtypeStruct((n_batch, 1, cols), bf16),
                jax.ShapeDtypeStruct((n_batch, 1, cols), bf16),
                jax.ShapeDtypeStruct((n_batch, width), bf16),
            ),
            in_specs=[any_spec] * 5 + [vm_spec] * 6,
            out_specs=(any_spec,) * 7 + (vm_spec,) * 3,
            scratch_shapes=[
                pltpu.VMEM((3, width, width), bf16),
                pltpu.VMEM((2, tok, width), bf16),
                pltpu.VMEM((tok, width), f32),
                pltpu.VMEM((tok, HEAD_DIM), f32),
                pltpu.VMEM((SLOTS, 3, group_n, tok, cols), bf16),
                pltpu.VMEM((3, seq, cols), bf16),
                pltpu.VMEM((2, seq, cols), bf16),
                pltpu.VMEM((2, group_n, tok, cols), bf16),
                pltpu.VMEM((group_n, tok, cols), bf16),
                pltpu.VMEM((width, width), bf16),
                pltpu.VMEM((tok, width), bf16),
                pltpu.VMEM((tok, width), bf16),
                pltpu.VMEM((tok, width), bf16),
                pltpu.VMEM((n_batch, cols), bf16),
                pltpu.VMEM((n_batch, cols), bf16),
                pltpu.VMEM((n_batch, cols), bf16),
                pltpu.VMEM((n_batch, cols), f32),
                pltpu.VMEM((group_n, n_batch, width), bf16),
                dma((3,)), dma((2,)), dma,
                dma((n_batch,)), dma((n_batch,)), dma((n_batch,)), dma((n_batch, 2)), dma((n_batch, 2)), dma((n_batch, 2)), dma((2,)), dma((2,)), dma((2,)),
                dma((2,)), dma((n_batch,)), dma((n_batch,)), dma((n_batch,)), dma((n_batch,)), dma, dma, dma, dma, dma, dma, dma,
            ],
            compiler_params=pltpu.CompilerParams(collective_id=0, has_side_effects=True, vmem_limit_bytes=VMEM_BYTES),
        )(prompt_blk, w_q, w_k, w_v, w_o, q_gain, k_gain, post, cos_t, sin_t, new_rows)

        row = lambda shape, at: pl.BlockSpec((1,) + shape, lambda b: (b,) + at)
        late = n_batch - LATE
        out_p, k_cache, v_cache = pl.pallas_call(
            output_kernel,
            grid=(n_batch,),
            out_shape=(
                jax.ShapeDtypeStruct((n_batch, tok, width), bf16),
                jax.ShapeDtypeStruct((n_batch, seq + 1, heads, HEAD_DIM), bf16),
                jax.ShapeDtypeStruct((n_batch, seq + 1, heads, HEAD_DIM), bf16),
            ),
            in_specs=[
                pl.BlockSpec((1, group_n, tok, cols), lambda b: (jnp.maximum(b, late), 0, 0, 0)),
                pl.BlockSpec((1, tok, width), lambda b: (jnp.maximum(b, late), 0, 0)),
                any_spec,
                vm_spec,
                pl.BlockSpec((1, tok, width), lambda b: (jnp.minimum(b, late - 1), 0, 0)),
                pl.BlockSpec((1, 1, seq, cols), lambda b: (1, b, 0, 0)),
                pl.BlockSpec((1, 1, seq, cols), lambda b: (2, b, 0, 0)),
                row((1, cols), (0, 0)),
                row((1, cols), (0, 0)),
            ],
            out_specs=(row((tok, width), (0, 0)), row((seq + 1, heads, HEAD_DIM), (0, 0, 0)), row((seq + 1, heads, HEAD_DIM), (0, 0, 0))),
            scratch_shapes=[pltpu.VMEM((width, width), bf16), pltpu.VMEM((tok, width), f32), dma],
            compiler_params=pltpu.CompilerParams(vmem_limit_bytes=VMEM_BYTES),
        )(o_all, prompt_blk, w_o, post, out_early, qkv, qkv, k_new, v_new)
        return out_p, k_cache, v_cache, out_d

    replicated = P()
    return jax.shard_map(
        device_step, mesh=mesh,
        in_specs=(P("dp", "sp", None), replicated, replicated, replicated, replicated, replicated, replicated, replicated, P("dp", None)),
        out_specs=(P("dp", "sp", None), P("dp", None, "sp", None), P("dp", None, "sp", None), P("dp", None)),
        check_vma=False)
```

```python
import functools

import jax
import jax.numpy as jnp
from jax import lax
from jax.experimental import pallas as pl
from jax.experimental.pallas import tpu as pltpu
from jax.sharding import PartitionSpec as P

HEAD_DIM = 128
ROPE_THETA = 500000.0
NORM_EPS = 1e-6
CORES = 2
LOG2E = 1.4426950408889634
SLOTS = 3
COL_TILE = 512
VMEM_BYTES = 66_000_000


def rope_rows():
    lane = jnp.arange(HEAD_DIM)
    inv_freq = ROPE_THETA ** (-(2 * (lane % (HEAD_DIM // 2))).astype(jnp.float32) / HEAD_DIM)
    return inv_freq[None], jnp.where(lane < HEAD_DIM // 2, -1.0, 1.0)[None]


def rotate(values, cos_t, sin_t):
    return values * cos_t + pltpu.roll(values, HEAD_DIM // 2, 1) * sin_t


def exchange_kernel(group_n, x_hbm, wq_hbm, wk_hbm, wv_hbm, wo_hbm, qgain_ref, kgain_ref, post_ref, freq_ref, sign_ref, new_ref,
                    qkv_ref, o_ref, relkv_ref, relq_ref, relo_ref, kvp_ref, outp_ref, knew_ref, vnew_ref, outd_ref,
                    w_vm, x_vm, raw_vm, ssq_vm, stage_vm, qkv_vm, ostage_vm, kvp_vm, olocal_vm, wo_vm, oin_vm, xo_vm, outv_vm, qnew_vm, knew_vm, vnew_vm, deco_vm, decp_vm, cos_vm, sin_vm,
                    w_sem, x_sem, wo_sem, send_sem, recvkv_sem, recvq_sem, relkv_sem, relq_sem, relo_sem, fwdkv_sem, fwdq_sem, fwdo_sem,
                    load_sem, osend_sem, oown_sem, orecv_sem, kvps_sem, kvpr_sem, kvpl_sem, olocal_sem, oin_sem, xo_sem, outv_sem, decs_sem, decr_sem):
    n_batch, tok, width = x_hbm.shape
    cols = width // group_n
    heads = cols // HEAD_DIM
    first_rows = CORES * tok
    chips = group_n // CORES
    me = lax.axis_index("sp")
    chip, core = me // CORES, me % CORES
    right = (chip + 1) % chips
    left = (chip + chips - 1) % chips
    far = (chip + 2) % chips
    right_dev, left_dev = right * CORES + core, left * CORES + core
    partner = chip * CORES + (1 - core)
    on_first = chip == 0
    w_hbm = (wq_hbm, wk_hbm, wv_hbm)
    gains = (qgain_ref, kgain_ref)
    scale2 = HEAD_DIM ** -0.5 * LOG2E
    contract_last = (((1,), (1,)), ((), ()))

    def remote(src, dst, s_sem, r_sem, dev):
        return pltpu.make_async_remote_copy(src_ref=src, dst_ref=dst, send_sem=s_sem, recv_sem=r_sem,
                                            device_id={"sp": dev}, device_id_type=pl.DeviceIdType.MESH)

    def drain(ref, sem):
        pltpu.make_async_copy(ref, ref, sem).wait()

    def with_split(source, use):
        mid, shift = tok // 2, tok // 8
        for n, holds in ((mid - shift, source == 1), (mid + shift, source == chips - 1), (mid, source % 2 == 0)):
            @pl.when(holds)
            def _():
                use(n)

    def w_copy(j, n):
        at = pl.ds(n * COL_TILE, COL_TILE)
        return pltpu.make_async_copy(w_hbm[j].at[:, at], w_vm.at[j, :, at], w_sem.at[j, n])

    def x_copy(t):
        return pltpu.make_async_copy(x_hbm.at[t], x_vm.at[lax.rem(t, 2)], x_sem.at[lax.rem(t, 2)])

    x_copy(0).start()
    for j in (2, 1, 0):
        for n in range(width // COL_TILE):
            w_copy(j, n).start()
    wo_copy = pltpu.make_async_copy(wo_hbm, wo_vm, wo_sem)
    wo_copy.start()

    barrier = pltpu.get_barrier_semaphore()
    for step in range(1, group_n):
        pl.semaphore_signal(barrier, inc=1, device_id={"sp": lax.rem(me + step, group_n)}, device_id_type=pl.DeviceIdType.MESH)
    place = lax.broadcasted_iota(jnp.int32, cos_vm.shape, 0)
    angles = jnp.where(place < tok, me * tok + place, group_n * tok).astype(jnp.float32) * freq_ref[...]
    cos_vm[...] = jnp.cos(angles)
    sin_vm[...] = jnp.sin(angles) * sign_ref[...]
    pl.semaphore_wait(barrier, group_n - 1)

    def send_tensor(t, slot, j):
        rows = pl.ds(me * tok, tok)
        far_devs = pl.ds(far * CORES, CORES)
        recv = recvkv_sem.at[t] if j else recvq_sem.at[t]

        def two_hops(n):
            for way, at, dev in ((0, pl.ds(0, n), right_dev), (1, pl.ds(n, tok - n), left_dev)):
                dst, sem = (relkv_ref.at[t, way, :, j - 1, at], relkv_sem.at[t, way]) if j else (relq_ref.at[t, way, :, at], relq_sem.at[t, way])
                remote(stage_vm.at[slot, j, far_devs, at], dst, send_sem.at[t], sem, dev).start()

        with_split(chip, two_hops)
        for side in (right, left):
            for c in range(CORES):
                dev = side * CORES + c
                remote(stage_vm.at[slot, j, dev], qkv_ref.at[j, t, rows], send_sem.at[t], recv, dev).start()
        remote(stage_vm.at[slot, j, partner], qkv_ref.at[j, t, rows], send_sem.at[t], recv, partner).start()
        pltpu.make_async_copy(stage_vm.at[slot, j, me], qkv_ref.at[j, t, rows], recv).start()

    def drain_sends(t):
        slot = lax.rem(t, SLOTS)

        @pl.when(on_first)
        def _():
            drain(stage_vm.at[slot, pl.ds(1, 2), pl.ds(0, group_n - 1)], send_sem.at[t])

        @pl.when(jnp.logical_not(on_first))
        def _():
            drain(stage_vm.at[slot, :, pl.ds(0, group_n - 1)], send_sem.at[t])

        @pl.when(me == 0)
        def _():
            drain(stage_vm.at[slot, pl.ds(1, 2)], kvps_sem.at[t])

    def project(t):
        slot = lax.rem(t, SLOTS)

        @pl.when(t >= SLOTS)
        def _():
            drain_sends(t - SLOTS)

        x_copy(t).wait()

        @pl.when(t + 1 < n_batch)
        def _():
            x_copy(t + 1).start()

        x_slot = lax.rem(t, 2)
        for j in (2, 1, 0):
            if j < 2:
                ssq_vm[...] = jnp.zeros_like(ssq_vm)

            def col_tile(n, _):
                @pl.when(t == 0)
                def _():
                    w_copy(j, n).wait()

                at = pl.ds(pl.multiple_of(n * COL_TILE, COL_TILE), COL_TILE)
                acc = jnp.dot(x_vm[x_slot], w_vm[j, :, at], preferred_element_type=jnp.float32)
                if j < 2:
                    raw_vm[:, at] = acc
                    sq = acc * acc
                    ssq_vm[...] += sum(sq[:, i * HEAD_DIM:(i + 1) * HEAD_DIM] for i in range(COL_TILE // HEAD_DIM))
                else:
                    for i in range(COL_TILE // cols):
                        stage_vm[slot, j, n * (COL_TILE // cols) + i] = acc[:, i * cols:(i + 1) * cols].astype(jnp.bfloat16)
                return 0

            lax.fori_loop(0, width // COL_TILE, col_tile, 0)
            if j < 2:
                inv = lax.rsqrt(jnp.sum(ssq_vm[...], axis=1, keepdims=True) / width + NORM_EPS)

                def group_tile(n, _):
                    for h in range(heads):
                        at = pl.ds(pl.multiple_of(n * cols + h * HEAD_DIM, HEAD_DIM), HEAD_DIM)
                        normed = raw_vm[:, at] * inv * gains[j][:, at]
                        stage_vm[slot, j, n, :, h * HEAD_DIM:(h + 1) * HEAD_DIM] = rotate(normed, cos_vm[:tok], sin_vm[:tok]).astype(jnp.bfloat16)
                    return 0

                lax.fori_loop(0, group_n, group_tile, 0)
            if j:
                send_tensor(t, slot, j)
            else:
                @pl.when(jnp.logical_not(on_first))
                def _():
                    send_tensor(t, slot, j)

        @pl.when(me == 0)
        def _():
            remote(stage_vm.at[slot, pl.ds(1, 2)], kvp_ref.at[t], kvps_sem.at[t], kvpr_sem.at[t], partner).start()

    def relay_ways(use):
        with_split(left, lambda n: use(0, left, left_dev, right, 0, n))
        with_split(right, lambda n: use(1, right, right_dev, left, n, tok - n))

    def forward(b):
        def way_kv(way, source, source_dev, to, first, n):
            at, dst_rows = pl.ds(first, n), pl.ds(source_dev * tok + first, n)
            drain(relkv_ref.at[b, way, :, :, at], relkv_sem.at[b, way])
            for c in range(CORES):
                remote(relkv_ref.at[b, way, c, :, at], qkv_ref.at[pl.ds(1, 2), b, dst_rows], fwdkv_sem.at[way], recvkv_sem.at[b], to * CORES + c).start()

            @pl.when(source != 0)
            def _():
                drain(relq_ref.at[b, way, :, at], relq_sem.at[b, way])
                for c in range(CORES):
                    remote(relq_ref.at[b, way, c, at], qkv_ref.at[0, b, dst_rows], fwdq_sem.at[way], recvq_sem.at[b], to * CORES + c).start()

        relay_ways(way_kv)

    def forward_o(b):
        def way_o(way, source, source_dev, to, first, n):
            at = pl.ds(first, n)

            @pl.when(to != 0)
            def _():
                drain(relo_ref.at[b, way, :, at], relo_sem.at[b, way])
                for c in range(CORES):
                    remote(relo_ref.at[b, way, c, at], o_ref.at[b, source_dev, at], fwdo_sem.at[way], orecv(b, source_dev), to * CORES + c).start()

        relay_ways(way_o)

    def drain_forwards():
        def way_all(way, source, source_dev, to, first, n):
            at = pl.ds(first, n)
            drain(relkv_ref.at[:, way, :, :, at], fwdkv_sem.at[way])

            @pl.when(source != 0)
            def _():
                drain(relq_ref.at[:, way, :, at], fwdq_sem.at[way])

            @pl.when(to != 0)
            def _():
                drain(relo_ref.at[:, way, :, at], fwdo_sem.at[way])

        relay_ways(way_all)

    def orecv(b, source_dev):
        return orecv_sem.at[b + source_dev * (b // (n_batch - 1))]

    def send_o(b, slot, dev):
        src = ostage_vm.at[slot, pl.ds(dev * tok, tok)]
        c = dev % CORES
        away = lax.rem(dev // CORES - chip + chips, chips)

        @pl.when(dev == me)
        def _():
            pltpu.make_async_copy(src, o_ref.at[b, me], oown_sem.at[b]).start()

        @pl.when(jnp.logical_and(dev != me, away != 2))
        def _():
            remote(src, o_ref.at[b, me], osend_sem.at[b], orecv(b, me), dev).start()

        @pl.when(away == 2)
        def _():
            def two_hops(n):
                remote(ostage_vm.at[slot, pl.ds(dev * tok, n)], relo_ref.at[b, 0, c, pl.ds(0, n)],
                       osend_sem.at[b], relo_sem.at[b, 0], right_dev).start()
                remote(ostage_vm.at[slot, pl.ds(dev * tok + n, tok - n)], relo_ref.at[b, 1, c, pl.ds(n, tok - n)],
                       osend_sem.at[b], relo_sem.at[b, 1], left_dev).start()

            with_split(chip, two_hops)

    def drain_o_sends(b, own):
        slot = lax.rem(b, 2)

        @pl.when(on_first)
        def _():
            drain(ostage_vm.at[slot, pl.ds(0, (group_n - CORES) * tok)], osend_sem.at[b])

        @pl.when(jnp.logical_not(on_first))
        def _():
            drain(ostage_vm.at[slot, pl.ds(0, (group_n - CORES - 1) * tok)], osend_sem.at[b])
            if own:
                drain(ostage_vm.at[slot, pl.ds(0, tok)], oown_sem.at[b])

    def new_row():
        def full(j):
            def col_tile(n, ssq):
                at = pl.ds(pl.multiple_of(n * COL_TILE, COL_TILE), COL_TILE)
                acc = jnp.dot(new_ref[...], w_vm[j, :, at], preferred_element_type=jnp.float32)
                return ssq + jnp.sum(acc * acc, axis=1, keepdims=True)

            ssq = lax.fori_loop(0, width // COL_TILE, col_tile, jnp.zeros((n_batch, 1), jnp.float32))
            return lax.rsqrt(ssq / width + NORM_EPS)

        own = pl.ds(pl.multiple_of(me * cols, cols), cols)
        for j, to in ((0, qnew_vm), (1, knew_vm)):
            inv = full(j)
            raw = jnp.dot(new_ref[...], w_vm[j, :, own], preferred_element_type=jnp.float32)
            normed = raw * inv * gains[j][:, own]
            for h in range(heads):
                at = slice(h * HEAD_DIM, (h + 1) * HEAD_DIM)
                to[:, at] = rotate(normed[:, at], cos_vm[tok:tok + 1], sin_vm[tok:tok + 1]).astype(jnp.bfloat16)
        vnew_vm[...] = jnp.dot(new_ref[...], w_vm[2, :, own], preferred_element_type=jnp.float32).astype(jnp.bfloat16)
        for b in range(n_batch):
            knew_ref[b] = knew_vm[b:b + 1]
            vnew_ref[b] = vnew_vm[b:b + 1]
        deco_vm[...] = jnp.zeros_like(deco_vm)

    def block_attention(q, k_diag, v_diag, k_past, v_past):
        keep = lax.broadcasted_iota(jnp.int32, (tok, tok), 0) >= lax.broadcasted_iota(jnp.int32, (tok, tok), 1)
        diag = lax.dot_general(q, k_diag, contract_last, preferred_element_type=jnp.float32)
        diag = jnp.where(keep, diag, -jnp.inf)
        top = jnp.max(diag, axis=1, keepdims=True)
        if k_past is not None:
            past = lax.dot_general(q, k_past, contract_last, preferred_element_type=jnp.float32)
            top = jnp.maximum(top, jnp.max(past, axis=1, keepdims=True))
            past = jnp.exp2((past - top) * scale2)
        diag = jnp.exp2((diag - top) * scale2)
        total = jnp.sum(diag, axis=1, keepdims=True)
        if k_past is not None:
            total = total + jnp.sum(past, axis=1, keepdims=True)
        inv = 1.0 / total
        out = jnp.dot((diag * inv).astype(jnp.bfloat16), v_diag, preferred_element_type=jnp.float32)
        if k_past is not None:
            out = out + jnp.dot((past * inv).astype(jnp.bfloat16), v_past, preferred_element_type=jnp.float32)
        return out.astype(jnp.bfloat16)

    def attend_first(b):
        slot = lax.rem(b, SLOTS)

        @pl.when(b >= 1)
        def _():
            drain(olocal_vm, olocal_sem)

        for which in range(CORES):
            @pl.when(core == which)
            def _():
                if which:
                    drain(kvp_ref.at[b], kvpr_sem.at[b])
                    load = pltpu.make_async_copy(kvp_ref.at[b], kvp_vm, kvpl_sem)
                    load.start()
                    load.wait()

                def group(g, _):
                    for h in range(heads):
                        at = slice(h * HEAD_DIM, (h + 1) * HEAD_DIM)
                        past = (kvp_vm[0, g, :, at], kvp_vm[1, g, :, at]) if which else (None, None)
                        olocal_vm[g, :, at] = block_attention(stage_vm[slot, 0, g, :, at], stage_vm[slot, 1, g, :, at], stage_vm[slot, 2, g, :, at], *past)
                    return 0

                lax.fori_loop(0, group_n, group, 0)

        pltpu.make_async_copy(olocal_vm, o_ref.at[b], olocal_sem).start()

    def attend(b):
        slot = lax.rem(b, 2)
        q_rows = pl.ds(first_rows, (group_n - CORES) * tok)
        drain(qkv_ref.at[pl.ds(1, 2), b], recvkv_sem.at[b])
        drain(qkv_ref.at[0, b, q_rows], recvq_sem.at[b])
        load_kv = pltpu.make_async_copy(qkv_ref.at[pl.ds(1, 2), b], qkv_vm.at[pl.ds(1, 2)], load_sem.at[0])
        load_q = pltpu.make_async_copy(qkv_ref.at[0, b, q_rows], qkv_vm.at[0, q_rows], load_sem.at[1])
        load_kv.start()
        load_q.start()

        @pl.when(b >= 2)
        def _():
            drain_o_sends(b - 2, True)

        load_kv.wait()
        load_q.wait()
        for blk in range(CORES, group_n):
            rows = slice(blk * tok, (blk + 1) * tok)

            def one_head(h, _):
                at = pl.ds(pl.multiple_of(h * HEAD_DIM, HEAD_DIM), HEAD_DIM)
                ostage_vm[slot, rows, at] = block_attention(qkv_vm[0, rows, at], qkv_vm[1, rows, at], qkv_vm[2, rows, at],
                                                            qkv_vm[1, :blk * tok, at], qkv_vm[2, :blk * tok, at])
                return 0

            lax.fori_loop(0, heads, one_head, 0)
            send_o(b, slot, blk)

        mine = lax.broadcasted_iota(jnp.int32, (n_batch, HEAD_DIM), 0) == b
        for h in range(heads):
            at = slice(h * HEAD_DIM, (h + 1) * HEAD_DIM)
            q = qnew_vm[:, at]
            past = lax.dot_general(q, qkv_vm[1, :, at], contract_last, preferred_element_type=jnp.float32)
            last = jnp.sum(q.astype(jnp.float32) * knew_vm[:, at].astype(jnp.float32), axis=1, keepdims=True)
            top = jnp.maximum(jnp.max(past, axis=1, keepdims=True), last)
            past, last = jnp.exp2((past - top) * scale2), jnp.exp2((last - top) * scale2)
            inv = 1.0 / (jnp.sum(past, axis=1, keepdims=True) + last)
            out = jnp.dot((past * inv).astype(jnp.bfloat16), qkv_vm[2, :, at], preferred_element_type=jnp.float32)
            out = out + (last * inv).astype(jnp.bfloat16).astype(jnp.float32) * vnew_vm[:, at].astype(jnp.float32)
            deco_vm[:, at] = jnp.where(mine, out, deco_vm[:, at])

    def finish_rows(b, load_x):
        inv = lax.rsqrt(jnp.sum(ssq_vm[...], axis=1, keepdims=True) / width + NORM_EPS)
        load_x.wait()

        def out_tile(n, _):
            at = pl.ds(pl.multiple_of(n * cols, cols), cols)
            outv_vm[:, at] = (xo_vm[:, at].astype(jnp.float32) + raw_vm[:, at] * inv * post_ref[:, at]).astype(jnp.bfloat16)
            return 0

        lax.fori_loop(0, group_n, out_tile, 0)
        pltpu.make_async_copy(outv_vm, outp_ref.at[b], outv_sem).start()

    def o_copy(b, g, k):
        return pltpu.make_async_copy(o_ref.at[b, g], oin_vm.at[:, pl.ds(pl.multiple_of(g * cols, cols), cols)], oin_sem.at[k])

    def output_rows(b):
        @pl.when(jnp.logical_not(on_first))
        def _():
            drain(o_ref.at[b, pl.ds(0, group_n - 1)], orecv_sem.at[b])

        for g in range(group_n):
            o_copy(b, g, 0).start()
        load_x = pltpu.make_async_copy(x_hbm.at[b], xo_vm, xo_sem)
        load_x.start()

        @pl.when(b >= 1)
        def _():
            drain(outv_vm, outv_sem)

        @pl.when(b == 0)
        def _():
            wo_copy.wait()

        ssq_vm[...] = jnp.zeros_like(ssq_vm)
        drain(oin_vm, oin_sem.at[0])

        def col_tile(n, _):
            at = pl.ds(pl.multiple_of(n * COL_TILE, COL_TILE), COL_TILE)
            acc = jnp.dot(oin_vm[...], wo_vm[:, at], preferred_element_type=jnp.float32)
            raw_vm[:, at] = acc
            sq = acc * acc
            ssq_vm[...] += sum(sq[:, i * HEAD_DIM:(i + 1) * HEAD_DIM] for i in range(COL_TILE // HEAD_DIM))
            return 0

        lax.fori_loop(0, width // COL_TILE, col_tile, 0)
        finish_rows(b, load_x)

    def last_rows(b):
        load_x = pltpu.make_async_copy(x_hbm.at[b], xo_vm, xo_sem)
        load_x.start()

        @pl.when(on_first)
        def _():
            drain(olocal_vm, olocal_sem)

        drain(outv_vm, outv_sem)
        ssq_vm[...] = jnp.zeros_like(ssq_vm)
        both = CORES * cols
        for k, source in enumerate((chip, right, left, far)):
            if k:
                @pl.when(jnp.logical_not(on_first))
                def _():
                    for c in range(CORES):
                        drain(o_ref.at[b, source * CORES + c], orecv(b, source * CORES + c))
            else:
                @pl.when(jnp.logical_not(on_first))
                def _():
                    drain(o_ref.at[b, me], oown_sem.at[b])
                    drain(o_ref.at[b, partner], orecv(b, partner))
            for c in range(CORES):
                o_copy(b, source * CORES + c, k).start()
            part = pl.ds(pl.multiple_of(source * both, both), both)
            drain(oin_vm.at[:, part], oin_sem.at[k])

            def col_tile(n, _):
                at = pl.ds(pl.multiple_of(n * COL_TILE, COL_TILE), COL_TILE)
                acc = jnp.dot(oin_vm[:, part], wo_vm[part, at], preferred_element_type=jnp.float32)
                if k:
                    acc = acc + raw_vm[:, at]
                raw_vm[:, at] = acc
                if k == 3:
                    sq = acc * acc
                    ssq_vm[...] += sum(sq[:, i * HEAD_DIM:(i + 1) * HEAD_DIM] for i in range(COL_TILE // HEAD_DIM))
                return 0

            lax.fori_loop(0, width // COL_TILE, col_tile, 0)
        finish_rows(b, load_x)

    def send_part():
        own = pl.ds(pl.multiple_of(me * cols, cols), cols)
        part = jnp.dot(deco_vm[...].astype(jnp.bfloat16), wo_vm[own], preferred_element_type=jnp.float32)
        decp_vm[me] = part.astype(jnp.bfloat16)
        for step in range(1, group_n):
            remote(decp_vm.at[me], decp_vm.at[me], decs_sem, decr_sem, lax.rem(me + step, group_n)).start()

    def step(t, _):
        @pl.when(t < n_batch)
        def _():
            project(t)

        @pl.when(t == 1)
        def _():
            new_row()

        @pl.when(t >= 2)
        def _():
            forward_o(t - 2)

        @pl.when(jnp.logical_and(on_first, t >= 1))
        def _():
            attend_first(t - 1)

        @pl.when(t >= 1)
        def _():
            attend(t - 1)

        @pl.when(t < n_batch)
        def _():
            forward(t)

        @pl.when(jnp.logical_and(t >= 3, t < n_batch))
        def _():
            output_rows(t - 3)

        return 0

    def rest(b, _):
        @pl.when(b == n_batch - 2)
        def _():
            drain_o_sends(b, True)

        output_rows(b)
        return 0

    lax.fori_loop(0, n_batch + 1, step, 0)
    send_part()
    forward_o(n_batch - 1)
    lax.fori_loop(n_batch - 3, n_batch - 1, rest, 0)

    drain(decp_vm.at[pl.ds(0, group_n - 1)], decs_sem)
    drain(decp_vm.at[pl.ds(0, group_n - 1)], decr_sem)
    proj = decp_vm[0].astype(jnp.float32)
    for g in range(1, group_n):
        proj = proj + decp_vm[g].astype(jnp.float32)
    inv = lax.rsqrt(jnp.sum(proj * proj, axis=1, keepdims=True) / width + NORM_EPS)
    outd_ref[...] = (new_ref[...].astype(jnp.float32) + proj * inv * post_ref[...]).astype(jnp.bfloat16)

    last_rows(n_batch - 1)
    for t in range(n_batch - SLOTS, n_batch):
        drain_sends(t)
    drain_o_sends(n_batch - 1, False)
    drain_forwards()
    drain(outv_vm, outv_sem)


def output_kernel(outp_ref, k_ref, v_ref, knew_ref, vnew_ref, outd_in_ref, out_ref, kc_ref, vc_ref, outd_ref):
    out_ref[...] = outp_ref[...]
    outd_ref[...] = outd_in_ref[...]
    seq, cols = k_ref.shape[2:]
    heads = cols // HEAD_DIM
    for src, new, to in ((k_ref, knew_ref, kc_ref), (v_ref, vnew_ref, vc_ref)):
        to[0, :seq] = src[0, 0].reshape(seq, heads, HEAD_DIM)
        to[0, seq:] = new[0].reshape(1, heads, HEAD_DIM)


def solution(mesh):
    group_n = mesh.shape["sp"]

    def device_step(prompt_blk, w_q, w_k, w_v, w_o, q_norm_w, k_norm_w, post_norm_w, new_rows):
        n_batch, tok, width = prompt_blk.shape
        cols = width // group_n
        heads = cols // HEAD_DIM
        seq = tok * group_n
        bf16, f32 = jnp.bfloat16, jnp.float32
        freq, sign = rope_rows()
        q_gain, k_gain, post = q_norm_w[None], k_norm_w[None], post_norm_w[None]
        any_spec = pl.BlockSpec(memory_space=pl.ANY)
        vm_spec = pl.BlockSpec(memory_space=pltpu.VMEM)
        dma = pltpu.SemaphoreType.DMA
        qkv, _, _, _, _, _, out_rows, k_new, v_new, out_d = pl.pallas_call(
            functools.partial(exchange_kernel, group_n),
            out_shape=(
                jax.ShapeDtypeStruct((3, n_batch, seq, cols), bf16),
                jax.ShapeDtypeStruct((n_batch, group_n, tok, cols), bf16),
                jax.ShapeDtypeStruct((n_batch, 2, CORES, 2, tok, cols), bf16),
                jax.ShapeDtypeStruct((n_batch, 2, CORES, tok, cols), bf16),
                jax.ShapeDtypeStruct((n_batch, 2, CORES, tok, cols), bf16),
                jax.ShapeDtypeStruct((n_batch, 2, group_n, tok, cols), bf16),
                jax.ShapeDtypeStruct((n_batch, tok, width), bf16),
                jax.ShapeDtypeStruct((n_batch, 1, cols), bf16),
                jax.ShapeDtypeStruct((n_batch, 1, cols), bf16),
                jax.ShapeDtypeStruct((n_batch, width), bf16),
            ),
            in_specs=[any_spec] * 5 + [vm_spec] * 6,
            out_specs=(any_spec,) * 7 + (vm_spec,) * 3,
            scratch_shapes=[
                pltpu.VMEM((3, width, width), bf16),
                pltpu.VMEM((2, tok, width), bf16),
                pltpu.VMEM((tok, width), f32),
                pltpu.VMEM((tok, HEAD_DIM), f32),
                pltpu.VMEM((SLOTS, 3, group_n, tok, cols), bf16),
                pltpu.VMEM((3, seq, cols), bf16),
                pltpu.VMEM((2, seq, cols), bf16),
                pltpu.VMEM((2, group_n, tok, cols), bf16),
                pltpu.VMEM((group_n, tok, cols), bf16),
                pltpu.VMEM((width, width), bf16),
                pltpu.VMEM((tok, width), bf16),
                pltpu.VMEM((tok, width), bf16),
                pltpu.VMEM((tok, width), bf16),
                pltpu.VMEM((n_batch, cols), bf16),
                pltpu.VMEM((n_batch, cols), bf16),
                pltpu.VMEM((n_batch, cols), bf16),
                pltpu.VMEM((n_batch, cols), f32),
                pltpu.VMEM((group_n, n_batch, width), bf16),
                pltpu.VMEM((tok + 8, HEAD_DIM), f32),
                pltpu.VMEM((tok + 8, HEAD_DIM), f32),
                dma((3, width // COL_TILE)), dma((2,)), dma,
                dma((n_batch,)), dma((n_batch,)), dma((n_batch,)), dma((n_batch, 2)), dma((n_batch, 2)), dma((n_batch, 2)), dma((2,)), dma((2,)), dma((2,)),
                dma((2,)), dma((n_batch,)), dma((n_batch,)), dma((n_batch + group_n,)), dma((n_batch,)), dma((n_batch,)), dma, dma, dma((group_n // CORES,)), dma, dma, dma, dma,
            ],
            compiler_params=pltpu.CompilerParams(collective_id=0, has_side_effects=True, vmem_limit_bytes=VMEM_BYTES),
        )(prompt_blk, w_q, w_k, w_v, w_o, q_gain, k_gain, post, freq, sign, new_rows)

        row = lambda shape, at: pl.BlockSpec((1,) + shape, lambda b: (b,) + at)
        whole = pl.BlockSpec((n_batch, width), lambda b: (0, 0))
        cache = row((seq + 1, heads, HEAD_DIM), (0, 0, 0))
        out_p, k_cache, v_cache, out_d = pl.pallas_call(
            output_kernel,
            grid=(n_batch,),
            out_shape=(
                jax.ShapeDtypeStruct((n_batch, tok, width), bf16),
                jax.ShapeDtypeStruct((n_batch, seq + 1, heads, HEAD_DIM), bf16),
                jax.ShapeDtypeStruct((n_batch, seq + 1, heads, HEAD_DIM), bf16),
                jax.ShapeDtypeStruct((n_batch, width), bf16),
            ),
            in_specs=[
                row((tok, width), (0, 0)),
                pl.BlockSpec((1, 1, seq, cols), lambda b: (1, b, 0, 0)),
                pl.BlockSpec((1, 1, seq, cols), lambda b: (2, b, 0, 0)),
                row((1, cols), (0, 0)),
                row((1, cols), (0, 0)),
                whole,
            ],
            out_specs=(row((tok, width), (0, 0)), cache, cache, whole),
            compiler_params=pltpu.CompilerParams(vmem_limit_bytes=VMEM_BYTES),
        )(out_rows, qkv, qkv, k_new, v_new, out_d)
        return out_p, k_cache, v_cache, out_d

    replicated = P()
    return jax.shard_map(
        device_step, mesh=mesh,
        in_specs=(P("dp", "sp", None), replicated, replicated, replicated, replicated, replicated, replicated, replicated, P("dp", None)),
        out_specs=(P("dp", "sp", None), P("dp", None, "sp", None), P("dp", None, "sp", None), P("dp", None)),
        check_vma=False)
```

```python
import functools

import jax
import jax.numpy as jnp
from jax import lax
from jax.experimental import pallas as pl
from jax.experimental.pallas import tpu as pltpu
from jax.sharding import PartitionSpec as P

HEAD_DIM = 128
ROPE_THETA = 500000.0
NORM_EPS = 1e-6
CORES = 2
LOG2E = 1.4426950408889634
SLOTS = 3
COL_TILE = 512
VMEM_BYTES = 66_000_000


def rope_rows():
    lane = jnp.arange(HEAD_DIM)
    inv_freq = ROPE_THETA ** (-(2 * (lane % (HEAD_DIM // 2))).astype(jnp.float32) / HEAD_DIM)
    return inv_freq[None], jnp.where(lane < HEAD_DIM // 2, -1.0, 1.0)[None]


def rotate(values, cos_t, sin_t):
    return values * cos_t + pltpu.roll(values, HEAD_DIM // 2, 1) * sin_t


def exchange_kernel(group_n, x_hbm, wq_hbm, wk_hbm, wv_hbm, wo_hbm, qgain_ref, kgain_ref, post_ref, freq_ref, sign_ref, new_ref,
                    qkv_ref, o_ref, relkv_ref, relq_ref, relo_ref, kvp_ref, outp_ref, knew_ref, vnew_ref, outd_ref,
                    w_vm, x_vm, raw_vm, ssq_vm, stage_vm, qkv_vm, ostage_vm, kvp_vm, olocal_vm, wo_vm, oin_vm, xo_vm, outv_vm, qnew_vm, knew_vm, vnew_vm, deco_vm, decp_vm, cos_vm, sin_vm,
                    w_sem, x_sem, wo_sem, send_sem, recvkv_sem, recvq_sem, relkv_sem, relq_sem, relo_sem, fwdkv_sem, fwdq_sem, fwdo_sem,
                    load_sem, osend_sem, oown_sem, orecv_sem, kvps_sem, kvpr_sem, kvpl_sem, olocal_sem, oin_sem, xo_sem, outv_sem, decs_sem, decr_sem):
    n_batch, tok, width = x_hbm.shape
    cols = width // group_n
    heads = cols // HEAD_DIM
    first_rows = CORES * tok
    chips = group_n // CORES
    me = lax.axis_index("sp")
    chip, core = me // CORES, me % CORES
    right = (chip + 1) % chips
    left = (chip + chips - 1) % chips
    far = (chip + 2) % chips
    right_dev, left_dev = right * CORES + core, left * CORES + core
    partner = chip * CORES + (1 - core)
    on_first = chip == 0
    w_hbm = (wq_hbm, wk_hbm, wv_hbm)
    gains = (qgain_ref, kgain_ref)
    scale2 = HEAD_DIM ** -0.5 * LOG2E
    contract_last = (((1,), (1,)), ((), ()))

    def remote(src, dst, s_sem, r_sem, dev):
        return pltpu.make_async_remote_copy(src_ref=src, dst_ref=dst, send_sem=s_sem, recv_sem=r_sem,
                                            device_id={"sp": dev}, device_id_type=pl.DeviceIdType.MESH)

    def drain(ref, sem):
        pltpu.make_async_copy(ref, ref, sem).wait()

    def with_split(source, use):
        mid, shift = tok // 2, tok // 8
        for n, holds in ((mid - shift, source == 1), (mid + shift, source == chips - 1), (mid, source % 2 == 0)):
            @pl.when(holds)
            def _():
                use(n)

    def w_copy(j):
        return pltpu.make_async_copy(w_hbm[j], w_vm.at[j], w_sem.at[j])

    def x_copy(t):
        return pltpu.make_async_copy(x_hbm.at[t], x_vm.at[lax.rem(t, 2)], x_sem.at[lax.rem(t, 2)])

    x_copy(0).start()
    w_copy(2).start()
    wo_copy = pltpu.make_async_copy(wo_hbm, wo_vm, wo_sem)

    barrier = pltpu.get_barrier_semaphore()
    for step in range(1, group_n):
        pl.semaphore_signal(barrier, inc=1, device_id={"sp": lax.rem(me + step, group_n)}, device_id_type=pl.DeviceIdType.MESH)
    place = lax.broadcasted_iota(jnp.int32, cos_vm.shape, 0)
    angles = jnp.where(place < tok, me * tok + place, group_n * tok).astype(jnp.float32) * freq_ref[...]
    cos_vm[...] = jnp.cos(angles)
    sin_vm[...] = jnp.sin(angles) * sign_ref[...]
    pl.semaphore_wait(barrier, group_n - 1)

    def send_tensor(t, slot, j):
        rows = pl.ds(me * tok, tok)
        far_devs = pl.ds(far * CORES, CORES)
        recv = recvkv_sem.at[t] if j else recvq_sem.at[t]

        def two_hops(n):
            for way, at, dev in ((0, pl.ds(0, n), right_dev), (1, pl.ds(n, tok - n), left_dev)):
                dst, sem = (relkv_ref.at[t, way, :, j - 1, at], relkv_sem.at[t, way]) if j else (relq_ref.at[t, way, :, at], relq_sem.at[t, way])
                remote(stage_vm.at[slot, j, far_devs, at], dst, send_sem.at[t], sem, dev).start()

        with_split(chip, two_hops)
        for side in (right, left):
            for c in range(CORES):
                dev = side * CORES + c
                remote(stage_vm.at[slot, j, dev], qkv_ref.at[j, t, rows], send_sem.at[t], recv, dev).start()
        remote(stage_vm.at[slot, j, partner], qkv_ref.at[j, t, rows], send_sem.at[t], recv, partner).start()
        pltpu.make_async_copy(stage_vm.at[slot, j, me], qkv_ref.at[j, t, rows], recv).start()

    def drain_sends(t):
        slot = lax.rem(t, SLOTS)

        @pl.when(on_first)
        def _():
            drain(stage_vm.at[slot, pl.ds(1, 2), pl.ds(0, group_n - 1)], send_sem.at[t])

        @pl.when(jnp.logical_not(on_first))
        def _():
            drain(stage_vm.at[slot, :, pl.ds(0, group_n - 1)], send_sem.at[t])

        @pl.when(me == 0)
        def _():
            drain(stage_vm.at[slot, pl.ds(1, 2)], kvps_sem.at[t])

    def project(t):
        slot = lax.rem(t, SLOTS)

        @pl.when(t >= SLOTS)
        def _():
            drain_sends(t - SLOTS)

        x_copy(t).wait()

        @pl.when(t + 1 < n_batch)
        def _():
            x_copy(t + 1).start()

        x_slot = lax.rem(t, 2)
        for j in (2, 1, 0):
            @pl.when(t == 0)
            def _():
                w_copy(j).wait()
                (w_copy(j - 1) if j else wo_copy).start()

            if j < 2:
                ssq_vm[...] = jnp.zeros_like(ssq_vm)

            def col_tile(n, _):
                at = pl.ds(pl.multiple_of(n * COL_TILE, COL_TILE), COL_TILE)
                acc = jnp.dot(x_vm[x_slot], w_vm[j, :, at], preferred_element_type=jnp.float32)
                if j < 2:
                    raw_vm[:, at] = acc
                    sq = acc * acc
                    ssq_vm[...] += sum(sq[:, i * HEAD_DIM:(i + 1) * HEAD_DIM] for i in range(COL_TILE // HEAD_DIM))
                else:
                    for i in range(COL_TILE // cols):
                        stage_vm[slot, j, n * (COL_TILE // cols) + i] = acc[:, i * cols:(i + 1) * cols].astype(jnp.bfloat16)
                return 0

            lax.fori_loop(0, width // COL_TILE, col_tile, 0)
            if j < 2:
                inv = lax.rsqrt(jnp.sum(ssq_vm[...], axis=1, keepdims=True) / width + NORM_EPS)

                def group_tile(n, _):
                    for h in range(heads):
                        at = pl.ds(pl.multiple_of(n * cols + h * HEAD_DIM, HEAD_DIM), HEAD_DIM)
                        normed = raw_vm[:, at] * inv * gains[j][:, at]
                        stage_vm[slot, j, n, :, h * HEAD_DIM:(h + 1) * HEAD_DIM] = rotate(normed, cos_vm[:tok], sin_vm[:tok]).astype(jnp.bfloat16)
                    return 0

                lax.fori_loop(0, group_n, group_tile, 0)
            if j:
                send_tensor(t, slot, j)
            else:
                @pl.when(jnp.logical_not(on_first))
                def _():
                    send_tensor(t, slot, j)

        @pl.when(me == 0)
        def _():
            remote(stage_vm.at[slot, pl.ds(1, 2)], kvp_ref.at[t], kvps_sem.at[t], kvpr_sem.at[t], partner).start()

    def relay_ways(use):
        with_split(left, lambda n: use(0, left, left_dev, right, 0, n))
        with_split(right, lambda n: use(1, right, right_dev, left, n, tok - n))

    def forward(b):
        def way_kv(way, source, source_dev, to, first, n):
            at, dst_rows = pl.ds(first, n), pl.ds(source_dev * tok + first, n)
            drain(relkv_ref.at[b, way, :, :, at], relkv_sem.at[b, way])
            for c in range(CORES):
                remote(relkv_ref.at[b, way, c, :, at], qkv_ref.at[pl.ds(1, 2), b, dst_rows], fwdkv_sem.at[way], recvkv_sem.at[b], to * CORES + c).start()

            @pl.when(source != 0)
            def _():
                drain(relq_ref.at[b, way, :, at], relq_sem.at[b, way])
                for c in range(CORES):
                    remote(relq_ref.at[b, way, c, at], qkv_ref.at[0, b, dst_rows], fwdq_sem.at[way], recvq_sem.at[b], to * CORES + c).start()

        relay_ways(way_kv)

    def forward_o(b):
        def way_o(way, source, source_dev, to, first, n):
            at = pl.ds(first, n)

            @pl.when(to != 0)
            def _():
                drain(relo_ref.at[b, way, :, at], relo_sem.at[b, way])
                for c in range(CORES):
                    remote(relo_ref.at[b, way, c, at], o_ref.at[b, source_dev, at], fwdo_sem.at[way], orecv(b, source_dev), to * CORES + c).start()

        relay_ways(way_o)

    def drain_forwards():
        def way_all(way, source, source_dev, to, first, n):
            at = pl.ds(first, n)
            drain(relkv_ref.at[:, way, :, :, at], fwdkv_sem.at[way])

            @pl.when(source != 0)
            def _():
                drain(relq_ref.at[:, way, :, at], fwdq_sem.at[way])

            @pl.when(to != 0)
            def _():
                drain(relo_ref.at[:, way, :, at], fwdo_sem.at[way])

        relay_ways(way_all)

    def orecv(b, source_dev):
        return orecv_sem.at[b + source_dev * (b // (n_batch - 1))]

    def send_o(b, slot, dev):
        src = ostage_vm.at[slot, pl.ds(dev * tok, tok)]
        c = dev % CORES
        away = lax.rem(dev // CORES - chip + chips, chips)

        @pl.when(dev == me)
        def _():
            pltpu.make_async_copy(src, o_ref.at[b, me], oown_sem.at[b]).start()

        @pl.when(jnp.logical_and(dev != me, away != 2))
        def _():
            remote(src, o_ref.at[b, me], osend_sem.at[b], orecv(b, me), dev).start()

        @pl.when(away == 2)
        def _():
            def two_hops(n):
                remote(ostage_vm.at[slot, pl.ds(dev * tok, n)], relo_ref.at[b, 0, c, pl.ds(0, n)],
                       osend_sem.at[b], relo_sem.at[b, 0], right_dev).start()
                remote(ostage_vm.at[slot, pl.ds(dev * tok + n, tok - n)], relo_ref.at[b, 1, c, pl.ds(n, tok - n)],
                       osend_sem.at[b], relo_sem.at[b, 1], left_dev).start()

            with_split(chip, two_hops)

    def drain_o_sends(b):
        slot = lax.rem(b, 2)

        @pl.when(on_first)
        def _():
            drain(ostage_vm.at[slot, pl.ds(0, (group_n - CORES) * tok)], osend_sem.at[b])

        @pl.when(jnp.logical_not(on_first))
        def _():
            drain(ostage_vm.at[slot, pl.ds(0, (group_n - CORES - 1) * tok)], osend_sem.at[b])

    def new_row():
        def full(j):
            def col_tile(n, ssq):
                at = pl.ds(pl.multiple_of(n * COL_TILE, COL_TILE), COL_TILE)
                acc = jnp.dot(new_ref[...], w_vm[j, :, at], preferred_element_type=jnp.float32)
                return ssq + jnp.sum(acc * acc, axis=1, keepdims=True)

            ssq = lax.fori_loop(0, width // COL_TILE, col_tile, jnp.zeros((n_batch, 1), jnp.float32))
            return lax.rsqrt(ssq / width + NORM_EPS)

        own = pl.ds(pl.multiple_of(me * cols, cols), cols)
        for j, to in ((0, qnew_vm), (1, knew_vm)):
            inv = full(j)
            raw = jnp.dot(new_ref[...], w_vm[j, :, own], preferred_element_type=jnp.float32)
            normed = raw * inv * gains[j][:, own]
            for h in range(heads):
                at = slice(h * HEAD_DIM, (h + 1) * HEAD_DIM)
                to[:, at] = rotate(normed[:, at], cos_vm[tok:tok + 1], sin_vm[tok:tok + 1]).astype(jnp.bfloat16)
        vnew_vm[...] = jnp.dot(new_ref[...], w_vm[2, :, own], preferred_element_type=jnp.float32).astype(jnp.bfloat16)
        for b in range(n_batch):
            knew_ref[b] = knew_vm[b:b + 1]
            vnew_ref[b] = vnew_vm[b:b + 1]
        deco_vm[...] = jnp.zeros_like(deco_vm)

    def block_attention(q, k_diag, v_diag, k_past, v_past):
        keep = lax.broadcasted_iota(jnp.int32, (tok, tok), 0) >= lax.broadcasted_iota(jnp.int32, (tok, tok), 1)
        diag = lax.dot_general(q, k_diag, contract_last, preferred_element_type=jnp.float32)
        diag = jnp.where(keep, diag, -jnp.inf)
        top = jnp.max(diag, axis=1, keepdims=True)
        if k_past is not None:
            past = lax.dot_general(q, k_past, contract_last, preferred_element_type=jnp.float32)
            top = jnp.maximum(top, jnp.max(past, axis=1, keepdims=True))
            past = jnp.exp2((past - top) * scale2)
        diag = jnp.exp2((diag - top) * scale2)
        total = jnp.sum(diag, axis=1, keepdims=True)
        if k_past is not None:
            total = total + jnp.sum(past, axis=1, keepdims=True)
        inv = 1.0 / total
        out = jnp.dot((diag * inv).astype(jnp.bfloat16), v_diag, preferred_element_type=jnp.float32)
        if k_past is not None:
            out = out + jnp.dot((past * inv).astype(jnp.bfloat16), v_past, preferred_element_type=jnp.float32)
        return out.astype(jnp.bfloat16)

    def attend_first(b):
        slot = lax.rem(b, SLOTS)

        @pl.when(b >= 1)
        def _():
            drain(olocal_vm, olocal_sem)

        for which in range(CORES):
            @pl.when(core == which)
            def _():
                if which:
                    drain(kvp_ref.at[b], kvpr_sem.at[b])
                    load = pltpu.make_async_copy(kvp_ref.at[b], kvp_vm, kvpl_sem)
                    load.start()
                    load.wait()

                def group(g, _):
                    for h in range(heads):
                        at = slice(h * HEAD_DIM, (h + 1) * HEAD_DIM)
                        past = (kvp_vm[0, g, :, at], kvp_vm[1, g, :, at]) if which else (None, None)
                        olocal_vm[g, :, at] = block_attention(stage_vm[slot, 0, g, :, at], stage_vm[slot, 1, g, :, at], stage_vm[slot, 2, g, :, at], *past)
                    return 0

                lax.fori_loop(0, group_n, group, 0)

        pltpu.make_async_copy(olocal_vm, o_ref.at[b], olocal_sem).start()

    def attend(b):
        slot = lax.rem(b, 2)
        q_rows = pl.ds(first_rows, (group_n - CORES) * tok)
        drain(qkv_ref.at[pl.ds(1, 2), b], recvkv_sem.at[b])
        drain(qkv_ref.at[0, b, q_rows], recvq_sem.at[b])
        load_kv = pltpu.make_async_copy(qkv_ref.at[pl.ds(1, 2), b], qkv_vm.at[pl.ds(1, 2)], load_sem.at[0])
        load_q = pltpu.make_async_copy(qkv_ref.at[0, b, q_rows], qkv_vm.at[0, q_rows], load_sem.at[1])
        load_kv.start()
        load_q.start()

        @pl.when(b >= 2)
        def _():
            drain_o_sends(b - 2)

        @pl.when(jnp.logical_and(b >= 1, jnp.logical_not(on_first)))
        def _():
            drain(o_ref.at[b - 1, me], oown_sem.at[b - 1])

        load_kv.wait()
        load_q.wait()
        for blk in range(CORES, group_n):
            rows = slice(blk * tok, (blk + 1) * tok)

            def one_head(h, _):
                at = pl.ds(pl.multiple_of(h * HEAD_DIM, HEAD_DIM), HEAD_DIM)
                ostage_vm[slot, rows, at] = block_attention(qkv_vm[0, rows, at], qkv_vm[1, rows, at], qkv_vm[2, rows, at],
                                                            qkv_vm[1, :blk * tok, at], qkv_vm[2, :blk * tok, at])
                return 0

            lax.fori_loop(0, heads, one_head, 0)
            send_o(b, slot, blk)

        mine = lax.broadcasted_iota(jnp.int32, (n_batch, HEAD_DIM), 0) == b
        for h in range(heads):
            at = slice(h * HEAD_DIM, (h + 1) * HEAD_DIM)
            q = qnew_vm[:, at]
            past = lax.dot_general(q, qkv_vm[1, :, at], contract_last, preferred_element_type=jnp.float32)
            last = jnp.sum(q.astype(jnp.float32) * knew_vm[:, at].astype(jnp.float32), axis=1, keepdims=True)
            top = jnp.maximum(jnp.max(past, axis=1, keepdims=True), last)
            past, last = jnp.exp2((past - top) * scale2), jnp.exp2((last - top) * scale2)
            inv = 1.0 / (jnp.sum(past, axis=1, keepdims=True) + last)
            out = jnp.dot((past * inv).astype(jnp.bfloat16), qkv_vm[2, :, at], preferred_element_type=jnp.float32)
            out = out + (last * inv).astype(jnp.bfloat16).astype(jnp.float32) * vnew_vm[:, at].astype(jnp.float32)
            deco_vm[:, at] = jnp.where(mine, out, deco_vm[:, at])

    def finish_rows(b, load_x):
        inv = lax.rsqrt(jnp.sum(ssq_vm[...], axis=1, keepdims=True) / width + NORM_EPS)
        load_x.wait()

        def out_tile(n, _):
            at = pl.ds(pl.multiple_of(n * cols, cols), cols)
            outv_vm[:, at] = (xo_vm[:, at].astype(jnp.float32) + raw_vm[:, at] * inv * post_ref[:, at]).astype(jnp.bfloat16)
            return 0

        lax.fori_loop(0, group_n, out_tile, 0)
        pltpu.make_async_copy(outv_vm, outp_ref.at[b], outv_sem).start()

    def o_copy(b, g, k):
        return pltpu.make_async_copy(o_ref.at[b, g], oin_vm.at[:, pl.ds(pl.multiple_of(g * cols, cols), cols)], oin_sem.at[k])

    def output_rows(b):
        @pl.when(jnp.logical_not(on_first))
        def _():
            drain(o_ref.at[b, pl.ds(0, group_n - 1)], orecv_sem.at[b])

        for g in range(group_n):
            o_copy(b, g, 0).start()
        load_x = pltpu.make_async_copy(x_hbm.at[b], xo_vm, xo_sem)
        load_x.start()

        @pl.when(b >= 1)
        def _():
            drain(outv_vm, outv_sem)

        @pl.when(b == 0)
        def _():
            wo_copy.wait()

        ssq_vm[...] = jnp.zeros_like(ssq_vm)
        drain(oin_vm, oin_sem.at[0])

        def col_tile(n, _):
            at = pl.ds(pl.multiple_of(n * COL_TILE, COL_TILE), COL_TILE)
            acc = jnp.dot(oin_vm[...], wo_vm[:, at], preferred_element_type=jnp.float32)
            raw_vm[:, at] = acc
            sq = acc * acc
            ssq_vm[...] += sum(sq[:, i * HEAD_DIM:(i + 1) * HEAD_DIM] for i in range(COL_TILE // HEAD_DIM))
            return 0

        lax.fori_loop(0, width // COL_TILE, col_tile, 0)
        finish_rows(b, load_x)

    def last_rows(b):
        load_x = pltpu.make_async_copy(x_hbm.at[b], xo_vm, xo_sem)
        load_x.start()

        @pl.when(on_first)
        def _():
            drain(olocal_vm, olocal_sem)

        drain(outv_vm, outv_sem)
        ssq_vm[...] = jnp.zeros_like(ssq_vm)
        both = CORES * cols
        for k, source in enumerate((chip, right, left, far)):
            if k:
                @pl.when(jnp.logical_not(on_first))
                def _():
                    for c in range(CORES):
                        drain(o_ref.at[b, source * CORES + c], orecv(b, source * CORES + c))
            else:
                @pl.when(jnp.logical_not(on_first))
                def _():
                    drain(o_ref.at[b, me], oown_sem.at[b])
                    drain(o_ref.at[b, partner], orecv(b, partner))
            for c in range(CORES):
                o_copy(b, source * CORES + c, k).start()
            part = pl.ds(pl.multiple_of(source * both, both), both)
            drain(oin_vm.at[:, part], oin_sem.at[k])

            def col_tile(n, _):
                at = pl.ds(pl.multiple_of(n * COL_TILE, COL_TILE), COL_TILE)
                acc = jnp.dot(oin_vm[:, part], wo_vm[part, at], preferred_element_type=jnp.float32)
                if k:
                    acc = acc + raw_vm[:, at]
                raw_vm[:, at] = acc
                if k == 3:
                    sq = acc * acc
                    ssq_vm[...] += sum(sq[:, i * HEAD_DIM:(i + 1) * HEAD_DIM] for i in range(COL_TILE // HEAD_DIM))
                return 0

            lax.fori_loop(0, width // COL_TILE, col_tile, 0)
        finish_rows(b, load_x)

    def send_part():
        own = pl.ds(pl.multiple_of(me * cols, cols), cols)
        part = jnp.dot(deco_vm[...].astype(jnp.bfloat16), wo_vm[own], preferred_element_type=jnp.float32)
        decp_vm[me] = part.astype(jnp.bfloat16)
        for step in range(1, group_n):
            remote(decp_vm.at[me], decp_vm.at[me], decs_sem, decr_sem, lax.rem(me + step, group_n)).start()

    def step(t, _):
        @pl.when(t < n_batch)
        def _():
            project(t)

        @pl.when(t == 1)
        def _():
            new_row()

        @pl.when(t >= 2)
        def _():
            forward_o(t - 2)

        @pl.when(t == n_batch)
        def _():
            output_rows(t - 3)

        @pl.when(t >= 1)
        def _():
            attend(t - 1)

        @pl.when(t < n_batch)
        def _():
            forward(t)

        @pl.when(jnp.logical_and(on_first, t < n_batch))
        def _():
            attend_first(t)

        @pl.when(jnp.logical_and(t >= 3, t < n_batch))
        def _():
            output_rows(t - 3)

        return 0

    lax.fori_loop(0, n_batch + 1, step, 0)
    forward_o(n_batch - 1)
    send_part()
    output_rows(n_batch - 2)

    drain(decp_vm.at[pl.ds(0, group_n - 1)], decs_sem)
    drain(decp_vm.at[pl.ds(0, group_n - 1)], decr_sem)
    proj = decp_vm[0].astype(jnp.float32)
    for g in range(1, group_n):
        proj = proj + decp_vm[g].astype(jnp.float32)
    inv = lax.rsqrt(jnp.sum(proj * proj, axis=1, keepdims=True) / width + NORM_EPS)
    outd_ref[...] = (new_ref[...].astype(jnp.float32) + proj * inv * post_ref[...]).astype(jnp.bfloat16)

    last_rows(n_batch - 1)
    for t in range(n_batch - SLOTS, n_batch):
        drain_sends(t)
    drain_o_sends(n_batch - 2)
    drain_o_sends(n_batch - 1)
    drain_forwards()
    drain(outv_vm, outv_sem)


def output_kernel(outp_ref, k_ref, v_ref, knew_ref, vnew_ref, outd_in_ref, out_ref, kc_ref, vc_ref, outd_ref):
    out_ref[...] = outp_ref[...]
    outd_ref[...] = outd_in_ref[...]
    seq, cols = k_ref.shape[2:]
    heads = cols // HEAD_DIM
    for src, new, to in ((k_ref, knew_ref, kc_ref), (v_ref, vnew_ref, vc_ref)):
        to[0, :seq] = src[0, 0].reshape(seq, heads, HEAD_DIM)
        to[0, seq:] = new[0].reshape(1, heads, HEAD_DIM)


def solution(mesh):
    group_n = mesh.shape["sp"]

    def device_step(prompt_blk, w_q, w_k, w_v, w_o, q_norm_w, k_norm_w, post_norm_w, new_rows):
        n_batch, tok, width = prompt_blk.shape
        cols = width // group_n
        heads = cols // HEAD_DIM
        seq = tok * group_n
        bf16, f32 = jnp.bfloat16, jnp.float32
        freq, sign = rope_rows()
        q_gain, k_gain, post = q_norm_w[None], k_norm_w[None], post_norm_w[None]
        any_spec = pl.BlockSpec(memory_space=pl.ANY)
        vm_spec = pl.BlockSpec(memory_space=pltpu.VMEM)
        dma = pltpu.SemaphoreType.DMA
        qkv, _, _, _, _, _, out_rows, k_new, v_new, out_d = pl.pallas_call(
            functools.partial(exchange_kernel, group_n),
            out_shape=(
                jax.ShapeDtypeStruct((3, n_batch, seq, cols), bf16),
                jax.ShapeDtypeStruct((n_batch, group_n, tok, cols), bf16),
                jax.ShapeDtypeStruct((n_batch, 2, CORES, 2, tok, cols), bf16),
                jax.ShapeDtypeStruct((n_batch, 2, CORES, tok, cols), bf16),
                jax.ShapeDtypeStruct((n_batch, 2, CORES, tok, cols), bf16),
                jax.ShapeDtypeStruct((n_batch, 2, group_n, tok, cols), bf16),
                jax.ShapeDtypeStruct((n_batch, tok, width), bf16),
                jax.ShapeDtypeStruct((n_batch, 1, cols), bf16),
                jax.ShapeDtypeStruct((n_batch, 1, cols), bf16),
                jax.ShapeDtypeStruct((n_batch, width), bf16),
            ),
            in_specs=[any_spec] * 5 + [vm_spec] * 6,
            out_specs=(any_spec,) * 7 + (vm_spec,) * 3,
            scratch_shapes=[
                pltpu.VMEM((3, width, width), bf16),
                pltpu.VMEM((2, tok, width), bf16),
                pltpu.VMEM((tok, width), f32),
                pltpu.VMEM((tok, HEAD_DIM), f32),
                pltpu.VMEM((SLOTS, 3, group_n, tok, cols), bf16),
                pltpu.VMEM((3, seq, cols), bf16),
                pltpu.VMEM((2, seq, cols), bf16),
                pltpu.VMEM((2, group_n, tok, cols), bf16),
                pltpu.VMEM((group_n, tok, cols), bf16),
                pltpu.VMEM((width, width), bf16),
                pltpu.VMEM((tok, width), bf16),
                pltpu.VMEM((tok, width), bf16),
                pltpu.VMEM((tok, width), bf16),
                pltpu.VMEM((n_batch, cols), bf16),
                pltpu.VMEM((n_batch, cols), bf16),
                pltpu.VMEM((n_batch, cols), bf16),
                pltpu.VMEM((n_batch, cols), f32),
                pltpu.VMEM((group_n, n_batch, width), bf16),
                pltpu.VMEM((tok + 8, HEAD_DIM), f32),
                pltpu.VMEM((tok + 8, HEAD_DIM), f32),
                dma((3,)), dma((2,)), dma,
                dma((n_batch,)), dma((n_batch,)), dma((n_batch,)), dma((n_batch, 2)), dma((n_batch, 2)), dma((n_batch, 2)), dma((2,)), dma((2,)), dma((2,)),
                dma((2,)), dma((n_batch,)), dma((n_batch,)), dma((n_batch + group_n,)), dma((n_batch,)), dma((n_batch,)), dma, dma, dma((group_n // CORES,)), dma, dma, dma, dma,
            ],
            compiler_params=pltpu.CompilerParams(collective_id=0, has_side_effects=True, vmem_limit_bytes=VMEM_BYTES),
        )(prompt_blk, w_q, w_k, w_v, w_o, q_gain, k_gain, post, freq, sign, new_rows)

        row = lambda shape, at: pl.BlockSpec((1,) + shape, lambda b: (b,) + at)
        whole = pl.BlockSpec((n_batch, width), lambda b: (0, 0))
        cache = row((seq + 1, heads, HEAD_DIM), (0, 0, 0))
        out_p, k_cache, v_cache, out_d = pl.pallas_call(
            output_kernel,
            grid=(n_batch,),
            out_shape=(
                jax.ShapeDtypeStruct((n_batch, tok, width), bf16),
                jax.ShapeDtypeStruct((n_batch, seq + 1, heads, HEAD_DIM), bf16),
                jax.ShapeDtypeStruct((n_batch, seq + 1, heads, HEAD_DIM), bf16),
                jax.ShapeDtypeStruct((n_batch, width), bf16),
            ),
            in_specs=[
                row((tok, width), (0, 0)),
                pl.BlockSpec((1, 1, seq, cols), lambda b: (1, b, 0, 0)),
                pl.BlockSpec((1, 1, seq, cols), lambda b: (2, b, 0, 0)),
                row((1, cols), (0, 0)),
                row((1, cols), (0, 0)),
                whole,
            ],
            out_specs=(row((tok, width), (0, 0)), cache, cache, whole),
            compiler_params=pltpu.CompilerParams(vmem_limit_bytes=VMEM_BYTES),
        )(out_rows, qkv, qkv, k_new, v_new, out_d)
        return out_p, k_cache, v_cache, out_d

    replicated = P()
    return jax.shard_map(
        device_step, mesh=mesh,
        in_specs=(P("dp", "sp", None), replicated, replicated, replicated, replicated, replicated, replicated, replicated, P("dp", None)),
        out_specs=(P("dp", "sp", None), P("dp", None, "sp", None), P("dp", None, "sp", None), P("dp", None)),
        check_vma=False)
```

```python
import functools

import jax
import jax.numpy as jnp
from jax import lax
from jax.experimental import pallas as pl
from jax.experimental.pallas import tpu as pltpu
from jax.sharding import PartitionSpec as P

HEAD_DIM = 128
ROPE_THETA = 500000.0
NORM_EPS = 1e-6
CORES = 2
LOG2E = 1.4426950408889634
SLOTS = 3
LATE = 2
COL_TILE = 512
VMEM_BYTES = 66_000_000


def rope_rows():
    lane = jnp.arange(HEAD_DIM)
    inv_freq = ROPE_THETA ** (-(2 * (lane % (HEAD_DIM // 2))).astype(jnp.float32) / HEAD_DIM)
    return inv_freq[None], jnp.where(lane < HEAD_DIM // 2, -1.0, 1.0)[None]


def rotate(values, cos_t, sin_t):
    return values * cos_t + pltpu.roll(values, HEAD_DIM // 2, 1) * sin_t


def exchange_kernel(group_n, x_hbm, wq_hbm, wk_hbm, wv_hbm, wo_hbm, qgain_ref, kgain_ref, post_ref, freq_ref, sign_ref, new_ref,
                    qkv_ref, o_ref, relkv_ref, relq_ref, relo_ref, kvp_ref, outp_ref, knew_ref, vnew_ref, outd_ref,
                    w_vm, x_vm, raw_vm, ssq_vm, stage_vm, qkv_vm, ostage_vm, kvp_vm, olocal_vm, wo_vm, oin_vm, xo_vm, outv_vm, qnew_vm, knew_vm, vnew_vm, deco_vm, decp_vm, cos_vm, sin_vm,
                    w_sem, x_sem, wo_sem, send_sem, recvkv_sem, recvq_sem, relkv_sem, relq_sem, relo_sem, fwdkv_sem, fwdq_sem, fwdo_sem,
                    load_sem, osend_sem, oown_sem, orecv_sem, kvps_sem, kvpr_sem, kvpl_sem, olocal_sem, oin_sem, xo_sem, outv_sem, decs_sem, decr_sem):
    n_batch, tok, width = x_hbm.shape
    cols = width // group_n
    heads = cols // HEAD_DIM
    first_rows = CORES * tok
    chips = group_n // CORES
    me = lax.axis_index("sp")
    chip, core = me // CORES, me % CORES
    right = (chip + 1) % chips
    left = (chip + chips - 1) % chips
    far = (chip + 2) % chips
    right_dev, left_dev = right * CORES + core, left * CORES + core
    partner = chip * CORES + (1 - core)
    on_first = chip == 0
    w_hbm = (wq_hbm, wk_hbm, wv_hbm)
    gains = (qgain_ref, kgain_ref)
    scale2 = HEAD_DIM ** -0.5 * LOG2E
    contract_last = (((1,), (1,)), ((), ()))

    def remote(src, dst, s_sem, r_sem, dev):
        return pltpu.make_async_remote_copy(src_ref=src, dst_ref=dst, send_sem=s_sem, recv_sem=r_sem,
                                            device_id={"sp": dev}, device_id_type=pl.DeviceIdType.MESH)

    def drain(ref, sem):
        pltpu.make_async_copy(ref, ref, sem).wait()

    def with_split(source, use):
        mid, shift = tok // 2, tok // 8
        for n, holds in ((mid - shift, source == 1), (mid + shift, source == chips - 1), (mid, source % 2 == 0)):
            @pl.when(holds)
            def _():
                use(n)

    def w_copy(j):
        return pltpu.make_async_copy(w_hbm[j], w_vm.at[j], w_sem.at[j])

    def x_copy(t):
        return pltpu.make_async_copy(x_hbm.at[t], x_vm.at[lax.rem(t, 2)], x_sem.at[lax.rem(t, 2)])

    x_copy(0).start()
    w_copy(2).start()
    w_copy(1).start()
    wo_copy = pltpu.make_async_copy(wo_hbm, wo_vm, wo_sem)

    barrier = pltpu.get_barrier_semaphore()
    for step in range(1, group_n):
        pl.semaphore_signal(barrier, inc=1, device_id={"sp": lax.rem(me + step, group_n)}, device_id_type=pl.DeviceIdType.MESH)
    place = lax.broadcasted_iota(jnp.int32, cos_vm.shape, 0)
    angles = jnp.where(place < tok, me * tok + place, group_n * tok).astype(jnp.float32) * freq_ref[...]
    cos_vm[...] = jnp.cos(angles)
    sin_vm[...] = jnp.sin(angles) * sign_ref[...]
    pl.semaphore_wait(barrier, group_n - 1)

    def send_tensor(t, slot, j):
        rows = pl.ds(me * tok, tok)
        far_devs = pl.ds(far * CORES, CORES)
        recv = recvkv_sem.at[t] if j else recvq_sem.at[t]

        def two_hops(n):
            for way, at, dev in ((0, pl.ds(0, n), right_dev), (1, pl.ds(n, tok - n), left_dev)):
                dst, sem = (relkv_ref.at[t, way, :, j - 1, at], relkv_sem.at[t, way]) if j else (relq_ref.at[t, way, :, at], relq_sem.at[t, way])
                remote(stage_vm.at[slot, j, far_devs, at], dst, send_sem.at[t], sem, dev).start()

        with_split(chip, two_hops)
        for side in (right, left):
            for c in range(CORES):
                dev = side * CORES + c
                remote(stage_vm.at[slot, j, dev], qkv_ref.at[j, t, rows], send_sem.at[t], recv, dev).start()
        remote(stage_vm.at[slot, j, partner], qkv_ref.at[j, t, rows], send_sem.at[t], recv, partner).start()
        pltpu.make_async_copy(stage_vm.at[slot, j, me], qkv_ref.at[j, t, rows], recv).start()

    def drain_sends(t):
        slot = lax.rem(t, SLOTS)

        @pl.when(on_first)
        def _():
            drain(stage_vm.at[slot, pl.ds(1, 2), pl.ds(0, group_n - 1)], send_sem.at[t])

        @pl.when(jnp.logical_not(on_first))
        def _():
            drain(stage_vm.at[slot, :, pl.ds(0, group_n - 1)], send_sem.at[t])

        @pl.when(me == 0)
        def _():
            drain(stage_vm.at[slot, pl.ds(1, 2)], kvps_sem.at[t])

    def project(t):
        slot = lax.rem(t, SLOTS)

        @pl.when(t >= SLOTS)
        def _():
            drain_sends(t - SLOTS)

        x_copy(t).wait()

        @pl.when(t + 1 < n_batch)
        def _():
            x_copy(t + 1).start()

        x_slot = lax.rem(t, 2)
        for j in (2, 1, 0):
            @pl.when(t == 0)
            def _():
                w_copy(j).wait()
                if j != 1:
                    (w_copy(0) if j else wo_copy).start()

            if j < 2:
                ssq_vm[...] = jnp.zeros_like(ssq_vm)

            def col_tile(n, _):
                at = pl.ds(pl.multiple_of(n * COL_TILE, COL_TILE), COL_TILE)
                acc = jnp.dot(x_vm[x_slot], w_vm[j, :, at], preferred_element_type=jnp.float32)
                if j < 2:
                    raw_vm[:, at] = acc
                    sq = acc * acc
                    ssq_vm[...] += sum(sq[:, i * HEAD_DIM:(i + 1) * HEAD_DIM] for i in range(COL_TILE // HEAD_DIM))
                else:
                    for i in range(COL_TILE // cols):
                        stage_vm[slot, j, n * (COL_TILE // cols) + i] = acc[:, i * cols:(i + 1) * cols].astype(jnp.bfloat16)
                return 0

            lax.fori_loop(0, width // COL_TILE, col_tile, 0)
            if j < 2:
                inv = lax.rsqrt(jnp.sum(ssq_vm[...], axis=1, keepdims=True) / width + NORM_EPS)

                def group_tile(n, _):
                    for h in range(heads):
                        at = pl.ds(pl.multiple_of(n * cols + h * HEAD_DIM, HEAD_DIM), HEAD_DIM)
                        normed = raw_vm[:, at] * inv * gains[j][:, at]
                        stage_vm[slot, j, n, :, h * HEAD_DIM:(h + 1) * HEAD_DIM] = rotate(normed, cos_vm[:tok], sin_vm[:tok]).astype(jnp.bfloat16)
                    return 0

                lax.fori_loop(0, group_n, group_tile, 0)
            if j:
                send_tensor(t, slot, j)
            else:
                @pl.when(jnp.logical_not(on_first))
                def _():
                    send_tensor(t, slot, j)

        @pl.when(me == 0)
        def _():
            remote(stage_vm.at[slot, pl.ds(1, 2)], kvp_ref.at[t], kvps_sem.at[t], kvpr_sem.at[t], partner).start()

    def relay_ways(use):
        with_split(left, lambda n: use(0, left, left_dev, right, 0, n))
        with_split(right, lambda n: use(1, right, right_dev, left, n, tok - n))

    def forward(b):
        def way_kv(way, source, source_dev, to, first, n):
            at, dst_rows = pl.ds(first, n), pl.ds(source_dev * tok + first, n)
            drain(relkv_ref.at[b, way, :, :, at], relkv_sem.at[b, way])
            for c in range(CORES):
                remote(relkv_ref.at[b, way, c, :, at], qkv_ref.at[pl.ds(1, 2), b, dst_rows], fwdkv_sem.at[way], recvkv_sem.at[b], to * CORES + c).start()

            @pl.when(source != 0)
            def _():
                drain(relq_ref.at[b, way, :, at], relq_sem.at[b, way])
                for c in range(CORES):
                    remote(relq_ref.at[b, way, c, at], qkv_ref.at[0, b, dst_rows], fwdq_sem.at[way], recvq_sem.at[b], to * CORES + c).start()

        relay_ways(way_kv)

    def forward_o(b):
        def way_o(way, source, source_dev, to, first, n):
            at = pl.ds(first, n)

            @pl.when(to != 0)
            def _():
                drain(relo_ref.at[b, way, :, at], relo_sem.at[b, way])
                for c in range(CORES):
                    remote(relo_ref.at[b, way, c, at], o_ref.at[b, source_dev, at], fwdo_sem.at[way], orecv_sem.at[b], to * CORES + c).start()

        relay_ways(way_o)

    def drain_forwards():
        def way_all(way, source, source_dev, to, first, n):
            at = pl.ds(first, n)
            drain(relkv_ref.at[:, way, :, :, at], fwdkv_sem.at[way])

            @pl.when(source != 0)
            def _():
                drain(relq_ref.at[:, way, :, at], fwdq_sem.at[way])

            @pl.when(to != 0)
            def _():
                drain(relo_ref.at[:, way, :, at], fwdo_sem.at[way])

        relay_ways(way_all)

    def send_o(b, slot, dev):
        src = ostage_vm.at[slot, pl.ds(dev * tok, tok)]
        c = dev % CORES
        away = lax.rem(dev // CORES - chip + chips, chips)

        @pl.when(dev == me)
        def _():
            pltpu.make_async_copy(src, o_ref.at[b, me], oown_sem.at[b]).start()

        @pl.when(jnp.logical_and(dev != me, away != 2))
        def _():
            remote(src, o_ref.at[b, me], osend_sem.at[b], orecv_sem.at[b], dev).start()

        @pl.when(away == 2)
        def _():
            def two_hops(n):
                remote(ostage_vm.at[slot, pl.ds(dev * tok, n)], relo_ref.at[b, 0, c, pl.ds(0, n)],
                       osend_sem.at[b], relo_sem.at[b, 0], right_dev).start()
                remote(ostage_vm.at[slot, pl.ds(dev * tok + n, tok - n)], relo_ref.at[b, 1, c, pl.ds(n, tok - n)],
                       osend_sem.at[b], relo_sem.at[b, 1], left_dev).start()

            with_split(chip, two_hops)

    def drain_o_sends(b):
        slot = lax.rem(b, 2)

        @pl.when(on_first)
        def _():
            drain(ostage_vm.at[slot, pl.ds(0, (group_n - CORES) * tok)], osend_sem.at[b])

        @pl.when(jnp.logical_not(on_first))
        def _():
            drain(ostage_vm.at[slot, pl.ds(0, (group_n - CORES - 1) * tok)], osend_sem.at[b])

    def new_row():
        def full(j):
            def col_tile(n, ssq):
                at = pl.ds(pl.multiple_of(n * COL_TILE, COL_TILE), COL_TILE)
                acc = jnp.dot(new_ref[...], w_vm[j, :, at], preferred_element_type=jnp.float32)
                return ssq + jnp.sum(acc * acc, axis=1, keepdims=True)

            ssq = lax.fori_loop(0, width // COL_TILE, col_tile, jnp.zeros((n_batch, 1), jnp.float32))
            return lax.rsqrt(ssq / width + NORM_EPS)

        own = pl.ds(pl.multiple_of(me * cols, cols), cols)
        for j, to in ((0, qnew_vm), (1, knew_vm)):
            inv = full(j)
            raw = jnp.dot(new_ref[...], w_vm[j, :, own], preferred_element_type=jnp.float32)
            normed = raw * inv * gains[j][:, own]
            for h in range(heads):
                at = slice(h * HEAD_DIM, (h + 1) * HEAD_DIM)
                to[:, at] = rotate(normed[:, at], cos_vm[tok:tok + 1], sin_vm[tok:tok + 1]).astype(jnp.bfloat16)
        vnew_vm[...] = jnp.dot(new_ref[...], w_vm[2, :, own], preferred_element_type=jnp.float32).astype(jnp.bfloat16)
        for b in range(n_batch):
            knew_ref[b] = knew_vm[b:b + 1]
            vnew_ref[b] = vnew_vm[b:b + 1]
        deco_vm[...] = jnp.zeros_like(deco_vm)

    def block_attention(q, k_diag, v_diag, k_past, v_past):
        keep = lax.broadcasted_iota(jnp.int32, (tok, tok), 0) >= lax.broadcasted_iota(jnp.int32, (tok, tok), 1)
        diag = lax.dot_general(q, k_diag, contract_last, preferred_element_type=jnp.float32)
        diag = jnp.where(keep, diag, -jnp.inf)
        top = jnp.max(diag, axis=1, keepdims=True)
        if k_past is not None:
            past = lax.dot_general(q, k_past, contract_last, preferred_element_type=jnp.float32)
            top = jnp.maximum(top, jnp.max(past, axis=1, keepdims=True))
            past = jnp.exp2((past - top) * scale2)
        diag = jnp.exp2((diag - top) * scale2)
        total = jnp.sum(diag, axis=1, keepdims=True)
        if k_past is not None:
            total = total + jnp.sum(past, axis=1, keepdims=True)
        inv = 1.0 / total
        out = jnp.dot((diag * inv).astype(jnp.bfloat16), v_diag, preferred_element_type=jnp.float32)
        if k_past is not None:
            out = out + jnp.dot((past * inv).astype(jnp.bfloat16), v_past, preferred_element_type=jnp.float32)
        return out.astype(jnp.bfloat16)

    def attend_first(b):
        slot = lax.rem(b, SLOTS)

        @pl.when(b >= 1)
        def _():
            drain(olocal_vm, olocal_sem)

        for which in range(CORES):
            @pl.when(core == which)
            def _():
                if which:
                    drain(kvp_ref.at[b], kvpr_sem.at[b])
                    load = pltpu.make_async_copy(kvp_ref.at[b], kvp_vm, kvpl_sem)
                    load.start()
                    load.wait()

                def group(g, _):
                    for h in range(heads):
                        at = slice(h * HEAD_DIM, (h + 1) * HEAD_DIM)
                        past = (kvp_vm[0, g, :, at], kvp_vm[1, g, :, at]) if which else (None, None)
                        olocal_vm[g, :, at] = block_attention(stage_vm[slot, 0, g, :, at], stage_vm[slot, 1, g, :, at], stage_vm[slot, 2, g, :, at], *past)
                    return 0

                lax.fori_loop(0, group_n, group, 0)

        pltpu.make_async_copy(olocal_vm, o_ref.at[b], olocal_sem).start()

    def attend(b):
        slot = lax.rem(b, 2)
        q_rows = pl.ds(first_rows, (group_n - CORES) * tok)
        drain(qkv_ref.at[pl.ds(1, 2), b], recvkv_sem.at[b])
        drain(qkv_ref.at[0, b, q_rows], recvq_sem.at[b])
        load_kv = pltpu.make_async_copy(qkv_ref.at[pl.ds(1, 2), b], qkv_vm.at[pl.ds(1, 2)], load_sem.at[0])
        load_q = pltpu.make_async_copy(qkv_ref.at[0, b, q_rows], qkv_vm.at[0, q_rows], load_sem.at[1])
        load_kv.start()
        load_q.start()

        @pl.when(b >= 2)
        def _():
            drain_o_sends(b - 2)

        @pl.when(jnp.logical_and(b >= 1, jnp.logical_not(on_first)))
        def _():
            drain(o_ref.at[b - 1, me], oown_sem.at[b - 1])

        load_kv.wait()
        load_q.wait()
        for blk in range(CORES, group_n):
            rows = slice(blk * tok, (blk + 1) * tok)

            def one_head(h, _):
                at = pl.ds(pl.multiple_of(h * HEAD_DIM, HEAD_DIM), HEAD_DIM)
                ostage_vm[slot, rows, at] = block_attention(qkv_vm[0, rows, at], qkv_vm[1, rows, at], qkv_vm[2, rows, at],
                                                            qkv_vm[1, :blk * tok, at], qkv_vm[2, :blk * tok, at])
                return 0

            lax.fori_loop(0, heads, one_head, 0)
            send_o(b, slot, blk)

        mine = lax.broadcasted_iota(jnp.int32, (n_batch, HEAD_DIM), 0) == b
        for h in range(heads):
            at = slice(h * HEAD_DIM, (h + 1) * HEAD_DIM)
            q = qnew_vm[:, at]
            past = lax.dot_general(q, qkv_vm[1, :, at], contract_last, preferred_element_type=jnp.float32)
            last = jnp.sum(q.astype(jnp.float32) * knew_vm[:, at].astype(jnp.float32), axis=1, keepdims=True)
            top = jnp.maximum(jnp.max(past, axis=1, keepdims=True), last)
            past, last = jnp.exp2((past - top) * scale2), jnp.exp2((last - top) * scale2)
            inv = 1.0 / (jnp.sum(past, axis=1, keepdims=True) + last)
            out = jnp.dot((past * inv).astype(jnp.bfloat16), qkv_vm[2, :, at], preferred_element_type=jnp.float32)
            out = out + (last * inv).astype(jnp.bfloat16).astype(jnp.float32) * vnew_vm[:, at].astype(jnp.float32)
            deco_vm[:, at] = jnp.where(mine, out, deco_vm[:, at])

    def finish_rows(b, load_x):
        inv = lax.rsqrt(jnp.sum(ssq_vm[...], axis=1, keepdims=True) / width + NORM_EPS)
        load_x.wait()

        def out_tile(n, _):
            at = pl.ds(pl.multiple_of(n * cols, cols), cols)
            outv_vm[:, at] = (xo_vm[:, at].astype(jnp.float32) + raw_vm[:, at] * inv * post_ref[:, at]).astype(jnp.bfloat16)
            return 0

        lax.fori_loop(0, group_n, out_tile, 0)
        pltpu.make_async_copy(outv_vm, outp_ref.at[b], outv_sem).start()

    def o_copy(b, g):
        return pltpu.make_async_copy(o_ref.at[b, g], oin_vm.at[:, pl.ds(pl.multiple_of(g * cols, cols), cols)], oin_sem)

    def output_rows(b):
        @pl.when(jnp.logical_not(on_first))
        def _():
            drain(o_ref.at[b, pl.ds(0, group_n - 1)], orecv_sem.at[b])

        for g in range(group_n):
            o_copy(b, g).start()
        load_x = pltpu.make_async_copy(x_hbm.at[b], xo_vm, xo_sem)
        load_x.start()

        @pl.when(b >= 1)
        def _():
            drain(outv_vm, outv_sem)

        @pl.when(b == 0)
        def _():
            wo_copy.wait()

        ssq_vm[...] = jnp.zeros_like(ssq_vm)
        drain(oin_vm, oin_sem)

        def col_tile(n, _):
            at = pl.ds(pl.multiple_of(n * COL_TILE, COL_TILE), COL_TILE)
            acc = jnp.dot(oin_vm[...], wo_vm[:, at], preferred_element_type=jnp.float32)
            raw_vm[:, at] = acc
            sq = acc * acc
            ssq_vm[...] += sum(sq[:, i * HEAD_DIM:(i + 1) * HEAD_DIM] for i in range(COL_TILE // HEAD_DIM))
            return 0

        lax.fori_loop(0, width // COL_TILE, col_tile, 0)
        finish_rows(b, load_x)

    def send_part():
        own = pl.ds(pl.multiple_of(me * cols, cols), cols)
        part = jnp.dot(deco_vm[...].astype(jnp.bfloat16), wo_vm[own], preferred_element_type=jnp.float32)
        decp_vm[me] = part.astype(jnp.bfloat16)
        for step in range(1, group_n):
            remote(decp_vm.at[me], decp_vm.at[me], decs_sem, decr_sem, lax.rem(me + step, group_n)).start()

    def step(t, _):
        @pl.when(t < n_batch)
        def _():
            project(t)

        @pl.when(t == 1)
        def _():
            new_row()

        @pl.when(t >= 2)
        def _():
            forward_o(t - 2)

        @pl.when(jnp.logical_and(on_first, t >= 1))
        def _():
            attend_first(t - 1)

        @pl.when(t >= 1)
        def _():
            attend(t - 1)

        @pl.when(t < n_batch)
        def _():
            forward(t)

        @pl.when(t == n_batch)
        def _():
            send_part()
            forward_o(n_batch - 1)

        @pl.when(jnp.logical_and(t >= 3, t < n_batch + 3 - LATE))
        def _():
            output_rows(t - 3)

        return 0

    lax.fori_loop(0, n_batch + 1, step, 0)

    drain(decp_vm.at[pl.ds(0, group_n - 1)], decs_sem)
    drain(decp_vm.at[pl.ds(0, group_n - 1)], decr_sem)
    proj = decp_vm[0].astype(jnp.float32)
    for g in range(1, group_n):
        proj = proj + decp_vm[g].astype(jnp.float32)
    inv = lax.rsqrt(jnp.sum(proj * proj, axis=1, keepdims=True) / width + NORM_EPS)
    outd_ref[...] = (new_ref[...].astype(jnp.float32) + proj * inv * post_ref[...]).astype(jnp.bfloat16)

    for t in range(n_batch - SLOTS, n_batch):
        drain_sends(t)
    drain_o_sends(n_batch - 2)
    drain_o_sends(n_batch - 1)
    drain_forwards()

    @pl.when(on_first)
    def _():
        drain(olocal_vm, olocal_sem)

    @pl.when(jnp.logical_not(on_first))
    def _():
        drain(o_ref.at[n_batch - 1, me], oown_sem.at[n_batch - 1])
        for b in range(n_batch - LATE, n_batch):
            drain(o_ref.at[b, pl.ds(0, group_n - 1)], orecv_sem.at[b])

    drain(outv_vm, outv_sem)


def output_kernel(o_ref, x_ref, wo_hbm, post_ref, outp_ref, k_ref, v_ref, knew_ref, vnew_ref, outd_in_ref, out_ref, kc_ref, vc_ref, outd_ref, wo_vm, raw_vm, wo_sem):
    _, group_n, tok, cols = o_ref.shape
    width = group_n * cols
    heads = cols // HEAD_DIM
    b, n_batch = pl.program_id(0), pl.num_programs(0)
    wo_copy = pltpu.make_async_copy(wo_hbm, wo_vm, wo_sem)

    @pl.when(b == 0)
    def _():
        wo_copy.start()

    @pl.when(b < n_batch - LATE)
    def _():
        out_ref[...] = outp_ref[...]

    @pl.when(b == n_batch - LATE)
    def _():
        wo_copy.wait()

    @pl.when(b >= n_batch - LATE)
    def _():
        o_all = jnp.concatenate([o_ref[0, g] for g in range(group_n)], axis=1)
        ssq = jnp.zeros((tok, 1), jnp.float32)
        for n in range(width // COL_TILE):
            at = slice(n * COL_TILE, (n + 1) * COL_TILE)
            acc = jnp.dot(o_all, wo_vm[:, at], preferred_element_type=jnp.float32)
            raw_vm[:, at] = acc
            ssq = ssq + jnp.sum(acc * acc, axis=1, keepdims=True)
        inv = lax.rsqrt(ssq / width + NORM_EPS)
        out_ref[0] = (x_ref[0].astype(jnp.float32) + raw_vm[...] * inv * post_ref[...]).astype(jnp.bfloat16)

    outd_ref[...] = outd_in_ref[...]
    seq = k_ref.shape[2]
    for src, new, to in ((k_ref, knew_ref, kc_ref), (v_ref, vnew_ref, vc_ref)):
        to[0, :seq] = src[0, 0].reshape(seq, heads, HEAD_DIM)
        to[0, seq:] = new[0].reshape(1, heads, HEAD_DIM)


def solution(mesh):
    group_n = mesh.shape["sp"]

    def device_step(prompt_blk, w_q, w_k, w_v, w_o, q_norm_w, k_norm_w, post_norm_w, new_rows):
        n_batch, tok, width = prompt_blk.shape
        cols = width // group_n
        heads = cols // HEAD_DIM
        seq = tok * group_n
        bf16, f32 = jnp.bfloat16, jnp.float32
        freq, sign = rope_rows()
        q_gain, k_gain, post = q_norm_w[None], k_norm_w[None], post_norm_w[None]
        any_spec = pl.BlockSpec(memory_space=pl.ANY)
        vm_spec = pl.BlockSpec(memory_space=pltpu.VMEM)
        dma = pltpu.SemaphoreType.DMA
        qkv, o_all, _, _, _, _, out_early, k_new, v_new, out_d = pl.pallas_call(
            functools.partial(exchange_kernel, group_n),
            out_shape=(
                jax.ShapeDtypeStruct((3, n_batch, seq, cols), bf16),
                jax.ShapeDtypeStruct((n_batch, group_n, tok, cols), bf16),
                jax.ShapeDtypeStruct((n_batch, 2, CORES, 2, tok, cols), bf16),
                jax.ShapeDtypeStruct((n_batch, 2, CORES, tok, cols), bf16),
                jax.ShapeDtypeStruct((n_batch, 2, CORES, tok, cols), bf16),
                jax.ShapeDtypeStruct((n_batch, 2, group_n, tok, cols), bf16),
                jax.ShapeDtypeStruct((n_batch - LATE, tok, width), bf16),
                jax.ShapeDtypeStruct((n_batch, 1, cols), bf16),
                jax.ShapeDtypeStruct((n_batch, 1, cols), bf16),
                jax.ShapeDtypeStruct((n_batch, width), bf16),
            ),
            in_specs=[any_spec] * 5 + [vm_spec] * 6,
            out_specs=(any_spec,) * 7 + (vm_spec,) * 3,
            scratch_shapes=[
                pltpu.VMEM((3, width, width), bf16),
                pltpu.VMEM((2, tok, width), bf16),
                pltpu.VMEM((tok, width), f32),
                pltpu.VMEM((tok, HEAD_DIM), f32),
                pltpu.VMEM((SLOTS, 3, group_n, tok, cols), bf16),
                pltpu.VMEM((3, seq, cols), bf16),
                pltpu.VMEM((2, seq, cols), bf16),
                pltpu.VMEM((2, group_n, tok, cols), bf16),
                pltpu.VMEM((group_n, tok, cols), bf16),
                pltpu.VMEM((width, width), bf16),
                pltpu.VMEM((tok, width), bf16),
                pltpu.VMEM((tok, width), bf16),
                pltpu.VMEM((tok, width), bf16),
                pltpu.VMEM((n_batch, cols), bf16),
                pltpu.VMEM((n_batch, cols), bf16),
                pltpu.VMEM((n_batch, cols), bf16),
                pltpu.VMEM((n_batch, cols), f32),
                pltpu.VMEM((group_n, n_batch, width), bf16),
                pltpu.VMEM((tok + 8, HEAD_DIM), f32),
                pltpu.VMEM((tok + 8, HEAD_DIM), f32),
                dma((3,)), dma((2,)), dma,
                dma((n_batch,)), dma((n_batch,)), dma((n_batch,)), dma((n_batch, 2)), dma((n_batch, 2)), dma((n_batch, 2)), dma((2,)), dma((2,)), dma((2,)),
                dma((2,)), dma((n_batch,)), dma((n_batch,)), dma((n_batch,)), dma((n_batch,)), dma((n_batch,)), dma, dma, dma, dma, dma, dma, dma,
            ],
            compiler_params=pltpu.CompilerParams(collective_id=0, has_side_effects=True, vmem_limit_bytes=VMEM_BYTES),
        )(prompt_blk, w_q, w_k, w_v, w_o, q_gain, k_gain, post, freq, sign, new_rows)

        row = lambda shape, at: pl.BlockSpec((1,) + shape, lambda b: (b,) + at)
        late = n_batch - LATE
        whole = pl.BlockSpec((n_batch, width), lambda b: (0, 0))
        cache = row((seq + 1, heads, HEAD_DIM), (0, 0, 0))
        out_p, k_cache, v_cache, out_d = pl.pallas_call(
            output_kernel,
            grid=(n_batch,),
            out_shape=(
                jax.ShapeDtypeStruct((n_batch, tok, width), bf16),
                jax.ShapeDtypeStruct((n_batch, seq + 1, heads, HEAD_DIM), bf16),
                jax.ShapeDtypeStruct((n_batch, seq + 1, heads, HEAD_DIM), bf16),
                jax.ShapeDtypeStruct((n_batch, width), bf16),
            ),
            in_specs=[
                pl.BlockSpec((1, group_n, tok, cols), lambda b: (jnp.maximum(b, late), 0, 0, 0)),
                pl.BlockSpec((1, tok, width), lambda b: (jnp.maximum(b, late), 0, 0)),
                any_spec,
                vm_spec,
                pl.BlockSpec((1, tok, width), lambda b: (jnp.minimum(b, late - 1), 0, 0)),
                pl.BlockSpec((1, 1, seq, cols), lambda b: (1, b, 0, 0)),
                pl.BlockSpec((1, 1, seq, cols), lambda b: (2, b, 0, 0)),
                row((1, cols), (0, 0)),
                row((1, cols), (0, 0)),
                whole,
            ],
            out_specs=(row((tok, width), (0, 0)), cache, cache, whole),
            scratch_shapes=[pltpu.VMEM((width, width), bf16), pltpu.VMEM((tok, width), f32), dma],
            compiler_params=pltpu.CompilerParams(vmem_limit_bytes=VMEM_BYTES),
        )(o_all, prompt_blk, w_o, post, out_early, qkv, qkv, k_new, v_new, out_d)
        return out_p, k_cache, v_cache, out_d

    replicated = P()
    return jax.shard_map(
        device_step, mesh=mesh,
        in_specs=(P("dp", "sp", None), replicated, replicated, replicated, replicated, replicated, replicated, replicated, P("dp", None)),
        out_specs=(P("dp", "sp", None), P("dp", None, "sp", None), P("dp", None, "sp", None), P("dp", None)),
        check_vma=False)
```

```python
import functools

import jax
import jax.numpy as jnp
from jax import lax
from jax.experimental import pallas as pl
from jax.experimental.pallas import tpu as pltpu
from jax.sharding import PartitionSpec as P

HEAD_DIM = 128
ROPE_THETA = 500000.0
NORM_EPS = 1e-6
CORES = 2
LOG2E = 1.4426950408889634
SLOTS = 3
LATE = 2
COL_TILE = 512
VMEM_BYTES = 66_000_000


def rope_rows():
    lane = jnp.arange(HEAD_DIM)
    inv_freq = ROPE_THETA ** (-(2 * (lane % (HEAD_DIM // 2))).astype(jnp.float32) / HEAD_DIM)
    return inv_freq[None], jnp.where(lane < HEAD_DIM // 2, -1.0, 1.0)[None]


def rotate(values, cos_t, sin_t):
    return values * cos_t + pltpu.roll(values, HEAD_DIM // 2, 1) * sin_t


def exchange_kernel(group_n, x_hbm, wq_hbm, wk_hbm, wv_hbm, wo_hbm, qgain_ref, kgain_ref, post_ref, freq_ref, sign_ref, new_ref,
                    qkv_ref, o_ref, relkv_ref, relq_ref, relo_ref, kvp_ref, outp_ref, knew_ref, vnew_ref, outd_ref,
                    w_vm, x_vm, raw_vm, ssq_vm, stage_vm, qkv_vm, ostage_vm, kvp_vm, olocal_vm, wo_vm, oin_vm, xo_vm, outv_vm, qnew_vm, knew_vm, vnew_vm, deco_vm, decp_vm, cos_vm, sin_vm,
                    w_sem, x_sem, wo_sem, send_sem, recvkv_sem, recvq_sem, relkv_sem, relq_sem, relo_sem, fwdkv_sem, fwdq_sem, fwdo_sem,
                    load_sem, osend_sem, oown_sem, orecv_sem, kvps_sem, kvpr_sem, kvpl_sem, olocal_sem, oin_sem, xo_sem, outv_sem, decs_sem, decr_sem):
    n_batch, tok, width = x_hbm.shape
    cols = width // group_n
    heads = cols // HEAD_DIM
    first_rows = CORES * tok
    chips = group_n // CORES
    me = lax.axis_index("sp")
    chip, core = me // CORES, me % CORES
    right = (chip + 1) % chips
    left = (chip + chips - 1) % chips
    far = (chip + 2) % chips
    right_dev, left_dev = right * CORES + core, left * CORES + core
    partner = chip * CORES + (1 - core)
    on_first = chip == 0
    w_hbm = (wq_hbm, wk_hbm, wv_hbm)
    gains = (qgain_ref, kgain_ref)
    scale2 = HEAD_DIM ** -0.5 * LOG2E
    contract_last = (((1,), (1,)), ((), ()))

    def remote(src, dst, s_sem, r_sem, dev):
        return pltpu.make_async_remote_copy(src_ref=src, dst_ref=dst, send_sem=s_sem, recv_sem=r_sem,
                                            device_id={"sp": dev}, device_id_type=pl.DeviceIdType.MESH)

    def drain(ref, sem):
        pltpu.make_async_copy(ref, ref, sem).wait()

    def with_split(source, use):
        mid, shift = tok // 2, tok // 8
        for n, holds in ((mid - shift, source == 1), (mid + shift, source == chips - 1), (mid, source % 2 == 0)):
            @pl.when(holds)
            def _():
                use(n)

    def w_copy(j):
        return pltpu.make_async_copy(w_hbm[j], w_vm.at[j], w_sem.at[j])

    def x_copy(t):
        return pltpu.make_async_copy(x_hbm.at[t], x_vm.at[lax.rem(t, 2)], x_sem.at[lax.rem(t, 2)])

    x_copy(0).start()
    w_copy(2).start()
    w_copy(1).start()
    wo_copy = pltpu.make_async_copy(wo_hbm, wo_vm, wo_sem)

    barrier = pltpu.get_barrier_semaphore()
    for step in range(1, group_n):
        pl.semaphore_signal(barrier, inc=1, device_id={"sp": lax.rem(me + step, group_n)}, device_id_type=pl.DeviceIdType.MESH)
    place = lax.broadcasted_iota(jnp.int32, cos_vm.shape, 0)
    angles = jnp.where(place < tok, me * tok + place, group_n * tok).astype(jnp.float32) * freq_ref[...]
    cos_vm[...] = jnp.cos(angles)
    sin_vm[...] = jnp.sin(angles) * sign_ref[...]
    pl.semaphore_wait(barrier, group_n - 1)

    def send_tensor(t, slot, j):
        rows = pl.ds(me * tok, tok)
        far_devs = pl.ds(far * CORES, CORES)
        recv = recvkv_sem.at[t] if j else recvq_sem.at[t]

        def two_hops(n):
            for way, at, dev in ((0, pl.ds(0, n), right_dev), (1, pl.ds(n, tok - n), left_dev)):
                dst, sem = (relkv_ref.at[t, way, :, j - 1, at], relkv_sem.at[t, way]) if j else (relq_ref.at[t, way, :, at], relq_sem.at[t, way])
                remote(stage_vm.at[slot, j, far_devs, at], dst, send_sem.at[t], sem, dev).start()

        with_split(chip, two_hops)
        for side in (right, left):
            for c in range(CORES):
                dev = side * CORES + c
                remote(stage_vm.at[slot, j, dev], qkv_ref.at[j, t, rows], send_sem.at[t], recv, dev).start()
        remote(stage_vm.at[slot, j, partner], qkv_ref.at[j, t, rows], send_sem.at[t], recv, partner).start()
        pltpu.make_async_copy(stage_vm.at[slot, j, me], qkv_ref.at[j, t, rows], recv).start()

    def drain_sends(t):
        slot = lax.rem(t, SLOTS)

        @pl.when(on_first)
        def _():
            drain(stage_vm.at[slot, pl.ds(1, 2), pl.ds(0, group_n - 1)], send_sem.at[t])

        @pl.when(jnp.logical_not(on_first))
        def _():
            drain(stage_vm.at[slot, :, pl.ds(0, group_n - 1)], send_sem.at[t])

        @pl.when(me == 0)
        def _():
            drain(stage_vm.at[slot, pl.ds(1, 2)], kvps_sem.at[t])

    def project(t):
        slot = lax.rem(t, SLOTS)

        @pl.when(t >= SLOTS)
        def _():
            drain_sends(t - SLOTS)

        x_copy(t).wait()

        @pl.when(t + 1 < n_batch)
        def _():
            x_copy(t + 1).start()

        x_slot = lax.rem(t, 2)
        for j in (2, 1, 0):
            @pl.when(t == 0)
            def _():
                w_copy(j).wait()
                if j != 1:
                    (w_copy(0) if j else wo_copy).start()

            if j < 2:
                ssq_vm[...] = jnp.zeros_like(ssq_vm)

            def col_tile(n, _):
                at = pl.ds(pl.multiple_of(n * COL_TILE, COL_TILE), COL_TILE)
                acc = jnp.dot(x_vm[x_slot], w_vm[j, :, at], preferred_element_type=jnp.float32)
                if j < 2:
                    raw_vm[:, at] = acc
                    sq = acc * acc
                    ssq_vm[...] += sum(sq[:, i * HEAD_DIM:(i + 1) * HEAD_DIM] for i in range(COL_TILE // HEAD_DIM))
                else:
                    for i in range(COL_TILE // cols):
                        stage_vm[slot, j, n * (COL_TILE // cols) + i] = acc[:, i * cols:(i + 1) * cols].astype(jnp.bfloat16)
                return 0

            lax.fori_loop(0, width // COL_TILE, col_tile, 0)
            if j < 2:
                inv = lax.rsqrt(jnp.sum(ssq_vm[...], axis=1, keepdims=True) / width + NORM_EPS)

                def group_tile(n, _):
                    for h in range(heads):
                        at = pl.ds(pl.multiple_of(n * cols + h * HEAD_DIM, HEAD_DIM), HEAD_DIM)
                        normed = raw_vm[:, at] * inv * gains[j][:, at]
                        stage_vm[slot, j, n, :, h * HEAD_DIM:(h + 1) * HEAD_DIM] = rotate(normed, cos_vm[:tok], sin_vm[:tok]).astype(jnp.bfloat16)
                    return 0

                lax.fori_loop(0, group_n, group_tile, 0)
            if j:
                send_tensor(t, slot, j)
            else:
                @pl.when(jnp.logical_not(on_first))
                def _():
                    send_tensor(t, slot, j)

        @pl.when(me == 0)
        def _():
            remote(stage_vm.at[slot, pl.ds(1, 2)], kvp_ref.at[t], kvps_sem.at[t], kvpr_sem.at[t], partner).start()

    def relay_ways(use):
        with_split(left, lambda n: use(0, left, left_dev, right, 0, n))
        with_split(right, lambda n: use(1, right, right_dev, left, n, tok - n))

    def forward(b):
        def way_kv(way, source, source_dev, to, first, n):
            at, dst_rows = pl.ds(first, n), pl.ds(source_dev * tok + first, n)
            drain(relkv_ref.at[b, way, :, :, at], relkv_sem.at[b, way])
            for c in range(CORES):
                remote(relkv_ref.at[b, way, c, :, at], qkv_ref.at[pl.ds(1, 2), b, dst_rows], fwdkv_sem.at[way], recvkv_sem.at[b], to * CORES + c).start()

            @pl.when(source != 0)
            def _():
                drain(relq_ref.at[b, way, :, at], relq_sem.at[b, way])
                for c in range(CORES):
                    remote(relq_ref.at[b, way, c, at], qkv_ref.at[0, b, dst_rows], fwdq_sem.at[way], recvq_sem.at[b], to * CORES + c).start()

        relay_ways(way_kv)

    def forward_o(b):
        def way_o(way, source, source_dev, to, first, n):
            at = pl.ds(first, n)

            @pl.when(to != 0)
            def _():
                drain(relo_ref.at[b, way, :, at], relo_sem.at[b, way])
                for c in range(CORES):
                    remote(relo_ref.at[b, way, c, at], o_ref.at[b, source_dev, at], fwdo_sem.at[way], orecv_sem.at[b], to * CORES + c).start()

        relay_ways(way_o)

    def drain_forwards():
        def way_all(way, source, source_dev, to, first, n):
            at = pl.ds(first, n)
            drain(relkv_ref.at[:, way, :, :, at], fwdkv_sem.at[way])

            @pl.when(source != 0)
            def _():
                drain(relq_ref.at[:, way, :, at], fwdq_sem.at[way])

            @pl.when(to != 0)
            def _():
                drain(relo_ref.at[:, way, :, at], fwdo_sem.at[way])

        relay_ways(way_all)

    def send_o(b, slot, dev):
        src = ostage_vm.at[slot, pl.ds(dev * tok, tok)]
        c = dev % CORES
        away = lax.rem(dev // CORES - chip + chips, chips)

        @pl.when(dev == me)
        def _():
            pltpu.make_async_copy(src, o_ref.at[b, me], oown_sem.at[b]).start()

        @pl.when(jnp.logical_and(dev != me, away != 2))
        def _():
            remote(src, o_ref.at[b, me], osend_sem.at[b], orecv_sem.at[b], dev).start()

        @pl.when(away == 2)
        def _():
            def two_hops(n):
                remote(ostage_vm.at[slot, pl.ds(dev * tok, n)], relo_ref.at[b, 0, c, pl.ds(0, n)],
                       osend_sem.at[b], relo_sem.at[b, 0], right_dev).start()
                remote(ostage_vm.at[slot, pl.ds(dev * tok + n, tok - n)], relo_ref.at[b, 1, c, pl.ds(n, tok - n)],
                       osend_sem.at[b], relo_sem.at[b, 1], left_dev).start()

            with_split(chip, two_hops)

    def drain_o_sends(b):
        slot = lax.rem(b, 2)

        @pl.when(on_first)
        def _():
            drain(ostage_vm.at[slot, pl.ds(0, (group_n - CORES) * tok)], osend_sem.at[b])

        @pl.when(jnp.logical_not(on_first))
        def _():
            drain(ostage_vm.at[slot, pl.ds(0, (group_n - CORES - 1) * tok)], osend_sem.at[b])

    def new_row():
        def full(j):
            def col_tile(n, ssq):
                at = pl.ds(pl.multiple_of(n * COL_TILE, COL_TILE), COL_TILE)
                acc = jnp.dot(new_ref[...], w_vm[j, :, at], preferred_element_type=jnp.float32)
                return ssq + jnp.sum(acc * acc, axis=1, keepdims=True)

            ssq = lax.fori_loop(0, width // COL_TILE, col_tile, jnp.zeros((n_batch, 1), jnp.float32))
            return lax.rsqrt(ssq / width + NORM_EPS)

        own = pl.ds(pl.multiple_of(me * cols, cols), cols)
        for j, to in ((0, qnew_vm), (1, knew_vm)):
            inv = full(j)
            raw = jnp.dot(new_ref[...], w_vm[j, :, own], preferred_element_type=jnp.float32)
            normed = raw * inv * gains[j][:, own]
            for h in range(heads):
                at = slice(h * HEAD_DIM, (h + 1) * HEAD_DIM)
                to[:, at] = rotate(normed[:, at], cos_vm[tok:tok + 1], sin_vm[tok:tok + 1]).astype(jnp.bfloat16)
        vnew_vm[...] = jnp.dot(new_ref[...], w_vm[2, :, own], preferred_element_type=jnp.float32).astype(jnp.bfloat16)
        for b in range(n_batch):
            knew_ref[b] = knew_vm[b:b + 1]
            vnew_ref[b] = vnew_vm[b:b + 1]
        deco_vm[...] = jnp.zeros_like(deco_vm)

    def block_attention(q, k_diag, v_diag, k_past, v_past):
        keep = lax.broadcasted_iota(jnp.int32, (tok, tok), 0) >= lax.broadcasted_iota(jnp.int32, (tok, tok), 1)
        diag = lax.dot_general(q, k_diag, contract_last, preferred_element_type=jnp.float32)
        diag = jnp.where(keep, diag, -jnp.inf)
        top = jnp.max(diag, axis=1, keepdims=True)
        if k_past is not None:
            past = lax.dot_general(q, k_past, contract_last, preferred_element_type=jnp.float32)
            top = jnp.maximum(top, jnp.max(past, axis=1, keepdims=True))
            past = jnp.exp2((past - top) * scale2)
        diag = jnp.exp2((diag - top) * scale2)
        total = jnp.sum(diag, axis=1, keepdims=True)
        if k_past is not None:
            total = total + jnp.sum(past, axis=1, keepdims=True)
        inv = 1.0 / total
        out = jnp.dot((diag * inv).astype(jnp.bfloat16), v_diag, preferred_element_type=jnp.float32)
        if k_past is not None:
            out = out + jnp.dot((past * inv).astype(jnp.bfloat16), v_past, preferred_element_type=jnp.float32)
        return out.astype(jnp.bfloat16)

    def attend_first(b):
        slot = lax.rem(b, SLOTS)

        @pl.when(b >= 1)
        def _():
            drain(olocal_vm, olocal_sem)

        for which in range(CORES):
            @pl.when(core == which)
            def _():
                if which:
                    drain(kvp_ref.at[b], kvpr_sem.at[b])
                    load = pltpu.make_async_copy(kvp_ref.at[b], kvp_vm, kvpl_sem)
                    load.start()
                    load.wait()

                def group(g, _):
                    for h in range(heads):
                        at = slice(h * HEAD_DIM, (h + 1) * HEAD_DIM)
                        past = (kvp_vm[0, g, :, at], kvp_vm[1, g, :, at]) if which else (None, None)
                        olocal_vm[g, :, at] = block_attention(stage_vm[slot, 0, g, :, at], stage_vm[slot, 1, g, :, at], stage_vm[slot, 2, g, :, at], *past)
                    return 0

                lax.fori_loop(0, group_n, group, 0)

        pltpu.make_async_copy(olocal_vm, o_ref.at[b], olocal_sem).start()

    def attend(b):
        slot = lax.rem(b, 2)
        q_rows = pl.ds(first_rows, (group_n - CORES) * tok)
        drain(qkv_ref.at[pl.ds(1, 2), b], recvkv_sem.at[b])
        drain(qkv_ref.at[0, b, q_rows], recvq_sem.at[b])
        load_kv = pltpu.make_async_copy(qkv_ref.at[pl.ds(1, 2), b], qkv_vm.at[pl.ds(1, 2)], load_sem.at[0])
        load_q = pltpu.make_async_copy(qkv_ref.at[0, b, q_rows], qkv_vm.at[0, q_rows], load_sem.at[1])
        load_kv.start()
        load_q.start()

        @pl.when(b >= 2)
        def _():
            drain_o_sends(b - 2)

        @pl.when(jnp.logical_and(b >= 1, jnp.logical_not(on_first)))
        def _():
            drain(o_ref.at[b - 1, me], oown_sem.at[b - 1])

        load_kv.wait()
        load_q.wait()
        for blk in range(CORES, group_n):
            rows = slice(blk * tok, (blk + 1) * tok)

            def one_head(h, _):
                at = pl.ds(pl.multiple_of(h * HEAD_DIM, HEAD_DIM), HEAD_DIM)
                ostage_vm[slot, rows, at] = block_attention(qkv_vm[0, rows, at], qkv_vm[1, rows, at], qkv_vm[2, rows, at],
                                                            qkv_vm[1, :blk * tok, at], qkv_vm[2, :blk * tok, at])
                return 0

            lax.fori_loop(0, heads, one_head, 0)
            send_o(b, slot, blk)

        mine = lax.broadcasted_iota(jnp.int32, (n_batch, HEAD_DIM), 0) == b
        for h in range(heads):
            at = slice(h * HEAD_DIM, (h + 1) * HEAD_DIM)
            q = qnew_vm[:, at]
            past = lax.dot_general(q, qkv_vm[1, :, at], contract_last, preferred_element_type=jnp.float32)
            last = jnp.sum(q.astype(jnp.float32) * knew_vm[:, at].astype(jnp.float32), axis=1, keepdims=True)
            top = jnp.maximum(jnp.max(past, axis=1, keepdims=True), last)
            past, last = jnp.exp2((past - top) * scale2), jnp.exp2((last - top) * scale2)
            inv = 1.0 / (jnp.sum(past, axis=1, keepdims=True) + last)
            out = jnp.dot((past * inv).astype(jnp.bfloat16), qkv_vm[2, :, at], preferred_element_type=jnp.float32)
            out = out + (last * inv).astype(jnp.bfloat16).astype(jnp.float32) * vnew_vm[:, at].astype(jnp.float32)
            deco_vm[:, at] = jnp.where(mine, out, deco_vm[:, at])

    def finish_rows(b, load_x):
        inv = lax.rsqrt(jnp.sum(ssq_vm[...], axis=1, keepdims=True) / width + NORM_EPS)
        load_x.wait()

        def out_tile(n, _):
            at = pl.ds(pl.multiple_of(n * cols, cols), cols)
            outv_vm[:, at] = (xo_vm[:, at].astype(jnp.float32) + raw_vm[:, at] * inv * post_ref[:, at]).astype(jnp.bfloat16)
            return 0

        lax.fori_loop(0, group_n, out_tile, 0)
        pltpu.make_async_copy(outv_vm, outp_ref.at[b], outv_sem).start()

    def o_copy(b, g):
        return pltpu.make_async_copy(o_ref.at[b, g], oin_vm.at[:, pl.ds(pl.multiple_of(g * cols, cols), cols)], oin_sem)

    def output_rows(b):
        @pl.when(jnp.logical_not(on_first))
        def _():
            drain(o_ref.at[b, pl.ds(0, group_n - 1)], orecv_sem.at[b])

        for g in range(group_n):
            o_copy(b, g).start()
        load_x = pltpu.make_async_copy(x_hbm.at[b], xo_vm, xo_sem)
        load_x.start()

        @pl.when(b >= 1)
        def _():
            drain(outv_vm, outv_sem)

        @pl.when(b == 0)
        def _():
            wo_copy.wait()

        ssq_vm[...] = jnp.zeros_like(ssq_vm)
        drain(oin_vm, oin_sem)

        def col_tile(n, _):
            at = pl.ds(pl.multiple_of(n * COL_TILE, COL_TILE), COL_TILE)
            acc = jnp.dot(oin_vm[...], wo_vm[:, at], preferred_element_type=jnp.float32)
            raw_vm[:, at] = acc
            sq = acc * acc
            ssq_vm[...] += sum(sq[:, i * HEAD_DIM:(i + 1) * HEAD_DIM] for i in range(COL_TILE // HEAD_DIM))
            return 0

        lax.fori_loop(0, width // COL_TILE, col_tile, 0)
        finish_rows(b, load_x)

    def send_part():
        own = pl.ds(pl.multiple_of(me * cols, cols), cols)
        part = jnp.dot(deco_vm[...].astype(jnp.bfloat16), wo_vm[own], preferred_element_type=jnp.float32)
        decp_vm[me] = part.astype(jnp.bfloat16)
        for step in range(1, group_n):
            remote(decp_vm.at[me], decp_vm.at[me], decs_sem, decr_sem, lax.rem(me + step, group_n)).start()

    def step(t, _):
        @pl.when(t < n_batch)
        def _():
            project(t)

        @pl.when(t == 1)
        def _():
            new_row()

        @pl.when(t >= 2)
        def _():
            forward_o(t - 2)

        @pl.when(jnp.logical_and(on_first, t >= 1))
        def _():
            attend_first(t - 1)

        @pl.when(t >= 1)
        def _():
            attend(t - 1)

        @pl.when(t < n_batch)
        def _():
            forward(t)

        @pl.when(t == n_batch)
        def _():
            send_part()
            forward_o(n_batch - 1)

        @pl.when(jnp.logical_and(t >= 3, t < n_batch + 3 - LATE))
        def _():
            output_rows(t - 3)

        return 0

    lax.fori_loop(0, n_batch + 1, step, 0)

    drain(decp_vm.at[pl.ds(0, group_n - 1)], decs_sem)
    drain(decp_vm.at[pl.ds(0, group_n - 1)], decr_sem)
    proj = decp_vm[0].astype(jnp.float32)
    for g in range(1, group_n):
        proj = proj + decp_vm[g].astype(jnp.float32)
    inv = lax.rsqrt(jnp.sum(proj * proj, axis=1, keepdims=True) / width + NORM_EPS)
    outd_ref[...] = (new_ref[...].astype(jnp.float32) + proj * inv * post_ref[...]).astype(jnp.bfloat16)

    for t in range(n_batch - SLOTS, n_batch):
        drain_sends(t)
    drain_o_sends(n_batch - 2)
    drain_o_sends(n_batch - 1)
    drain_forwards()

    @pl.when(on_first)
    def _():
        drain(olocal_vm, olocal_sem)

    @pl.when(jnp.logical_not(on_first))
    def _():
        drain(o_ref.at[n_batch - 1, me], oown_sem.at[n_batch - 1])
        for b in range(n_batch - LATE, n_batch):
            drain(o_ref.at[b, pl.ds(0, group_n - 1)], orecv_sem.at[b])

    drain(outv_vm, outv_sem)


def output_kernel(o_ref, x_ref, wo_hbm, post_ref, outp_ref, k_ref, v_ref, knew_ref, vnew_ref, outd_in_ref, out_ref, kc_ref, vc_ref, outd_ref, wo_vm, raw_vm, wo_sem):
    _, group_n, tok, cols = o_ref.shape
    width = group_n * cols
    heads = cols // HEAD_DIM
    b, n_batch = pl.program_id(0), pl.num_programs(0)
    late = n_batch - LATE
    first = late - LATE
    wo_copy = pltpu.make_async_copy(wo_hbm, wo_vm, wo_sem)

    @pl.when(b == 0)
    def _():
        wo_copy.start()

    @pl.when(b < late)
    def _():
        out_ref[...] = outp_ref[...]

    @pl.when(b == first)
    def _():
        wo_copy.wait()

    @pl.when(b >= first)
    def _():
        which, half = (b - first) // 2, (b - first) % 2
        o_all = jnp.concatenate([o_ref[0, g] for g in range(group_n)], axis=1)
        for n in range(width // 2 // COL_TILE):
            at = pl.ds(pl.multiple_of(half * (width // 2) + n * COL_TILE, COL_TILE), COL_TILE)
            raw_vm[which, :, at] = jnp.dot(o_all, wo_vm[:, at], preferred_element_type=jnp.float32)

    @pl.when(b >= late)
    def _():
        rows = raw_vm[b - late]
        inv = lax.rsqrt(jnp.sum(rows * rows, axis=1, keepdims=True) / width + NORM_EPS)
        out_ref[0] = (x_ref[0].astype(jnp.float32) + rows * inv * post_ref[...]).astype(jnp.bfloat16)

    outd_ref[...] = outd_in_ref[...]
    seq = k_ref.shape[2]
    for src, new, to in ((k_ref, knew_ref, kc_ref), (v_ref, vnew_ref, vc_ref)):
        to[0, :seq] = src[0, 0].reshape(seq, heads, HEAD_DIM)
        to[0, seq:] = new[0].reshape(1, heads, HEAD_DIM)


def solution(mesh):
    group_n = mesh.shape["sp"]

    def device_step(prompt_blk, w_q, w_k, w_v, w_o, q_norm_w, k_norm_w, post_norm_w, new_rows):
        n_batch, tok, width = prompt_blk.shape
        cols = width // group_n
        heads = cols // HEAD_DIM
        seq = tok * group_n
        bf16, f32 = jnp.bfloat16, jnp.float32
        freq, sign = rope_rows()
        q_gain, k_gain, post = q_norm_w[None], k_norm_w[None], post_norm_w[None]
        any_spec = pl.BlockSpec(memory_space=pl.ANY)
        vm_spec = pl.BlockSpec(memory_space=pltpu.VMEM)
        dma = pltpu.SemaphoreType.DMA
        qkv, o_all, _, _, _, _, out_early, k_new, v_new, out_d = pl.pallas_call(
            functools.partial(exchange_kernel, group_n),
            out_shape=(
                jax.ShapeDtypeStruct((3, n_batch, seq, cols), bf16),
                jax.ShapeDtypeStruct((n_batch, group_n, tok, cols), bf16),
                jax.ShapeDtypeStruct((n_batch, 2, CORES, 2, tok, cols), bf16),
                jax.ShapeDtypeStruct((n_batch, 2, CORES, tok, cols), bf16),
                jax.ShapeDtypeStruct((n_batch, 2, CORES, tok, cols), bf16),
                jax.ShapeDtypeStruct((n_batch, 2, group_n, tok, cols), bf16),
                jax.ShapeDtypeStruct((n_batch - LATE, tok, width), bf16),
                jax.ShapeDtypeStruct((n_batch, 1, cols), bf16),
                jax.ShapeDtypeStruct((n_batch, 1, cols), bf16),
                jax.ShapeDtypeStruct((n_batch, width), bf16),
            ),
            in_specs=[any_spec] * 5 + [vm_spec] * 6,
            out_specs=(any_spec,) * 7 + (vm_spec,) * 3,
            scratch_shapes=[
                pltpu.VMEM((3, width, width), bf16),
                pltpu.VMEM((2, tok, width), bf16),
                pltpu.VMEM((tok, width), f32),
                pltpu.VMEM((tok, HEAD_DIM), f32),
                pltpu.VMEM((SLOTS, 3, group_n, tok, cols), bf16),
                pltpu.VMEM((3, seq, cols), bf16),
                pltpu.VMEM((2, seq, cols), bf16),
                pltpu.VMEM((2, group_n, tok, cols), bf16),
                pltpu.VMEM((group_n, tok, cols), bf16),
                pltpu.VMEM((width, width), bf16),
                pltpu.VMEM((tok, width), bf16),
                pltpu.VMEM((tok, width), bf16),
                pltpu.VMEM((tok, width), bf16),
                pltpu.VMEM((n_batch, cols), bf16),
                pltpu.VMEM((n_batch, cols), bf16),
                pltpu.VMEM((n_batch, cols), bf16),
                pltpu.VMEM((n_batch, cols), f32),
                pltpu.VMEM((group_n, n_batch, width), bf16),
                pltpu.VMEM((tok + 8, HEAD_DIM), f32),
                pltpu.VMEM((tok + 8, HEAD_DIM), f32),
                dma((3,)), dma((2,)), dma,
                dma((n_batch,)), dma((n_batch,)), dma((n_batch,)), dma((n_batch, 2)), dma((n_batch, 2)), dma((n_batch, 2)), dma((2,)), dma((2,)), dma((2,)),
                dma((2,)), dma((n_batch,)), dma((n_batch,)), dma((n_batch,)), dma((n_batch,)), dma((n_batch,)), dma, dma, dma, dma, dma, dma, dma,
            ],
            compiler_params=pltpu.CompilerParams(collective_id=0, has_side_effects=True, vmem_limit_bytes=VMEM_BYTES),
        )(prompt_blk, w_q, w_k, w_v, w_o, q_gain, k_gain, post, freq, sign, new_rows)

        row = lambda shape, at: pl.BlockSpec((1,) + shape, lambda b: (b,) + at)
        late = n_batch - LATE
        whole = pl.BlockSpec((n_batch, width), lambda b: (0, 0))
        cache = row((seq + 1, heads, HEAD_DIM), (0, 0, 0))
        out_p, k_cache, v_cache, out_d = pl.pallas_call(
            output_kernel,
            grid=(n_batch,),
            out_shape=(
                jax.ShapeDtypeStruct((n_batch, tok, width), bf16),
                jax.ShapeDtypeStruct((n_batch, seq + 1, heads, HEAD_DIM), bf16),
                jax.ShapeDtypeStruct((n_batch, seq + 1, heads, HEAD_DIM), bf16),
                jax.ShapeDtypeStruct((n_batch, width), bf16),
            ),
            in_specs=[
                pl.BlockSpec((1, group_n, tok, cols), lambda b: (late + b // late, 0, 0, 0)),
                pl.BlockSpec((1, tok, width), lambda b: (jnp.maximum(b, late), 0, 0)),
                any_spec,
                vm_spec,
                pl.BlockSpec((1, tok, width), lambda b: (jnp.minimum(b, late - 1), 0, 0)),
                pl.BlockSpec((1, 1, seq, cols), lambda b: (1, b, 0, 0)),
                pl.BlockSpec((1, 1, seq, cols), lambda b: (2, b, 0, 0)),
                row((1, cols), (0, 0)),
                row((1, cols), (0, 0)),
                whole,
            ],
            out_specs=(row((tok, width), (0, 0)), cache, cache, whole),
            scratch_shapes=[pltpu.VMEM((width, width), bf16), pltpu.VMEM((LATE, tok, width), f32), dma],
            compiler_params=pltpu.CompilerParams(vmem_limit_bytes=VMEM_BYTES),
        )(o_all, prompt_blk, w_o, post, out_early, qkv, qkv, k_new, v_new, out_d)
        return out_p, k_cache, v_cache, out_d

    replicated = P()
    return jax.shard_map(
        device_step, mesh=mesh,
        in_specs=(P("dp", "sp", None), replicated, replicated, replicated, replicated, replicated, replicated, replicated, P("dp", None)),
        out_specs=(P("dp", "sp", None), P("dp", None, "sp", None), P("dp", None, "sp", None), P("dp", None)),
        check_vma=False)
```
